128 devices in a mesh: layer: 32 (over z, x, core), split: 4 (over y).
Axes of the slice: x: 4, y: 4, z: 4, core: 2. Of those that a mesh axis runs over, the one named last changes fastest.
Arguments:
- right_side: float32 [128, 512, 128], P('layer', 'split'), may hold values from -6 to 6
- diagonal: float32 [128, 512, 128], P('layer', 'split'), may hold values from 0.1 to 1
- inverses: float32 [128, 512, 512], P('layer', None, 'split'), may hold values from -1 to 1, as said below
Outputs:
- solution_field: float32 [128, 512, 128], P('layer', 'split')
- residual: float32 [128, 512, 128], P('layer', 'split')
The draws below stay inside these ranges and needn't reach their ends.
Inputs may be any that keep to these rules, and one draw needn't show every extreme that they name: `inverses`: each plane's inverse is a diagonal matrix with entries between 0.5 and 1 plus a dense coupling with zero diagonal and spectral norm below 0.2.
All inputs are finite; a program needn't handle non-finite values.
Results may differ from the reference program's by a relative error of at most 0.0003.
Values sent between devices are 32-bit elements; how exact they have to be, the bound alone decides.
A program may use at most 64 MiB of HBM per device.

```python
import jax
import jax.numpy as jnp
from jax import lax

NX = 512
NY = 128
SHEET_TOTAL = 128


def draw_inverses(key, part):
    speed_seed, sheet_seed, pulse_seed, linkage_seed = jax.random.split(jax.random.fold_in(key, 11), 4)
    low_rate = jnp.log(0.5 / SHEET_TOTAL)
    high_rate = jnp.log(1.0 / 30.0)
    base_rate = jnp.exp(jax.random.uniform(speed_seed, (1, NX), jnp.float32, low_rate, high_rate))
    plane_factor = jax.random.uniform(sheet_seed, (SHEET_TOTAL, 1), jnp.float32, 0.6, 1.4)
    retained_share = jnp.exp(-base_rate * plane_factor)
    pulse_batches = jax.random.uniform(pulse_seed, (SHEET_TOTAL, 1), jnp.float32) < 6.0 / SHEET_TOTAL
    retained_share = jnp.where(pulse_batches, 0.6 * retained_share, retained_share)
    coupling = jax.random.normal(linkage_seed, (SHEET_TOTAL, NX, NX), jnp.float32) * (0.05 / jnp.sqrt(1.0 * NX))
    identity = jnp.eye(NX, dtype=jnp.float32)[None, :, :]
    coupling = coupling * (1.0 - identity)
    return coupling + retained_share[:, :, None] * identity


def block_scale(own_key, extent, shards, smallest, high):
    def one(axis_at, parts):
        steps = jax.random.uniform(jax.random.fold_in(jax.random.fold_in(own_key, 6), axis_at), (parts,), jnp.float32, smallest / len(shards), high / len(shards))
        return jnp.repeat(jnp.exp(steps), extent[axis_at] // parts).reshape((-1,) + (1,) * (len(extent) - axis_at - 1))

    level = one(*shards[0])
    for cut in shards[1:]:
        level = level * one(*cut)
    return level


def gaussian(stream_key, dims, deviation, limit, shards=(), kind=jnp.bfloat16):
    gain = block_scale(stream_key, dims, shards, -0.22, 0.18) if shards else 1.0
    values = jax.random.normal(stream_key, dims, jnp.float32) * deviation * gain
    return jnp.minimum(jnp.maximum(values, -limit), limit).astype(kind)


def setup_inputs(seed: int = 0) -> dict:
    key_list = jax.random.split(jax.random.key(seed), 4)
    right_side = gaussian(key_list[0], (SHEET_TOTAL, NX, NY), 1.0, 6.0, ((0, 32), (1, 4)), jnp.float32)
    diagonal = jnp.clip(0.1 + 0.9 * jax.random.uniform(key_list[1], (SHEET_TOTAL, NX, NY), jnp.float32) ** block_scale(key_list[1], (SHEET_TOTAL, NX, NY), ((0, 32), (1, 4)), -0.2, 0.2), 0.1, 1.0)
    inverses = draw_inverses(jax.random.fold_in(key_list[3], 71), 0)
    return {"right_side": right_side, "diagonal": diagonal, "inverses": inverses}


def stencil(values, diagonal):
    padded = jnp.pad(values, 1)
    beside = padded[2:, 1:-1, 1:-1] + padded[:-2, 1:-1, 1:-1]
    beside = beside + padded[1:-1, 2:, 1:-1] + padded[1:-1, :-2, 1:-1]
    beside = beside + padded[1:-1, 1:-1, 2:] + padded[1:-1, 1:-1, :-2]
    return (6.0 + diagonal) * values - beside


def reference(right_side, diagonal, inverses):
    highest = lax.Precision.HIGHEST

    def down_plane(carried, inputs):
        matrix, source = inputs
        carried = jnp.dot(matrix, source + carried, precision=highest)
        return carried, carried

    start = jnp.zeros((NX, NY), jnp.float32)
    _, lower_sweep = lax.scan(down_plane, start, (inverses, right_side))

    def up_plane(carried, inputs):
        matrix, below = inputs
        summed = below + jnp.dot(matrix, carried, precision=highest)
        return summed, summed

    _, direction = lax.scan(up_plane, start, (inverses, lower_sweep), reverse=True)
    image = stencil(direction, diagonal)
    step_alpha = jnp.sum(right_side * right_side) / jnp.sum(right_side * image)
    middle = right_side - step_alpha * image
    tangent = stencil(middle, diagonal)
    step_omega = jnp.sum(tangent * middle) / jnp.sum(tangent * tangent)
    return step_alpha * direction + step_omega * middle, middle - step_omega * tangent
```

```python
import functools

import jax
import jax.numpy as jnp
from jax import lax
from jax.experimental import pallas as pl
from jax.experimental.pallas import tpu as pltpu
from jax.sharding import PartitionSpec as P

MESH = pl.DeviceIdType.MESH
F32 = jnp.float32
BF16 = jnp.bfloat16


def split2(x):
    high = x.astype(BF16)
    return high, (x - high.astype(F32)).astype(BF16)


def mm(x, w_high, w_low):
    high, low = split2(x)
    dot = functools.partial(jnp.dot, preferred_element_type=F32)
    return dot(high, w_high) + (dot(low, w_high) + dot(high, w_low))


def mm_ref(x, pair):
    return mm(x, pair[0], pair[1])


def store_pair(pair, x):
    high, low = split2(x)
    pair[0] = high
    pair[1] = low


def sweep_kernel(
    nlayer, nsplit, nchunk,
    rhs_ref, inv_ref, out_ref,
    gbuf, mats, rsend, cols, low, pf, qf, pown, qown, pall, qall, pin, qin,
    cvec, cin, ain, aout, amid, evec, ein, bin_, bout, bcore,
    rs_send, rs_recv, g_send, g_recv, c_send, c_recv, d_send, d_recv, u_send, u_recv,
):
    planes, nx, width = inv_ref.shape
    ysize = rhs_ref.shape[2]
    yb = ysize // nsplit
    cb = yb // nchunk
    half = width // 2
    layer = lax.axis_index("layer")
    s = lax.axis_index("split")
    core = lax.rem(layer, 2)
    chip = layer // 2
    nchip = nlayer // 2
    right = lax.rem(s + 1, nsplit)
    left = lax.rem(s + nsplit - 1, nsplit)
    other = layer + 1 - 2 * core
    first = chip == 0
    last = chip == nchip - 1

    def rows(owner, start, size):
        return pl.ds(pl.multiple_of(owner * width + start, half), size)

    barrier = pltpu.get_barrier_semaphore()

    def greet(l, t):
        pl.semaphore_signal(barrier, inc=1, device_id=(l, t), device_id_type=MESH)

    for d in range(1, nsplit):
        greet(layer, lax.rem(s + d, nsplit))
    greet(other, s)

    @pl.when(jnp.logical_and(core == 0, jnp.logical_not(first)))
    def _():
        greet(layer - 2, s)

    @pl.when(jnp.logical_and(core == 0, jnp.logical_not(last)))
    def _():
        greet(layer + 2, s)

    for k in range(planes):
        gbuf[k, rows(s, 0, width), :] = inv_ref[k].T
    for k in range(planes):
        rsend[k] = rhs_ref[k].T
    for k in range(planes):
        cols[k, :, pl.ds(pl.multiple_of(s * width, width), width)] = rsend[
            k, pl.ds(pl.multiple_of(s * yb, yb), yb), :
        ]

    ends = jnp.where(first, 1, 0) + jnp.where(last, 1, 0)
    pl.semaphore_wait(barrier, nsplit + jnp.where(core == 0, 2 - ends, 0))

    def remote(src, dst, send, recv, l, t):
        return pltpu.make_async_remote_copy(
            src_ref=src, dst_ref=dst, send_sem=send, recv_sem=recv,
            device_id=(l, t), device_id_type=MESH,
        )

    def regroup(d):
        t = lax.rem(s + d, nsplit)
        return remote(
            rsend.at[:, pl.ds(pl.multiple_of(t * yb, yb), yb), :],
            cols.at[:, :, pl.ds(pl.multiple_of(s * width, width), width)],
            rs_send.at[d - 1], rs_recv.at[d - 1], layer, t,
        )

    def own_right(k):
        part = gbuf.at[k, rows(s, 0, width), :]
        return remote(part, part, g_send.at[0, k], g_recv.at[0, k], layer, right)

    def own_left(k):
        part = gbuf.at[k, rows(s, 0, width), :]
        return remote(part, part, g_send.at[1, k], g_recv.at[1, k], layer, left)

    def pass_right(k):
        part = gbuf.at[k, rows(left, 0, half), :]
        return remote(part, part, g_send.at[2, k], g_recv.at[2, k], layer, right)

    def pass_left(k):
        part = gbuf.at[k, rows(right, half, half), :]
        return remote(part, part, g_send.at[3, k], g_recv.at[3, k], layer, left)

    for d in range(1, nsplit):
        regroup(d).start()
    for k in range(min(2, planes)):
        own_right(k).start()
        own_left(k).start()

    def relay(k):
        own_right(k).wait_recv()
        pass_right(k).start()
        own_left(k).wait_recv()
        pass_left(k).start()
        if k + 2 < planes:
            own_right(k + 2).start()
            own_left(k + 2).start()

    def absorb(k):
        pass_right(k).wait_recv()
        pass_left(k).wait_recv()
        full = gbuf[k]
        high, lowpart = split2(full)
        mats[k, 0] = high
        mats[k, 1] = lowpart
        if k == 0:
            for d in range(1, nsplit):
                regroup(d).wait_recv()
            cvec[...] = mm(cols[0], high, lowpart)
            pf[...] = full
            qown[0] = high
            qown[1] = lowpart
        else:
            cvec[...] = mm(cols[k] + cvec[...], high, lowpart)
            pf[...] = mm(pf[...], high, lowpart)

    def absorb_up(k):
        if k > 0:
            qf[...] = mm(gbuf[k], qown[0], qown[1])
            store_pair(qown, qf[...])

    for k in range(planes):
        relay(k)
        if k > 0:
            absorb(k - 1)
            absorb_up(k - 1)
    absorb(planes - 1)

    give_p = remote(pf, pin, c_send.at[0], c_recv.at[0], other, s)
    give_q = remote(qf, qin, c_send.at[1], c_recv.at[1], other, s)
    give_c = remote(cvec, cin, c_send.at[2], c_recv.at[2], other, s)
    give_a = remote(amid, ain.at[pl.ds(0, yb), :], c_send.at[3], c_recv.at[3], other, s)
    give_e = remote(evec, ein, c_send.at[4], c_recv.at[4], other, s)

    def chunk(q):
        return pl.ds(q * cb, cb)

    def give_b(q):
        return remote(
            bin_.at[chunk(q), :], bcore.at[chunk(q), :],
            c_send.at[5 + q], c_recv.at[5 + q], other, s,
        )

    def hand_down(q):
        return remote(
            aout.at[chunk(q), :], ain.at[chunk(q), :], d_send.at[q], d_recv.at[q], layer + 2, s
        )

    def hand_up(q):
        return remote(
            bout.at[chunk(q), :], bin_.at[chunk(q), :], u_send.at[q], u_recv.at[q], layer - 2, s
        )

    @pl.when(core == 1)
    def _():
        give_c.start()
        give_p.start()

    absorb_up(planes - 1)

    def down_sweep(state):
        for k in range(planes):
            source = cols[k] if state is None else cols[k] + state
            state = mm(source, mats[k, 0], mats[k, 1])
            low[k] = state

    def up_partial():
        state = low[planes - 1]
        for k in range(planes - 2, -1, -1):
            state = low[k] + mm(state, mats[k, 0], mats[k, 1])
        evec[...] = state

    def up_sweep(state):
        for k in range(planes - 1, -1, -1):
            if state is None:
                state = low[k]
            else:
                state = low[k] + mm(state, mats[k, 0], mats[k, 1])
            out_ref[k] = state

    @pl.when(core == 1)
    def _():
        give_q.start()
        give_a.wait_recv()
        down_sweep(ain[pl.ds(0, yb), :])
        up_partial()
        give_e.start()

        @pl.when(last)
        def _():
            up_sweep(None)

        @pl.when(jnp.logical_not(last))
        def _():
            for q in range(nchunk):
                give_b(q).wait_recv()
            up_sweep(bcore[...])

        give_c.wait_send()
        give_p.wait_send()
        give_q.wait_send()
        give_e.wait_send()

    @pl.when(core == 0)
    def _():
        store_pair(pown, pf[...])
        give_c.wait_recv()
        give_p.wait_recv()
        store_pair(pin_pair := pall, pin[...])
        aout[...] = mm_ref(cvec[...], pin_pair) + cin[...]

        @pl.when(first)
        def _():
            for q in range(nchunk):
                hand_down(q).start()
            amid[...] = cvec[...]
            give_a.start()
            down_sweep(None)

        @pl.when(jnp.logical_not(first))
        def _():
            product = mm_ref(pf[...], pin_pair)
            store_pair(pall, product)
            for q in range(nchunk):
                hand_down(q).wait_recv()
                aout[chunk(q), :] = aout[chunk(q), :] + mm_ref(ain[chunk(q), :], pall)

                @pl.when(jnp.logical_not(last))
                def _():
                    hand_down(q).start()

            amid[...] = cvec[...] + mm_ref(ain[pl.ds(0, yb), :], pown)
            give_a.start()
            down_sweep(ain[pl.ds(0, yb), :])

        up_partial()
        give_q.wait_recv()
        store_pair(qin_pair := pown, qin[...])
        give_e.wait_recv()
        bout[...] = evec[...] + mm_ref(ein[...], qown)

        @pl.when(last)
        def _():
            for q in range(nchunk):
                hand_up(q).start()
            up_sweep(ein[...])

        @pl.when(jnp.logical_not(last))
        def _():
            store_pair(qall, mm_ref(qin[...], qown))
            for q in range(nchunk):
                hand_up(q).wait_recv()
                give_b(q).start()

                @pl.when(jnp.logical_not(first))
                def _():
                    bout[chunk(q), :] = bout[chunk(q), :] + mm_ref(bin_[chunk(q), :], qall)
                    hand_up(q).start()

            up_sweep(ein[...] + mm_ref(bin_[...], qin_pair))
            for q in range(nchunk):
                give_b(q).wait_send()
                hand_down(q).wait_send()

        @pl.when(jnp.logical_not(first))
        def _():
            for q in range(nchunk):
                hand_up(q).wait_send()

        give_a.wait_send()

    for d in range(1, nsplit):
        regroup(d).wait_send()
    for k in range(planes):
        own_right(k).wait_send()
        own_left(k).wait_send()
        pass_right(k).wait_send()
        pass_left(k).wait_send()


def sweeps(right_side, inverses, nlayer, nsplit):
    planes, nx, width = inverses.shape
    ysize = right_side.shape[2]
    yb = ysize // nsplit
    nchunk = 2
    vmem = pl.BlockSpec(memory_space=pltpu.VMEM)
    square = pltpu.VMEM((nx, nx), F32)
    pair = pltpu.VMEM((2, nx, nx), BF16)
    strip = pltpu.VMEM((yb, nx), F32)
    dma = pltpu.SemaphoreType.DMA
    return pl.pallas_call(
        functools.partial(sweep_kernel, nlayer, nsplit, nchunk),
        out_shape=jax.ShapeDtypeStruct((planes, yb, nx), F32),
        in_specs=[vmem, vmem],
        out_specs=vmem,
        scratch_shapes=[
            pltpu.VMEM((planes, nx, nx), F32),
            pltpu.VMEM((planes, 2, nx, nx), BF16),
            pltpu.VMEM((planes, ysize, width), F32),
            pltpu.VMEM((planes, yb, nx), F32),
            pltpu.VMEM((planes, yb, nx), F32),
            square, square, pair, pair, pair, pair, square, square,
            strip, strip, strip, strip, strip, strip, strip, strip, strip, strip,
            dma((nsplit - 1,)), dma((nsplit - 1,)),
            dma((4, planes)), dma((4, planes)),
            dma((5 + nchunk,)), dma((5 + nchunk,)),
            dma((nchunk,)), dma((nchunk,)),
            dma((nchunk,)), dma((nchunk,)),
        ],
        compiler_params=pltpu.CompilerParams(
            collective_id=0, has_side_effects=True, vmem_limit_bytes=56 * 1024 * 1024
        ),
        name="sweeps",
    )(right_side, inverses)


def shifted(x, axis, dim):
    size, length = lax.axis_size(axis), x.shape[dim]
    up = [(i, i + 1) for i in range(size - 1)]
    last = lax.slice_in_dim(x, length - 1, length, axis=dim)
    first = lax.slice_in_dim(x, 0, 1, axis=dim)
    low = lax.ppermute(last, axis, up)
    high = lax.ppermute(first, axis, [(b, a) for a, b in up])
    return low, high


def stencil(values, diagonal):
    low0, high0 = shifted(values, "layer", 0)
    low1, high1 = shifted(values, "split", 1)
    beside = jnp.concatenate([low0, values[:-1]], 0) + jnp.concatenate([values[1:], high0], 0)
    beside = beside + jnp.concatenate([low1, values[:, :-1]], 1)
    beside = beside + jnp.concatenate([values[:, 1:], high1], 1)
    y_upper = jnp.pad(values[:, :, 1:], ((0, 0), (0, 0), (0, 1)))
    y_lower = jnp.pad(values[:, :, :-1], ((0, 0), (0, 0), (1, 0)))
    return (6.0 + diagonal) * values - beside - y_upper - y_lower


def per_device(nlayer, nsplit, right_side, diagonal, inverses):
    applied_rhs = stencil(right_side, diagonal)
    swept = sweeps(right_side, inverses, nlayer, nsplit)
    regrouped = lax.all_to_all(swept, "split", split_axis=2, concat_axis=1, tiled=True)
    direction = jnp.swapaxes(regrouped, 1, 2)
    image = stencil(direction, diagonal)
    applied_image = stencil(image, diagonal)
    pairs = (
        (right_side, right_side), (right_side, image),
        (applied_rhs, right_side), (applied_rhs, image),
        (applied_image, right_side), (applied_image, image),
        (applied_rhs, applied_rhs), (applied_rhs, applied_image), (applied_image, applied_image),
    )
    sums = lax.psum(jnp.stack([jnp.sum(a * b) for a, b in pairs]), ("layer", "split"))
    rr, ri, ar, ai, br, bi, aa, ab, bb = [sums[i] for i in range(9)]
    alpha = rr / ri
    middle = right_side - alpha * image
    tangent = applied_rhs - alpha * applied_image
    cross = ar - alpha * (ai + br) + alpha * alpha * bi
    own = aa - 2.0 * alpha * ab + alpha * alpha * bb
    omega = cross / own
    return alpha * direction + omega * middle, middle - omega * tangent


def solution(mesh):
    spec = P("layer", "split", None)
    return jax.shard_map(
        functools.partial(per_device, mesh.shape["layer"], mesh.shape["split"]),
        mesh=mesh,
        in_specs=(spec, spec, P("layer", None, "split")),
        out_specs=(spec, spec),
        check_vma=False,
    )
```

```python
import functools

import jax
import jax.numpy as jnp
from jax import lax
from jax.experimental import pallas as pl
from jax.experimental.pallas import tpu as pltpu
from jax.sharding import PartitionSpec as P

MESH = pl.DeviceIdType.MESH
F32 = jnp.float32
BF16 = jnp.bfloat16


def split2(x):
    high = x.astype(BF16)
    return high, (x - high.astype(F32)).astype(BF16)


def mm(x, w_high, w_low):
    high, low = split2(x)
    dot = functools.partial(jnp.dot, preferred_element_type=F32)
    n = x.shape[0]
    if n > 128:
        return dot(high, w_high) + (dot(low, w_high) + dot(high, w_low))
    both = dot(jnp.concatenate([high, low], 0), w_high)
    return both[:n] + (both[n:] + dot(high, w_low))


def mm_ref(x, pair):
    return mm(x, pair[0], pair[1])


def store_pair(pair, x):
    high, low = split2(x)
    pair[0] = high
    pair[1] = low


def sweep_kernel(
    nlayer, nsplit, nchunk, nrow,
    rhs_ref, diag_ref, inv_ref, sol_ref, res_ref,
    gbuf, mats, rsend, dsend, cols, dcols, low, dirb, imb, aimb, arb,
    pf, qf, pown, qown, pall, qall, pin, qin,
    cvec, cin, ain, aout, amid, evec, ein, bin_, bout, bcore,
    zlow, zhigh, ylow, yhigh, edges, lines, flat, part, group, whole,
    rs_send, rs_recv, g_send, g_recv, c_send, c_recv, d_send, d_recv, u_send, u_recv,
    h_send, h_recv, l_send, l_recv, n_send, n_recv, w_send, w_recv,
):
    planes, nx, width = inv_ref.shape
    ysize = rhs_ref.shape[2]
    yb = ysize // nsplit
    cb = yb // nchunk
    half = width // 2
    layer = lax.axis_index("layer")
    s = lax.axis_index("split")
    core = lax.rem(layer, 2)
    chip = layer // 2
    nchip = nlayer // 2
    right = lax.rem(s + 1, nsplit)
    left = lax.rem(s + nsplit - 1, nsplit)
    other = layer + 1 - 2 * core
    first = chip == 0
    last = chip == nchip - 1

    def rows(owner, start, size):
        return pl.ds(pl.multiple_of(owner * width + start, half), size)

    def lanes(t):
        return pl.ds(pl.multiple_of(t * width, width), width)

    def lines_of(t):
        return pl.ds(pl.multiple_of(t * yb, yb), yb)

    for empty in (zlow, zhigh, ylow, yhigh, edges, part):
        empty[...] = jnp.zeros_like(empty)

    barrier = pltpu.get_barrier_semaphore()

    def greet(l, t):
        pl.semaphore_signal(barrier, inc=1, device_id=(l, t), device_id_type=MESH)

    for d in range(1, nsplit):
        greet(layer, lax.rem(s + d, nsplit))
    for d in range(nsplit):
        greet(other, lax.rem(s + d, nsplit))
    for d in range(1, nchip):
        greet(2 * lax.rem(chip + d, nchip) + core, s)
    side = layer - 1 + 2 * core
    inner = jnp.logical_and(side >= 0, side < nlayer)

    @pl.when(inner)
    def _():
        greet(side, s)

    for k in range(planes):
        gbuf[k, rows(s, 0, width), :] = inv_ref[k].T
    for source, sent, mine in ((rhs_ref, rsend, cols), (diag_ref, dsend, dcols)):
        for k in range(planes):
            sent[k] = source[k].T
        for k in range(planes):
            mine[k, :, lanes(s)] = sent[k, lines_of(s), :]

    pl.semaphore_wait(barrier, 2 * nsplit - 1 + nchip - 1 + jnp.where(inner, 1, 0))

    def remote(src, dst, send, recv, l, t):
        return pltpu.make_async_remote_copy(
            src_ref=src, dst_ref=dst, send_sem=send, recv_sem=recv,
            device_id=(l, t), device_id_type=MESH,
        )

    def regroup(n, d):
        t = lax.rem(s + d, nsplit)
        sent, mine = ((rsend, cols), (dsend, dcols))[n]
        return remote(
            sent.at[:, lines_of(t), :], mine.at[:, :, lanes(s)],
            rs_send.at[n, d - 1], rs_recv.at[n, d - 1], layer, t,
        )

    def spread(n, d):
        t = lax.rem(s + d, nsplit)
        return remote(
            (dirb, imb, aimb, arb)[n].at[:, :, lanes(t)], lines.at[n, :, lines_of(s), :],
            l_send.at[n, d - 1], l_recv.at[n, d - 1], layer, t,
        )

    def spread_start(n):
        for d in range(1, nsplit):
            spread(n, d).start()
        for k in range(planes):
            lines[n, k, lines_of(s), :] = (dirb, imb, aimb, arb)[n][k, :, lanes(s)]

    def spread_finish(n):
        for d in range(1, nsplit):
            spread(n, d).wait_recv()
        for k in range(planes):
            flat[n, k] = lines[n, k].T

    def halo(n, i):
        values = (cols, dirb, imb)[n]
        src = (values.at[planes - 1], values.at[0], edges.at[n, 0], edges.at[n, 1])[i]
        dst = (zlow, zhigh, ylow, yhigh)[i].at[n]
        l, t = ((layer + 1, s), (layer - 1, s), (layer, s + 1), (layer, s - 1))[i]
        return remote(src, dst, h_send.at[n, i], h_recv.at[n, i], l, t)

    to_high, to_low = layer < nlayer - 1, layer > 0
    to_right, to_left = s < nsplit - 1, s > 0
    gives = (to_high, to_low, to_right, to_left)
    takes = (to_low, to_high, to_left, to_right)

    def halo_start(n):
        values = (cols, dirb, imb)[n]
        for i in range(2):
            pl.when(gives[i])(lambda i=i: halo(n, i).start())
        for k in range(planes):
            edges[n, 0, k : k + 1, :] = values[k, yb - 1 : yb, :]
            edges[n, 1, k : k + 1, :] = values[k, 0:1, :]
        for i in range(2, 4):
            pl.when(gives[i])(lambda i=i: halo(n, i).start())

    def halo_wait(n):
        for i in range(4):
            pl.when(takes[i])(lambda i=i: halo(n, i).wait_recv())

    row = lax.broadcasted_iota(jnp.int32, (yb, nx), 0)
    lane = lax.broadcasted_iota(jnp.int32, (yb, nx), 1)

    def apply_operator(n, result):
        values = (cols, dirb, imb)[n]
        for k in range(planes):
            v = values[k]
            below = values[k - 1] if k > 0 else zlow[n]
            above = values[k + 1] if k < planes - 1 else zhigh[n]
            x_low = jnp.where(lane == 0, 0.0, pltpu.roll(v, 1, 1))
            x_high = jnp.where(lane == nx - 1, 0.0, pltpu.roll(v, nx - 1, 1))
            y_low = jnp.where(row == 0, ylow[n, k : k + 1, :], pltpu.roll(v, 1, 0))
            y_high = jnp.where(row == yb - 1, yhigh[n, k : k + 1, :], pltpu.roll(v, yb - 1, 0))
            beside = (below + above) + (x_low + x_high) + (y_low + y_high)
            result[k] = (6.0 + dcols[k]) * v - beside

    def put_sum(i, a, b):
        total = a[0] * b[0]
        for k in range(1, planes):
            total = total + a[k] * b[k]
        total = jnp.sum(total, axis=0, keepdims=True)
        lane_sum = total[:, :width]
        for t in range(1, nsplit):
            lane_sum = lane_sum + total[:, t * width : (t + 1) * width]
        part[i : i + 1, :] = lane_sum

    def prepare():
        for d in range(1, nsplit):
            regroup(1, d).wait_recv()
        halo_wait(0)
        apply_operator(0, arb)
        spread_start(3)
        put_sum(0, cols, cols)
        put_sum(1, arb, cols)
        put_sum(2, arb, arb)

    def own_right(k):
        part = gbuf.at[k, rows(s, 0, width), :]
        return remote(part, part, g_send.at[0, k], g_recv.at[0, k], layer, right)

    def own_left(k):
        part = gbuf.at[k, rows(s, 0, width), :]
        return remote(part, part, g_send.at[1, k], g_recv.at[1, k], layer, left)

    def pass_right(k):
        part = gbuf.at[k, rows(left, 0, half), :]
        return remote(part, part, g_send.at[2, k], g_recv.at[2, k], layer, right)

    def pass_left(k):
        part = gbuf.at[k, rows(right, half, half), :]
        return remote(part, part, g_send.at[3, k], g_recv.at[3, k], layer, left)

    for d in range(1, nsplit):
        regroup(0, d).start()
    for k in range(min(2, planes)):
        own_right(k).start()
        own_left(k).start()

    def relay(k):
        own_right(k).wait_recv()
        pass_right(k).start()
        own_left(k).wait_recv()
        pass_left(k).start()
        if k + 2 < planes:
            own_right(k + 2).start()
            own_left(k + 2).start()
        if k == planes - 1:
            for d in range(1, nsplit):
                regroup(1, d).start()

    def absorb(k):
        pass_right(k).wait_recv()
        pass_left(k).wait_recv()
        full = gbuf[k]
        high, lowpart = split2(full)
        mats[k, 0] = high
        mats[k, 1] = lowpart
        if k == 0:
            for d in range(1, nsplit):
                regroup(0, d).wait_recv()
            halo_start(0)
            cvec[...] = mm(cols[0], high, lowpart)
            pf[...] = full
            qown[0] = high
            qown[1] = lowpart
        else:
            cvec[...] = mm(cols[k] + cvec[...], high, lowpart)
            pf[...] = mm(pf[...], high, lowpart)

    def absorb_up(k):
        if k > 0:
            qf[...] = mm(gbuf[k], qown[0], qown[1])
            store_pair(qown, qf[...])

    for k in range(planes):
        relay(k)
        if k > 0:
            absorb(k - 1)
            absorb_up(k - 1)
    absorb(planes - 1)

    give_p = remote(pf, pin, c_send.at[0], c_recv.at[0], other, s)
    give_q = remote(qf, qin, c_send.at[1], c_recv.at[1], other, s)
    give_c = remote(cvec, cin, c_send.at[2], c_recv.at[2], other, s)
    give_a = remote(amid, ain.at[pl.ds(0, yb), :], c_send.at[3], c_recv.at[3], other, s)
    give_e = remote(evec, ein, c_send.at[4], c_recv.at[4], other, s)

    def chunk(q):
        return pl.ds(q * cb, cb)

    def give_b(q):
        return remote(
            bin_.at[chunk(q), :], bcore.at[chunk(q), :],
            c_send.at[5 + q], c_recv.at[5 + q], other, s,
        )

    def hand_down(q):
        return remote(
            aout.at[chunk(q), :], ain.at[chunk(q), :], d_send.at[q], d_recv.at[q], layer + 2, s
        )

    def hand_up(q):
        return remote(
            bout.at[chunk(q), :], bin_.at[chunk(q), :], u_send.at[q], u_recv.at[q], layer - 2, s
        )

    @pl.when(core == 1)
    def _():
        give_c.start()
        give_p.start()

    absorb_up(planes - 1)

    def down_sweep(state):
        for k in range(planes):
            source = cols[k] if state is None else cols[k] + state
            state = mm(source, mats[k, 0], mats[k, 1])
            low[k] = state

    def up_partial():
        state = low[planes - 1]
        for k in range(planes - 2, -1, -1):
            state = low[k] + mm(state, mats[k, 0], mats[k, 1])
        evec[...] = state

    def up_sweep(state):
        for k in range(planes - 1, -1, -1):
            if state is None:
                state = low[k]
            else:
                state = low[k] + mm(state, mats[k, 0], mats[k, 1])
            dirb[k] = state

    @pl.when(core == 1)
    def _():
        give_q.start()
        prepare()
        give_a.wait_recv()
        down_sweep(ain[pl.ds(0, yb), :])
        up_partial()
        give_e.start()

        @pl.when(last)
        def _():
            up_sweep(None)

        @pl.when(jnp.logical_not(last))
        def _():
            for q in range(nchunk):
                give_b(q).wait_recv()
            up_sweep(bcore[...])

        give_c.wait_send()
        give_p.wait_send()
        give_q.wait_send()
        give_e.wait_send()

    @pl.when(core == 0)
    def _():
        store_pair(pown, pf[...])
        give_c.wait_recv()
        give_p.wait_recv()
        store_pair(pall, pin[...])
        aout[...] = mm_ref(cvec[...], pall) + cin[...]

        @pl.when(last)
        def _():
            prepare()

        @pl.when(first)
        def _():
            for q in range(nchunk):
                hand_down(q).start()
            amid[...] = cvec[...]
            give_a.start()
            down_sweep(None)

        @pl.when(jnp.logical_not(first))
        def _():
            product = mm_ref(pf[...], pall)
            store_pair(pall, product)
            for q in range(nchunk):
                hand_down(q).wait_recv()
                aout[chunk(q), :] = aout[chunk(q), :] + mm_ref(ain[chunk(q), :], pall)

                @pl.when(jnp.logical_not(last))
                def _():
                    hand_down(q).start()

            amid[...] = cvec[...] + mm_ref(ain[pl.ds(0, yb), :], pown)
            give_a.start()
            down_sweep(ain[pl.ds(0, yb), :])

        up_partial()
        give_q.wait_recv()
        store_pair(pown, qin[...])
        give_e.wait_recv()
        bout[...] = evec[...] + mm_ref(ein[...], qown)

        @pl.when(last)
        def _():
            for q in range(nchunk):
                hand_up(q).start()
            up_sweep(ein[...])

        @pl.when(jnp.logical_not(last))
        def _():
            store_pair(qall, mm_ref(qin[...], qown))
            prepare()
            for q in range(nchunk):
                hand_up(q).wait_recv()
                give_b(q).start()

                @pl.when(jnp.logical_not(first))
                def _():
                    bout[chunk(q), :] = bout[chunk(q), :] + mm_ref(bin_[chunk(q), :], qall)
                    hand_up(q).start()

            up_sweep(ein[...] + mm_ref(bin_[...], pown))
            for q in range(nchunk):
                give_b(q).wait_send()
                hand_down(q).wait_send()

        @pl.when(jnp.logical_not(first))
        def _():
            for q in range(nchunk):
                hand_up(q).wait_send()

        give_a.wait_send()

    halo_start(1)
    spread_start(0)
    halo_wait(1)
    apply_operator(1, imb)
    halo_start(2)
    spread_start(1)
    halo_wait(2)
    apply_operator(2, aimb)
    spread_start(2)
    put_sum(3, cols, imb)
    put_sum(4, arb, imb)
    put_sum(5, aimb, cols)
    put_sum(6, aimb, imb)
    put_sum(7, arb, aimb)
    put_sum(8, aimb, aimb)

    place = core * nsplit + s
    count = 2 * nsplit

    def near(d):
        at = lax.rem(place + d, count)
        return remote(
            group.at[place], group.at[place], n_send.at[d - 1], n_recv.at[d - 1],
            2 * chip + at // nsplit, lax.rem(at, nsplit),
        )

    def far(d):
        at = lax.rem(chip + d, nchip)
        return remote(
            whole.at[chip], whole.at[chip], w_send.at[d - 1], w_recv.at[d - 1],
            2 * at + core, s,
        )

    group[place] = part[...]
    for d in range(1, count):
        near(d).start()
    for n in (3, 0):
        spread_finish(n)
    for d in range(1, count):
        near(d).wait_recv()
    total = group[0]
    for i in range(1, count):
        total = total + group[i]
    whole[chip] = total
    for d in range(1, nchip):
        far(d).start()
    for n in (1, 2):
        spread_finish(n)
    for d in range(1, nchip):
        far(d).wait_recv()
    total = whole[0]
    for i in range(1, nchip):
        total = total + whole[i]
    sums = jnp.sum(total, axis=1, keepdims=True)
    rr, ar, aa, ri, ai, br, bi, ab, bb = [sums[i : i + 1, :] for i in range(9)]
    alpha = rr / ri
    cross = ar - alpha * (ai + br) + alpha * alpha * bi
    own = aa - 2.0 * alpha * ab + alpha * alpha * bb
    omega = cross / own
    for k in range(planes):
        middle = rhs_ref[k] - alpha * flat[1, k]
        sol_ref[k] = alpha * flat[0, k] + omega * middle
        res_ref[k] = middle - omega * (flat[3, k] - alpha * flat[2, k])

    for n in range(2):
        for d in range(1, nsplit):
            regroup(n, d).wait_send()
    for k in range(planes):
        own_right(k).wait_send()
        own_left(k).wait_send()
        pass_right(k).wait_send()
        pass_left(k).wait_send()
    for n in range(4):
        for d in range(1, nsplit):
            spread(n, d).wait_send()
    for n in range(3):
        for i in range(4):
            pl.when(gives[i])(lambda n=n, i=i: halo(n, i).wait_send())
    for d in range(1, count):
        near(d).wait_send()
    for d in range(1, nchip):
        far(d).wait_send()


def per_device(nlayer, nsplit, right_side, diagonal, inverses):
    planes, nx, width = inverses.shape
    ysize = right_side.shape[2]
    yb = ysize // nsplit
    nchip = nlayer // 2
    nchunk = 2
    nrow = 16
    vmem = pl.BlockSpec(memory_space=pltpu.VMEM)
    square = pltpu.VMEM((nx, nx), F32)
    pair = pltpu.VMEM((2, nx, nx), BF16)
    strip = pltpu.VMEM((yb, nx), F32)
    columns = pltpu.VMEM((planes, yb, nx), F32)
    block = pltpu.VMEM((planes, ysize, width), F32)
    dma = pltpu.SemaphoreType.DMA
    shape = jax.ShapeDtypeStruct((planes, width, ysize), F32)
    return pl.pallas_call(
        functools.partial(sweep_kernel, nlayer, nsplit, nchunk, nrow),
        out_shape=(shape, shape),
        in_specs=[vmem] * 3,
        out_specs=(vmem, vmem),
        scratch_shapes=[
            pltpu.VMEM((planes, nx, nx), F32),
            pltpu.VMEM((planes, 2, nx, nx), BF16),
            block, block,
            columns, columns, columns, columns, columns, columns, columns,
            square, square, pair, pair, pair, pair, square, square,
            strip, strip, strip, strip, strip, strip, strip, strip, strip, strip,
            pltpu.VMEM((3, yb, nx), F32), pltpu.VMEM((3, yb, nx), F32),
            pltpu.VMEM((3, 8, nx), F32), pltpu.VMEM((3, 8, nx), F32),
            pltpu.VMEM((3, 2, 8, nx), F32),
            pltpu.VMEM((4, planes, ysize, width), F32),
            pltpu.VMEM((4, planes, width, ysize), F32),
            pltpu.VMEM((nrow, width), F32),
            pltpu.VMEM((2 * nsplit, nrow, width), F32),
            pltpu.VMEM((nchip, nrow, width), F32),
            dma((2, nsplit - 1)), dma((2, nsplit - 1)),
            dma((4, planes)), dma((4, planes)),
            dma((5 + nchunk,)), dma((5 + nchunk,)),
            dma((nchunk,)), dma((nchunk,)),
            dma((nchunk,)), dma((nchunk,)),
            dma((3, 4)), dma((3, 4)),
            dma((4, nsplit - 1)), dma((4, nsplit - 1)),
            dma((2 * nsplit - 1,)), dma((2 * nsplit - 1,)),
            dma((nchip - 1,)), dma((nchip - 1,)),
        ],
        compiler_params=pltpu.CompilerParams(
            collective_id=0, has_side_effects=True, vmem_limit_bytes=56 * 1024 * 1024
        ),
        name="sweeps",
    )(right_side, diagonal, inverses)


def solution(mesh):
    spec = P("layer", "split", None)
    return jax.shard_map(
        functools.partial(per_device, mesh.shape["layer"], mesh.shape["split"]),
        mesh=mesh,
        in_specs=(spec, spec, P("layer", None, "split")),
        out_specs=(spec, spec),
        check_vma=False,
    )
```

```python
import functools

import jax
import jax.numpy as jnp
from jax import lax
from jax.experimental import pallas as pl
from jax.experimental.pallas import tpu as pltpu
from jax.sharding import PartitionSpec as P

MESH = pl.DeviceIdType.MESH
F32 = jnp.float32
BF16 = jnp.bfloat16


def split2(x):
    high = x.astype(BF16)
    return high, (x - high.astype(F32)).astype(BF16)


def mm(x, w_high, w_low):
    high, low = split2(x)
    dot = functools.partial(jnp.dot, preferred_element_type=F32)
    n = x.shape[0]
    if n > 128:
        return dot(high, w_high) + (dot(low, w_high) + dot(high, w_low))
    both = dot(jnp.concatenate([high, low], 0), w_high)
    return both[:n] + (both[n:] + dot(high, w_low))


def mm_ref(x, pair):
    return mm(x, pair[0], pair[1])


def mm_pairs(x, pair):
    dot = functools.partial(jnp.dot, preferred_element_type=F32)
    return dot(x[0], pair[0]) + (dot(x[1], pair[0]) + dot(x[0], pair[1]))


def store_pair(pair, x):
    high, low = split2(x)
    pair[0] = high
    pair[1] = low


def sweep_kernel(
    nlayer, nsplit, nchunk, nrow,
    rhs_ref, diag_ref, inv_ref, sol_ref, res_ref,
    gbuf, mats, rsend, dsend, cols, dcols, low, dirb, imb, aimb, arb,
    pf, qf, pown, qown, pall, qall, q1, pin, qin,
    cvec, cin, ain, amid, evec, ein, bin_, bcore, zin, zout,
    xf, mbuf, xpair, xrow, vown, vbuf, inbuf,
    zlow, zhigh, ylow, yhigh, edges, lines, flat, part, group, whole,
    rs_send, rs_recv, g_send, g_recv, c_send, c_recv,
    x_send, x_recv, v_send, v_recv, i_send, i_recv, z_send, z_recv, y_send, y_recv,
    h_send, h_recv, l_send, l_recv, n_send, n_recv, w_send, w_recv,
):
    planes, nx, width = inv_ref.shape
    ysize = rhs_ref.shape[2]
    yb = ysize // nsplit
    cb = yb // nchunk
    half = width // 2
    layer = lax.axis_index("layer")
    s = lax.axis_index("split")
    core = lax.rem(layer, 2)
    chip = layer // 2
    nchip = nlayer // 2
    right = lax.rem(s + 1, nsplit)
    left = lax.rem(s + nsplit - 1, nsplit)
    other = layer + 1 - 2 * core
    npos = 4
    pos, line = lax.rem(chip, npos), chip // npos
    nline = nchip // npos

    def rows(owner, start, size):
        return pl.ds(pl.multiple_of(owner * width + start, half), size)

    def lanes(t):
        return pl.ds(pl.multiple_of(t * width, width), width)

    def lines_of(t):
        return pl.ds(pl.multiple_of(t * yb, yb), yb)

    for empty in (zlow, zhigh, ylow, yhigh, edges, part):
        empty[...] = jnp.zeros_like(empty)

    barrier = pltpu.get_barrier_semaphore()

    def greet(l, t):
        pl.semaphore_signal(barrier, inc=1, device_id=(l, t), device_id_type=MESH)

    for d in range(1, nsplit):
        greet(layer, lax.rem(s + d, nsplit))
    for d in range(nsplit):
        greet(other, lax.rem(s + d, nsplit))
    for d in range(1, nchip):
        greet(2 * lax.rem(chip + d, nchip) + core, s)
    side = layer - 1 + 2 * core
    inner = jnp.logical_and(side >= 0, side < nlayer)

    @pl.when(inner)
    def _():
        greet(side, s)

    for k in range(planes):
        gbuf[k, rows(s, 0, width), :] = inv_ref[k].T
    for source, sent, mine in ((rhs_ref, rsend, cols), (diag_ref, dsend, dcols)):
        for k in range(planes):
            sent[k] = source[k].T
        for k in range(planes):
            mine[k, :, lanes(s)] = sent[k, lines_of(s), :]

    pl.semaphore_wait(barrier, 2 * nsplit - 1 + nchip - 1 + jnp.where(inner, 1, 0))

    def remote(src, dst, send, recv, l, t):
        return pltpu.make_async_remote_copy(
            src_ref=src, dst_ref=dst, send_sem=send, recv_sem=recv,
            device_id=(l, t), device_id_type=MESH,
        )

    def regroup(n, d):
        t = lax.rem(s + d, nsplit)
        sent, mine = ((rsend, cols), (dsend, dcols))[n]
        return remote(
            sent.at[:, lines_of(t), :], mine.at[:, :, lanes(s)],
            rs_send.at[n, d - 1], rs_recv.at[n, d - 1], layer, t,
        )

    def spread(n, d):
        t = lax.rem(s + d, nsplit)
        return remote(
            (dirb, imb, aimb, arb)[n].at[:, :, lanes(t)], lines.at[n, :, lines_of(s), :],
            l_send.at[n, d - 1], l_recv.at[n, d - 1], layer, t,
        )

    def spread_start(n):
        for d in range(1, nsplit):
            spread(n, d).start()
        for k in range(planes):
            lines[n, k, lines_of(s), :] = (dirb, imb, aimb, arb)[n][k, :, lanes(s)]

    def spread_finish(n):
        for d in range(1, nsplit):
            spread(n, d).wait_recv()
        for k in range(planes):
            flat[n, k] = lines[n, k].T

    def halo(n, i):
        values = (cols, dirb, imb)[n]
        src = (values.at[planes - 1], values.at[0], edges.at[n, 0], edges.at[n, 1])[i]
        dst = (zlow, zhigh, ylow, yhigh)[i].at[n]
        l, t = ((layer + 1, s), (layer - 1, s), (layer, s + 1), (layer, s - 1))[i]
        return remote(src, dst, h_send.at[n, i], h_recv.at[n, i], l, t)

    to_high, to_low = layer < nlayer - 1, layer > 0
    to_right, to_left = s < nsplit - 1, s > 0
    gives = (to_high, to_low, to_right, to_left)
    takes = (to_low, to_high, to_left, to_right)

    def halo_start(n):
        values = (cols, dirb, imb)[n]
        for i in range(2):
            pl.when(gives[i])(lambda i=i: halo(n, i).start())
        for k in range(planes):
            edges[n, 0, k : k + 1, :] = values[k, yb - 1 : yb, :]
            edges[n, 1, k : k + 1, :] = values[k, 0:1, :]
        for i in range(2, 4):
            pl.when(gives[i])(lambda i=i: halo(n, i).start())

    def halo_wait(n):
        for i in range(4):
            pl.when(takes[i])(lambda i=i: halo(n, i).wait_recv())

    row = lax.broadcasted_iota(jnp.int32, (yb, nx), 0)
    lane = lax.broadcasted_iota(jnp.int32, (yb, nx), 1)

    def apply_operator(n, result):
        values = (cols, dirb, imb)[n]
        for k in range(planes):
            v = values[k]
            below = values[k - 1] if k > 0 else zlow[n]
            above = values[k + 1] if k < planes - 1 else zhigh[n]
            x_low = jnp.where(lane == 0, 0.0, pltpu.roll(v, 1, 1))
            x_high = jnp.where(lane == nx - 1, 0.0, pltpu.roll(v, nx - 1, 1))
            y_low = jnp.where(row == 0, ylow[n, k : k + 1, :], pltpu.roll(v, 1, 0))
            y_high = jnp.where(row == yb - 1, yhigh[n, k : k + 1, :], pltpu.roll(v, yb - 1, 0))
            beside = (below + above) + (x_low + x_high) + (y_low + y_high)
            result[k] = (6.0 + dcols[k]) * v - beside

    def put_sum(i, a, b):
        total = a[0] * b[0]
        for k in range(1, planes):
            total = total + a[k] * b[k]
        total = jnp.sum(total, axis=0, keepdims=True)
        lane_sum = total[:, :width]
        for t in range(1, nsplit):
            lane_sum = lane_sum + total[:, t * width : (t + 1) * width]
        part[i : i + 1, :] = lane_sum

    def prepare():
        for d in range(1, nsplit):
            regroup(1, d).wait_recv()
        halo_wait(0)
        apply_operator(0, arb)
        spread_start(3)
        put_sum(0, cols, cols)
        put_sum(1, arb, cols)
        put_sum(2, arb, arb)

    def own_right(k):
        part = gbuf.at[k, rows(s, 0, width), :]
        return remote(part, part, g_send.at[0, k], g_recv.at[0, k], layer, right)

    def own_left(k):
        part = gbuf.at[k, rows(s, 0, width), :]
        return remote(part, part, g_send.at[1, k], g_recv.at[1, k], layer, left)

    def pass_right(k):
        part = gbuf.at[k, rows(left, 0, half), :]
        return remote(part, part, g_send.at[2, k], g_recv.at[2, k], layer, right)

    def pass_left(k):
        part = gbuf.at[k, rows(right, half, half), :]
        return remote(part, part, g_send.at[3, k], g_recv.at[3, k], layer, left)

    for d in range(1, nsplit):
        regroup(0, d).start()
    for k in range(min(2, planes)):
        own_right(k).start()
        own_left(k).start()

    def relay(k):
        own_right(k).wait_recv()
        pass_right(k).start()
        own_left(k).wait_recv()
        pass_left(k).start()
        if k + 2 < planes:
            own_right(k + 2).start()
            own_left(k + 2).start()
        if k == planes - 1:
            for d in range(1, nsplit):
                regroup(1, d).start()

    def absorb(k):
        pass_right(k).wait_recv()
        pass_left(k).wait_recv()
        full = gbuf[k]
        high, lowpart = split2(full)
        mats[k, 0] = high
        mats[k, 1] = lowpart
        if k == 0:
            for d in range(1, nsplit):
                regroup(0, d).wait_recv()
            halo_start(0)
            cvec[...] = mm(cols[0], high, lowpart)
            pf[...] = full
            qown[0] = high
            qown[1] = lowpart
        else:
            cvec[...] = mm(cols[k] + cvec[...], high, lowpart)
            pf[...] = mm(pf[...], high, lowpart)

    def absorb_up(k):
        if k > 0:
            qf[...] = mm(gbuf[k], qown[0], qown[1])
            store_pair(qown, qf[...])

    for k in range(planes):
        relay(k)
        if k > 0:
            absorb(k - 1)
            absorb_up(k - 1)
    absorb(planes - 1)

    give_p = remote(pf, pin, c_send.at[0], c_recv.at[0], other, s)
    give_q = remote(qf, qin, c_send.at[1], c_recv.at[1], other, s)
    give_c = remote(cvec, cin, c_send.at[2], c_recv.at[2], other, s)
    give_a = remote(amid, ain, c_send.at[3], c_recv.at[3], other, s)
    give_e = remote(evec, ein, c_send.at[4], c_recv.at[4], other, s)
    give_b = remote(bin_, bcore, c_send.at[5], c_recv.at[5], other, s)

    hosts = (npos - 1, 0)

    def row_layer(at):
        return 2 * (line * npos + at)

    def chunk(q):
        return pl.ds(q * cb, cb)

    def hand_matrix(way, step):
        part = xf.at[way], mbuf.at[step]
        if step == 1:
            part = tuple(ref.at[rows(s, 0, width), :] for ref in part)
        return remote(*part, x_send.at[way], x_recv.at[step], row_layer(hosts[way]), s)

    def hand_vector(way, step):
        return remote(
            vown.at[way], vbuf.at[step], v_send.at[way], v_recv.at[step],
            row_layer(hosts[way]), s,
        )

    def hand_input(way, step):
        return remote(
            inbuf.at[step], (ain, bin_)[way], i_send.at[step], i_recv.at[way],
            row_layer(step if way == 0 else npos - 1 - step), s,
        )

    def hand_on(way, q):
        return remote(
            zout.at[chunk(q), :], zin.at[chunk(q), :], z_send.at[q], z_recv.at[q],
            layer + (2 - 4 * way) * npos, s,
        )

    def ring(i):
        owner, start, size = ((s, 0, width), (s, 0, width), (left, 0, half), (right, half, half))[i]
        part = mbuf.at[1, rows(owner, start, size), :]
        return remote(
            part, part, y_send.at[i], y_recv.at[i], layer, (right, left, right, left)[i]
        )

    def for_step(way, do):
        for step in range(npos - 1):
            at = step if way == 0 else npos - 1 - step
            pl.when(pos == at)(functools.partial(do, step))

    def host_prepare(way):
        store_pair(pall if way == 0 else qall, xf[way])
        own = pall if way == 0 else qall
        hand_matrix(way, 1).wait_recv()
        ring(0).start()
        ring(1).start()
        hand_matrix(way, 0).wait_recv()
        store_pair(xpair.at[0], mbuf[0])
        ring(0).wait_recv()
        ring(2).start()
        ring(1).wait_recv()
        ring(3).start()
        ring(2).wait_recv()
        ring(3).wait_recv()
        store_pair(xpair.at[1], mbuf[1])
        store_pair(xrow, mm_ref(mbuf[0], xpair.at[1]))
        hand_matrix(way, 2).wait_recv()
        store_pair(xpair.at[2], mbuf[2])
        mbuf[2] = mm_pairs(xrow, xpair.at[2])
        store_pair(xrow, mm_ref(mbuf[2], own))

    def host_chain(way):
        own = pall if way == 0 else qall
        starts = line == 0 if way == 0 else line == nline - 1
        ends = line == nline - 1 if way == 0 else line == 0
        for step in range(npos - 1):
            hand_vector(way, step).wait_recv()
        total = vbuf[0]
        for step in range(1, npos - 1):
            total = vbuf[step] + mm_ref(total, xpair.at[step])
        zout[...] = vown[way] + mm_ref(total, own)

        @pl.when(starts)
        def _():
            inbuf[0] = jnp.zeros((yb, nx), F32)
            if nline > 1:
                for q in range(nchunk):
                    hand_on(way, q).start()

        @pl.when(jnp.logical_not(starts))
        def _():
            for q in range(nchunk):
                hand_on(way, q).wait_recv()

                @pl.when(jnp.logical_not(ends))
                def _():
                    zout[chunk(q), :] = zout[chunk(q), :] + mm_ref(zin[chunk(q), :], xrow)
                    hand_on(way, q).start()

            inbuf[0] = zin[...]

        state = inbuf[0]
        for step in range(npos - 1):
            hand_input(way, step).start()
            state = vbuf[step] + mm_ref(state, xpair.at[step])
            if step < npos - 2:
                inbuf[step + 1] = state
        (ain, bin_)[way][...] = state

    def host_finish(way):
        ends = line == nline - 1 if way == 0 else line == 0
        for step in range(npos - 1):
            hand_input(way, step).wait_send()
        for i in range(4):
            ring(i).wait_send()

        @pl.when(jnp.logical_not(ends))
        def _():
            for q in range(nchunk):
                hand_on(way, q).wait_send()

    @pl.when(core == 1)
    def _():
        give_c.start()
        give_p.start()

    absorb_up(planes - 1)

    def down_sweep(state):
        for k in range(planes):
            state = mm(cols[k] + state, mats[k, 0], mats[k, 1])
            low[k] = state

    def up_partial():
        state = low[planes - 1]
        for k in range(planes - 2, -1, -1):
            state = low[k] + mm(state, mats[k, 0], mats[k, 1])
        evec[...] = state

    def up_sweep(state):
        for k in range(planes - 1, -1, -1):
            state = low[k] + mm(state, mats[k, 0], mats[k, 1])
            dirb[k] = state

    @pl.when(core == 1)
    def _():
        give_q.start()
        prepare()
        give_a.wait_recv()
        down_sweep(ain[...])
        up_partial()
        give_e.start()
        give_b.wait_recv()
        up_sweep(bcore[...])
        give_c.wait_send()
        give_p.wait_send()
        give_q.wait_send()
        give_e.wait_send()

    @pl.when(core == 0)
    def _():
        store_pair(pown, pf[...])
        give_c.wait_recv()
        give_p.wait_recv()
        store_pair(pall, pin[...])
        vown[0] = mm_ref(cvec[...], pall) + cin[...]
        for_step(0, lambda step: hand_vector(0, step).start())
        xf[0] = mm_pairs(pown, pall)
        for_step(0, lambda step: hand_matrix(0, step).start())
        give_q.wait_recv()
        store_pair(q1, qin[...])
        xf[1] = mm_pairs(q1, qown)
        for_step(1, lambda step: hand_matrix(1, step).start())
        prepare()

        @pl.when(pos == hosts[0])
        def _():
            host_prepare(0)
            host_chain(0)

        @pl.when(pos == hosts[1])
        def _():
            host_prepare(1)

        for_step(0, lambda step: hand_input(0, step).wait_recv())
        amid[...] = cvec[...] + mm_ref(ain[...], pown)
        give_a.start()
        down_sweep(ain[...])
        up_partial()
        give_e.wait_recv()
        vown[1] = evec[...] + mm_ref(ein[...], qown)
        for_step(1, lambda step: hand_vector(1, step).start())

        @pl.when(pos == hosts[1])
        def _():
            host_chain(1)

        for_step(1, lambda step: hand_input(1, step).wait_recv())
        give_b.start()
        up_sweep(ein[...] + mm_ref(bin_[...], q1))
        give_a.wait_send()
        give_b.wait_send()
        for way in range(2):
            for_step(way, lambda step, way=way: hand_vector(way, step).wait_send())
            for_step(way, lambda step, way=way: hand_matrix(way, step).wait_send())
            pl.when(pos == hosts[way])(functools.partial(host_finish, way))

    halo_start(1)
    spread_start(0)
    halo_wait(1)
    apply_operator(1, imb)
    halo_start(2)
    spread_start(1)
    halo_wait(2)
    apply_operator(2, aimb)
    spread_start(2)
    put_sum(3, cols, imb)
    put_sum(4, arb, imb)
    put_sum(5, aimb, cols)
    put_sum(6, aimb, imb)
    put_sum(7, arb, aimb)
    put_sum(8, aimb, aimb)

    place = core * nsplit + s
    count = 2 * nsplit

    def near(d):
        at = lax.rem(place + d, count)
        return remote(
            group.at[place], group.at[place], n_send.at[d - 1], n_recv.at[d - 1],
            2 * chip + at // nsplit, lax.rem(at, nsplit),
        )

    def far(d):
        at = lax.rem(chip + d, nchip)
        return remote(
            whole.at[chip], whole.at[chip], w_send.at[d - 1], w_recv.at[d - 1],
            2 * at + core, s,
        )

    group[place] = part[...]
    for d in range(1, count):
        near(d).start()
    for n in (3, 0):
        spread_finish(n)
    for d in range(1, count):
        near(d).wait_recv()
    total = group[0]
    for i in range(1, count):
        total = total + group[i]
    whole[chip] = total
    for d in range(1, nchip):
        far(d).start()
    for n in (1, 2):
        spread_finish(n)
    for d in range(1, nchip):
        far(d).wait_recv()
    total = whole[0]
    for i in range(1, nchip):
        total = total + whole[i]
    sums = jnp.sum(total, axis=1, keepdims=True)
    rr, ar, aa, ri, ai, br, bi, ab, bb = [sums[i : i + 1, :] for i in range(9)]
    alpha = rr / ri
    cross = ar - alpha * (ai + br) + alpha * alpha * bi
    own = aa - 2.0 * alpha * ab + alpha * alpha * bb
    omega = cross / own
    for k in range(planes):
        middle = rhs_ref[k] - alpha * flat[1, k]
        sol_ref[k] = alpha * flat[0, k] + omega * middle
        res_ref[k] = middle - omega * (flat[3, k] - alpha * flat[2, k])

    for n in range(2):
        for d in range(1, nsplit):
            regroup(n, d).wait_send()
    for k in range(planes):
        own_right(k).wait_send()
        own_left(k).wait_send()
        pass_right(k).wait_send()
        pass_left(k).wait_send()
    for n in range(4):
        for d in range(1, nsplit):
            spread(n, d).wait_send()
    for n in range(3):
        for i in range(4):
            pl.when(gives[i])(lambda n=n, i=i: halo(n, i).wait_send())
    for d in range(1, count):
        near(d).wait_send()
    for d in range(1, nchip):
        far(d).wait_send()


def per_device(nlayer, nsplit, right_side, diagonal, inverses):
    planes, nx, width = inverses.shape
    ysize = right_side.shape[2]
    yb = ysize // nsplit
    nchip = nlayer // 2
    nchunk = 2
    nrow = 16
    vmem = pl.BlockSpec(memory_space=pltpu.VMEM)
    square = pltpu.VMEM((nx, nx), F32)
    pair = pltpu.VMEM((2, nx, nx), BF16)
    strip = pltpu.VMEM((yb, nx), F32)
    columns = pltpu.VMEM((planes, yb, nx), F32)
    block = pltpu.VMEM((planes, ysize, width), F32)
    dma = pltpu.SemaphoreType.DMA
    shape = jax.ShapeDtypeStruct((planes, width, ysize), F32)
    return pl.pallas_call(
        functools.partial(sweep_kernel, nlayer, nsplit, nchunk, nrow),
        out_shape=(shape, shape),
        in_specs=[vmem] * 3,
        out_specs=(vmem, vmem),
        scratch_shapes=[
            pltpu.VMEM((planes, nx, nx), F32),
            pltpu.VMEM((planes, 2, nx, nx), BF16),
            block, block,
            columns, columns, columns, columns, columns, columns, columns,
            square, square, pair, pair, pair, pair, pair, square, square,
            strip, strip, strip, strip, strip, strip, strip, strip, strip, strip,
            pltpu.VMEM((2, nx, nx), F32), pltpu.VMEM((3, nx, nx), F32),
            pltpu.VMEM((3, 2, nx, nx), BF16), pair,
            pltpu.VMEM((2, yb, nx), F32), pltpu.VMEM((3, yb, nx), F32),
            pltpu.VMEM((3, yb, nx), F32),
            pltpu.VMEM((3, yb, nx), F32), pltpu.VMEM((3, yb, nx), F32),
            pltpu.VMEM((3, 8, nx), F32), pltpu.VMEM((3, 8, nx), F32),
            pltpu.VMEM((3, 2, 8, nx), F32),
            pltpu.VMEM((4, planes, ysize, width), F32),
            pltpu.VMEM((4, planes, width, ysize), F32),
            pltpu.VMEM((nrow, width), F32),
            pltpu.VMEM((2 * nsplit, nrow, width), F32),
            pltpu.VMEM((nchip, nrow, width), F32),
            dma((2, nsplit - 1)), dma((2, nsplit - 1)),
            dma((4, planes)), dma((4, planes)),
            dma((6,)), dma((6,)),
            dma((2,)), dma((3,)), dma((2,)), dma((3,)), dma((3,)), dma((2,)),
            dma((nchunk,)), dma((nchunk,)), dma((4,)), dma((4,)),
            dma((3, 4)), dma((3, 4)),
            dma((4, nsplit - 1)), dma((4, nsplit - 1)),
            dma((2 * nsplit - 1,)), dma((2 * nsplit - 1,)),
            dma((nchip - 1,)), dma((nchip - 1,)),
        ],
        compiler_params=pltpu.CompilerParams(
            collective_id=0, has_side_effects=True, vmem_limit_bytes=56 * 1024 * 1024
        ),
        name="sweeps",
    )(right_side, diagonal, inverses)


def solution(mesh):
    spec = P("layer", "split", None)
    return jax.shard_map(
        functools.partial(per_device, mesh.shape["layer"], mesh.shape["split"]),
        mesh=mesh,
        in_specs=(spec, spec, P("layer", None, "split")),
        out_specs=(spec, spec),
        check_vma=False,
    )
```

```python
import functools

import jax
import jax.numpy as jnp
from jax import lax
from jax.experimental import pallas as pl
from jax.experimental.pallas import tpu as pltpu
from jax.sharding import PartitionSpec as P

MESH = pl.DeviceIdType.MESH
F32 = jnp.float32
BF16 = jnp.bfloat16


def split2(x):
    high = x.astype(BF16)
    return high, (x - high.astype(F32)).astype(BF16)


def mm(x, w_high, w_low):
    high, low = split2(x)
    dot = functools.partial(jnp.dot, preferred_element_type=F32)
    n = x.shape[0]
    if n > 128:
        return dot(high, w_high) + (dot(low, w_high) + dot(high, w_low))
    both = dot(jnp.concatenate([high, low], 0), w_high)
    return both[:n] + (both[n:] + dot(high, w_low))


def mm_ref(x, pair):
    return mm(x, pair[0], pair[1])


def mm_pairs(x, pair):
    dot = functools.partial(jnp.dot, preferred_element_type=F32)
    return dot(x[0], pair[0]) + (dot(x[1], pair[0]) + dot(x[0], pair[1]))


def store_pair(pair, x):
    high, low = split2(x)
    pair[0] = high
    pair[1] = low


def sweep_kernel(
    nlayer, nsplit, nchunk, nrow,
    rhs_ref, diag_ref, inv_ref, sol_ref, res_ref,
    gbuf, mats, rsend, dsend, cols, dcols, low, dirb, imb, aimb, arb,
    pf, qf, pown, qown, pall, qall, q1, pin, qin,
    cvec, cin, ain, amid, evec, ein, bin_, bcore, zin, zout,
    xf, mbuf, xpair, xrow, vown, vbuf, inbuf,
    prefix, rf, rin, rpair, azero, ezero, ein0,
    zlow, zhigh, ylow, yhigh, edges, lines, flat, part, group, whole,
    rs_send, rs_recv, g_send, g_recv, c_send, c_recv,
    x_send, x_recv, v_send, v_recv, i_send, i_recv, z_send, z_recv, y_send, y_recv,
    h_send, h_recv, l_send, l_recv, n_send, n_recv, w_send, w_recv,
):
    planes, nx, width = inv_ref.shape
    ysize = rhs_ref.shape[2]
    yb = ysize // nsplit
    cb = yb // nchunk
    half = width // 2
    layer = lax.axis_index("layer")
    s = lax.axis_index("split")
    core = lax.rem(layer, 2)
    chip = layer // 2
    nchip = nlayer // 2
    right = lax.rem(s + 1, nsplit)
    left = lax.rem(s + nsplit - 1, nsplit)
    other = layer + 1 - 2 * core
    npos = 4
    pos, line = lax.rem(chip, npos), chip // npos
    nline = nchip // npos

    def rows(owner, start, size):
        return pl.ds(pl.multiple_of(owner * width + start, half), size)

    def lanes(t):
        return pl.ds(pl.multiple_of(t * width, width), width)

    def lines_of(t):
        return pl.ds(pl.multiple_of(t * yb, yb), yb)

    for empty in (zlow, zhigh, ylow, yhigh, edges, part):
        empty[...] = jnp.zeros_like(empty)

    barrier = pltpu.get_barrier_semaphore()

    def greet(l, t):
        pl.semaphore_signal(barrier, inc=1, device_id=(l, t), device_id_type=MESH)

    for d in range(1, nsplit):
        greet(layer, lax.rem(s + d, nsplit))
    for d in range(nsplit):
        greet(other, lax.rem(s + d, nsplit))
    for d in range(1, nchip):
        greet(2 * lax.rem(chip + d, nchip) + core, s)
    side = layer - 1 + 2 * core
    inner = jnp.logical_and(side >= 0, side < nlayer)

    @pl.when(inner)
    def _():
        greet(side, s)

    for k in range(planes):
        gbuf[k, rows(s, 0, width), :] = inv_ref[k].T
    for source, sent, mine in ((rhs_ref, rsend, cols), (diag_ref, dsend, dcols)):
        for k in range(planes):
            sent[k] = source[k].T
        for k in range(planes):
            mine[k, :, lanes(s)] = sent[k, lines_of(s), :]

    pl.semaphore_wait(barrier, 2 * nsplit - 1 + nchip - 1 + jnp.where(inner, 1, 0))

    def remote(src, dst, send, recv, l, t):
        return pltpu.make_async_remote_copy(
            src_ref=src, dst_ref=dst, send_sem=send, recv_sem=recv,
            device_id=(l, t), device_id_type=MESH,
        )

    def regroup(n, d):
        t = lax.rem(s + d, nsplit)
        sent, mine = ((rsend, cols), (dsend, dcols))[n]
        return remote(
            sent.at[:, lines_of(t), :], mine.at[:, :, lanes(s)],
            rs_send.at[n, d - 1], rs_recv.at[n, d - 1], layer, t,
        )

    def spread(n, d):
        t = lax.rem(s + d, nsplit)
        return remote(
            (dirb, imb, aimb, arb)[n].at[:, :, lanes(t)], lines.at[n, :, lines_of(s), :],
            l_send.at[n, d - 1], l_recv.at[n, d - 1], layer, t,
        )

    def spread_start(n):
        for d in range(1, nsplit):
            spread(n, d).start()
        for k in range(planes):
            lines[n, k, lines_of(s), :] = (dirb, imb, aimb, arb)[n][k, :, lanes(s)]

    def spread_finish(n):
        for d in range(1, nsplit):
            spread(n, d).wait_recv()
        for k in range(planes):
            flat[n, k] = lines[n, k].T

    def halo(n, i):
        values = (cols, dirb, imb)[n]
        src = (values.at[planes - 1], values.at[0], edges.at[n, 0], edges.at[n, 1])[i]
        dst = (zlow, zhigh, ylow, yhigh)[i].at[n]
        l, t = ((layer + 1, s), (layer - 1, s), (layer, s + 1), (layer, s - 1))[i]
        return remote(src, dst, h_send.at[n, i], h_recv.at[n, i], l, t)

    to_high, to_low = layer < nlayer - 1, layer > 0
    to_right, to_left = s < nsplit - 1, s > 0
    gives = (to_high, to_low, to_right, to_left)
    takes = (to_low, to_high, to_left, to_right)

    def halo_start(n):
        values = (cols, dirb, imb)[n]
        for i in range(2):
            pl.when(gives[i])(lambda i=i: halo(n, i).start())
        for k in range(planes):
            edges[n, 0, k : k + 1, :] = values[k, yb - 1 : yb, :]
            edges[n, 1, k : k + 1, :] = values[k, 0:1, :]
        for i in range(2, 4):
            pl.when(gives[i])(lambda i=i: halo(n, i).start())

    def halo_wait(n):
        for i in range(4):
            pl.when(takes[i])(lambda i=i: halo(n, i).wait_recv())

    row = lax.broadcasted_iota(jnp.int32, (yb, nx), 0)
    lane = lax.broadcasted_iota(jnp.int32, (yb, nx), 1)

    def apply_operator(n, result):
        values = (cols, dirb, imb)[n]
        for k in range(planes):
            v = values[k]
            below = values[k - 1] if k > 0 else zlow[n]
            above = values[k + 1] if k < planes - 1 else zhigh[n]
            x_low = jnp.where(lane == 0, 0.0, pltpu.roll(v, 1, 1))
            x_high = jnp.where(lane == nx - 1, 0.0, pltpu.roll(v, nx - 1, 1))
            y_low = jnp.where(row == 0, ylow[n, k : k + 1, :], pltpu.roll(v, 1, 0))
            y_high = jnp.where(row == yb - 1, yhigh[n, k : k + 1, :], pltpu.roll(v, yb - 1, 0))
            beside = (below + above) + (x_low + x_high) + (y_low + y_high)
            result[k] = (6.0 + dcols[k]) * v - beside

    def put_sum(i, a, b):
        total = a[0] * b[0]
        for k in range(1, planes):
            total = total + a[k] * b[k]
        total = jnp.sum(total, axis=0, keepdims=True)
        lane_sum = total[:, :width]
        for t in range(1, nsplit):
            lane_sum = lane_sum + total[:, t * width : (t + 1) * width]
        part[i : i + 1, :] = lane_sum

    def prepare():
        for d in range(1, nsplit):
            regroup(1, d).wait_recv()
        halo_wait(0)
        apply_operator(0, arb)
        spread_start(3)
        put_sum(0, cols, cols)
        put_sum(1, arb, cols)
        put_sum(2, arb, arb)

    def own_right(k):
        part = gbuf.at[k, rows(s, 0, width), :]
        return remote(part, part, g_send.at[0, k], g_recv.at[0, k], layer, right)

    def own_left(k):
        part = gbuf.at[k, rows(s, 0, width), :]
        return remote(part, part, g_send.at[1, k], g_recv.at[1, k], layer, left)

    def pass_right(k):
        part = gbuf.at[k, rows(left, 0, half), :]
        return remote(part, part, g_send.at[2, k], g_recv.at[2, k], layer, right)

    def pass_left(k):
        part = gbuf.at[k, rows(right, half, half), :]
        return remote(part, part, g_send.at[3, k], g_recv.at[3, k], layer, left)

    for d in range(1, nsplit):
        regroup(0, d).start()
    for k in range(min(2, planes)):
        own_right(k).start()
        own_left(k).start()

    def relay(k):
        own_right(k).wait_recv()
        pass_right(k).start()
        own_left(k).wait_recv()
        pass_left(k).start()
        if k + 2 < planes:
            own_right(k + 2).start()
            own_left(k + 2).start()
        if k == planes - 1:
            for d in range(1, nsplit):
                regroup(1, d).start()

    def absorb(k):
        pass_right(k).wait_recv()
        pass_left(k).wait_recv()
        full = gbuf[k]
        high, lowpart = split2(full)
        mats[k, 0] = high
        mats[k, 1] = lowpart
        if k == 0:
            for d in range(1, nsplit):
                regroup(0, d).wait_recv()
            halo_start(0)
            cvec[...] = mm(cols[0], high, lowpart)
            pf[...] = full
            qown[0] = high
            qown[1] = lowpart
        else:
            cvec[...] = mm(cols[k] + cvec[...], high, lowpart)
            prefix[k - 1] = pf[...]
            pf[...] = mm(pf[...], high, lowpart)

    def absorb_up(k):
        if k > 0:
            qf[...] = mm(gbuf[k], qown[0], qown[1])
            store_pair(qown, qf[...])

    for k in range(planes):
        relay(k)
        if k > 0:
            absorb(k - 1)
            absorb_up(k - 1)
    absorb(planes - 1)

    give_p = remote(pf, pin, c_send.at[0], c_recv.at[0], other, s)
    give_q = remote(qf, qin, c_send.at[1], c_recv.at[1], other, s)
    give_c = remote(cvec, cin, c_send.at[2], c_recv.at[2], other, s)
    give_a = remote(amid, ain, c_send.at[3], c_recv.at[3], other, s)
    give_e = remote(evec, ein, c_send.at[4], c_recv.at[4], other, s)
    give_b = remote(bin_, bcore, c_send.at[5], c_recv.at[5], other, s)
    give_r = remote(rf, rin, c_send.at[6], c_recv.at[6], other, s)
    give_a0 = remote(cvec, azero, c_send.at[7], c_recv.at[7], other, s)
    give_e0 = remote(ezero, ein0, c_send.at[8], c_recv.at[8], other, s)

    hosts = (npos - 1, 0)

    def row_layer(at):
        return 2 * (line * npos + at)

    def chunk(q):
        return pl.ds(q * cb, cb)

    def shared(step):
        return (0, width) if step == 1 else (nx // 2, width // 2)

    def hand_share(way, step):
        base, size = shared(step)
        part = pl.ds(pl.multiple_of(base + s * size, size), size)
        return remote(
            xf.at[way, part, :], mbuf.at[step, part, :],
            x_send.at[way, 0], x_recv.at[step, 0], row_layer(hosts[way]), s,
        )

    def hand_whole(way, step):
        part = pl.ds(0, nx // 2)
        return remote(
            xf.at[way, part, :], mbuf.at[step, part, :],
            x_send.at[way, 1], x_recv.at[step, 1], row_layer(hosts[way]), s,
        )

    def hand_wholes(way, do):
        for step in (0, 2):
            at = step if way == 0 else npos - 1 - step
            pl.when(pos == at)(functools.partial(do, step))

    def hand_vector(way, step):
        return remote(
            vown.at[way], vbuf.at[step], v_send.at[way], v_recv.at[step],
            row_layer(hosts[way]), s,
        )

    def hand_input(way, step):
        return remote(
            inbuf.at[step], (ain, bin_)[way], i_send.at[step], i_recv.at[way],
            row_layer(step if way == 0 else npos - 1 - step), s,
        )

    def hand_on(way, q):
        return remote(
            zout.at[chunk(q), :], zin.at[chunk(q), :], z_send.at[q], z_recv.at[q],
            layer + (2 - 4 * way) * npos, s,
        )

    def ring(step, i):
        base, size = shared(step)
        owner, start, length = (
            (s, 0, size), (s, 0, size), (left, 0, size // 2), (right, size // 2, size // 2)
        )[i]
        rows_at = pl.multiple_of(base + owner * size + start, size // 2)
        part = mbuf.at[step, pl.ds(rows_at, length), :]
        return remote(
            part, part, y_send.at[step, i], y_recv.at[step, i], layer,
            (right, left, right, left)[i],
        )

    def for_step(way, do):
        for step in range(npos - 1):
            at = step if way == 0 else npos - 1 - step
            pl.when(pos == at)(functools.partial(do, step))

    def host_prepare(way):
        own = pall if way == 0 else qall
        store_pair(own, xf[way])
        order = (1, 0, 2)
        for step in order:
            hand_share(way, step).wait_recv()
            ring(step, 0).start()
            ring(step, 1).start()
        for step in order:
            ring(step, 0).wait_recv()
            ring(step, 2).start()
            ring(step, 1).wait_recv()
            ring(step, 3).start()
        upper, lower = pl.ds(0, nx // 2), pl.ds(nx // 2, nx // 2)
        for step in order:
            ring(step, 2).wait_recv()
            ring(step, 3).wait_recv()
            if step == 1:
                store_pair(xpair.at[1], mbuf[1])
            if step == 0:
                pf[lower, :] = mm_ref(mbuf[0, lower, :], xpair.at[1])
            if step == 2:
                pin[lower, :] = mm_ref(mbuf[2, lower, :], own)
        hand_whole(way, 0).wait_recv()
        pf[upper, :] = mm_ref(mbuf[0, upper, :], xpair.at[1])
        hand_whole(way, 2).wait_recv()
        pin[upper, :] = mm_ref(mbuf[2, upper, :], own)
        store_pair(xrow, pin[...])
        pf[...] = mm_ref(pf[...], xrow)
        store_pair(xrow, pf[...])
        for step in (0, 2):
            store_pair(xpair.at[step], mbuf[step])

    def host_chain(way):
        own = pall if way == 0 else qall
        starts = line == 0 if way == 0 else line == nline - 1
        ends = line == nline - 1 if way == 0 else line == 0
        for step in range(npos - 1):
            hand_vector(way, step).wait_recv()
        total = vbuf[0]
        for step in range(1, npos - 1):
            total = vbuf[step] + mm_ref(total, xpair.at[step])
        zout[...] = vown[way] + mm_ref(total, own)

        @pl.when(starts)
        def _():
            inbuf[0] = jnp.zeros((yb, nx), F32)
            if nline > 1:
                for q in range(nchunk):
                    hand_on(way, q).start()

        @pl.when(jnp.logical_not(starts))
        def _():
            for q in range(nchunk):
                hand_on(way, q).wait_recv()

                @pl.when(jnp.logical_not(ends))
                def _():
                    zout[chunk(q), :] = zout[chunk(q), :] + mm_ref(zin[chunk(q), :], xrow)
                    hand_on(way, q).start()

            inbuf[0] = zin[...]

        state = inbuf[0]
        for step in range(npos - 1):
            hand_input(way, step).start()
            state = vbuf[step] + mm_ref(state, xpair.at[step])
            if step < npos - 2:
                inbuf[step + 1] = state
        (ain, bin_)[way][...] = state

    def host_finish(way):
        ends = line == nline - 1 if way == 0 else line == 0
        for step in range(npos - 1):
            hand_input(way, step).wait_send()
        for step in range(npos - 1):
            for i in range(4):
                ring(step, i).wait_send()

        @pl.when(jnp.logical_not(ends))
        def _():
            for q in range(nchunk):
                hand_on(way, q).wait_send()

    @pl.when(core == 1)
    def _():
        give_c.start()
        give_p.start()

    absorb_up(planes - 1)

    def down_sweep(state):
        for k in range(planes):
            state = mm(cols[k] + state, mats[k, 0], mats[k, 1])
            low[k] = state

    def up_partial(result):
        state = low[planes - 1]
        for k in range(planes - 2, -1, -1):
            state = low[k] + mm(state, mats[k, 0], mats[k, 1])
        result[...] = state

    def response():
        rf[...] = prefix[planes - 2] + mm(pf[...], mats[planes - 2, 0], mats[planes - 2, 1])
        for k in range(planes - 3, -1, -1):
            rf[...] = prefix[k] + mm(rf[...], mats[k, 0], mats[k, 1])

    def up_sweep(state):
        for k in range(planes - 1, -1, -1):
            state = low[k] + mm(state, mats[k, 0], mats[k, 1])
            dirb[k] = state

    @pl.when(core == 1)
    def _():
        give_q.start()
        response()
        give_r.start()
        give_a0.wait_recv()
        down_sweep(azero[...])
        up_partial(ezero)
        give_e0.start()
        prepare()
        give_a.wait_recv()
        down_sweep(ain[...])
        up_partial(evec)
        give_e.start()
        give_b.wait_recv()
        up_sweep(bcore[...])
        for give in (give_c, give_p, give_q, give_r, give_e0, give_e):
            give.wait_send()

    @pl.when(core == 0)
    def _():
        give_a0.start()
        store_pair(pown, pf[...])
        give_c.wait_recv()
        give_p.wait_recv()
        store_pair(pall, pin[...])
        vown[0] = mm_ref(cvec[...], pall) + cin[...]
        for_step(0, lambda step: hand_vector(0, step).start())
        xf[0] = mm_pairs(pown, pall)
        for_step(0, lambda step: hand_share(0, step).start())
        give_q.wait_recv()
        store_pair(q1, qin[...])
        xf[1] = mm_pairs(q1, qown)
        for_step(1, lambda step: hand_share(1, step).start())
        hand_wholes(0, lambda step: hand_whole(0, step).start())
        hand_wholes(1, lambda step: hand_whole(1, step).start())
        prepare()

        @pl.when(pos == hosts[0])
        def _():
            give_r.wait_recv()
            give_e0.wait_recv()
            host_prepare(0)
            host_chain(0)

        @pl.when(pos != hosts[0])
        def _():
            response()
            give_r.wait_recv()
            store_pair(rpair, rin[...])
            rin[...] = mm_ref(pf[...], rpair)
            rf[...] = rf[...] + mm_ref(rin[...], qown)
            store_pair(rpair, rf[...])
            down_sweep(jnp.zeros((yb, nx), F32))
            up_partial(ezero)
            give_e0.wait_recv()
            ezero[...] = ezero[...] + mm_ref(ein0[...], qown)

        @pl.when(pos == hosts[1])
        def _():
            host_prepare(1)

        for_step(0, lambda step: hand_input(0, step).wait_recv())

        @pl.when(pos != hosts[0])
        def _():
            vown[1] = ezero[...] + mm_ref(ain[...], rpair)
            for_step(1, lambda step: hand_vector(1, step).start())

        amid[...] = cvec[...] + mm_ref(ain[...], pown)
        give_a.start()
        down_sweep(ain[...])

        @pl.when(pos == hosts[0])
        def _():
            up_partial(evec)
            give_e.wait_recv()
            vown[1] = evec[...] + mm_ref(ein[...], qown)
            hand_vector(1, 0).start()

        @pl.when(pos == hosts[1])
        def _():
            host_chain(1)

        @pl.when(pos != hosts[0])
        def _():
            give_e.wait_recv()

        for_step(1, lambda step: hand_input(1, step).wait_recv())
        give_b.start()
        up_sweep(ein[...] + mm_ref(bin_[...], q1))
        give_a0.wait_send()
        give_a.wait_send()
        give_b.wait_send()
        for way in range(2):
            for_step(way, lambda step, way=way: hand_vector(way, step).wait_send())
            for_step(way, lambda step, way=way: hand_share(way, step).wait_send())
            hand_wholes(way, lambda step, way=way: hand_whole(way, step).wait_send())
            pl.when(pos == hosts[way])(functools.partial(host_finish, way))

    halo_start(1)
    spread_start(0)
    halo_wait(1)
    apply_operator(1, imb)
    halo_start(2)
    spread_start(1)
    halo_wait(2)
    apply_operator(2, aimb)
    spread_start(2)
    put_sum(3, cols, imb)
    put_sum(4, arb, imb)
    put_sum(5, aimb, cols)
    put_sum(6, aimb, imb)
    put_sum(7, arb, aimb)
    put_sum(8, aimb, aimb)

    place = core * nsplit + s
    count = 2 * nsplit

    def near(d):
        at = lax.rem(place + d, count)
        return remote(
            group.at[place], group.at[place], n_send.at[d - 1], n_recv.at[d - 1],
            2 * chip + at // nsplit, lax.rem(at, nsplit),
        )

    def far(d):
        at = lax.rem(chip + d, nchip)
        return remote(
            whole.at[chip], whole.at[chip], w_send.at[d - 1], w_recv.at[d - 1],
            2 * at + core, s,
        )

    group[place] = part[...]
    for d in range(1, count):
        near(d).start()
    for n in (3, 0):
        spread_finish(n)
    for d in range(1, count):
        near(d).wait_recv()
    total = group[0]
    for i in range(1, count):
        total = total + group[i]
    whole[chip] = total
    for d in range(1, nchip):
        far(d).start()
    for n in (1, 2):
        spread_finish(n)
    for d in range(1, nchip):
        far(d).wait_recv()
    total = whole[0]
    for i in range(1, nchip):
        total = total + whole[i]
    sums = jnp.sum(total, axis=1, keepdims=True)
    rr, ar, aa, ri, ai, br, bi, ab, bb = [sums[i : i + 1, :] for i in range(9)]
    alpha = rr / ri
    cross = ar - alpha * (ai + br) + alpha * alpha * bi
    own = aa - 2.0 * alpha * ab + alpha * alpha * bb
    omega = cross / own
    for k in range(planes):
        middle = rhs_ref[k] - alpha * flat[1, k]
        sol_ref[k] = alpha * flat[0, k] + omega * middle
        res_ref[k] = middle - omega * (flat[3, k] - alpha * flat[2, k])

    for n in range(2):
        for d in range(1, nsplit):
            regroup(n, d).wait_send()
    for k in range(planes):
        own_right(k).wait_send()
        own_left(k).wait_send()
        pass_right(k).wait_send()
        pass_left(k).wait_send()
    for n in range(4):
        for d in range(1, nsplit):
            spread(n, d).wait_send()
    for n in range(3):
        for i in range(4):
            pl.when(gives[i])(lambda n=n, i=i: halo(n, i).wait_send())
    for d in range(1, count):
        near(d).wait_send()
    for d in range(1, nchip):
        far(d).wait_send()


def per_device(nlayer, nsplit, right_side, diagonal, inverses):
    planes, nx, width = inverses.shape
    ysize = right_side.shape[2]
    yb = ysize // nsplit
    nchip = nlayer // 2
    nchunk = 2
    nrow = 16
    vmem = pl.BlockSpec(memory_space=pltpu.VMEM)
    square = pltpu.VMEM((nx, nx), F32)
    pair = pltpu.VMEM((2, nx, nx), BF16)
    strip = pltpu.VMEM((yb, nx), F32)
    columns = pltpu.VMEM((planes, yb, nx), F32)
    block = pltpu.VMEM((planes, ysize, width), F32)
    dma = pltpu.SemaphoreType.DMA
    shape = jax.ShapeDtypeStruct((planes, width, ysize), F32)
    return pl.pallas_call(
        functools.partial(sweep_kernel, nlayer, nsplit, nchunk, nrow),
        out_shape=(shape, shape),
        in_specs=[vmem] * 3,
        out_specs=(vmem, vmem),
        scratch_shapes=[
            pltpu.VMEM((planes, nx, nx), F32),
            pltpu.VMEM((planes, 2, nx, nx), BF16),
            block, block,
            columns, columns, columns, columns, columns, columns, columns,
            square, square, pair, pair, pair, pair, pair, square, square,
            strip, strip, strip, strip, strip, strip, strip, strip, strip, strip,
            pltpu.VMEM((2, nx, nx), F32), pltpu.VMEM((3, nx, nx), F32),
            pltpu.VMEM((3, 2, nx, nx), BF16), pair,
            pltpu.VMEM((2, yb, nx), F32), pltpu.VMEM((3, yb, nx), F32),
            pltpu.VMEM((3, yb, nx), F32),
            pltpu.VMEM((planes - 1, nx, nx), F32), square, square, pair, strip, strip, strip,
            pltpu.VMEM((3, yb, nx), F32), pltpu.VMEM((3, yb, nx), F32),
            pltpu.VMEM((3, 8, nx), F32), pltpu.VMEM((3, 8, nx), F32),
            pltpu.VMEM((3, 2, 8, nx), F32),
            pltpu.VMEM((4, planes, ysize, width), F32),
            pltpu.VMEM((4, planes, width, ysize), F32),
            pltpu.VMEM((nrow, width), F32),
            pltpu.VMEM((2 * nsplit, nrow, width), F32),
            pltpu.VMEM((nchip, nrow, width), F32),
            dma((2, nsplit - 1)), dma((2, nsplit - 1)),
            dma((4, planes)), dma((4, planes)),
            dma((9,)), dma((9,)),
            dma((2, 2)), dma((3, 2)), dma((2,)), dma((3,)), dma((3,)), dma((2,)),
            dma((nchunk,)), dma((nchunk,)), dma((3, 4)), dma((3, 4)),
            dma((3, 4)), dma((3, 4)),
            dma((4, nsplit - 1)), dma((4, nsplit - 1)),
            dma((2 * nsplit - 1,)), dma((2 * nsplit - 1,)),
            dma((nchip - 1,)), dma((nchip - 1,)),
        ],
        compiler_params=pltpu.CompilerParams(
            collective_id=0, has_side_effects=True, vmem_limit_bytes=56 * 1024 * 1024
        ),
        name="sweeps",
    )(right_side, diagonal, inverses)


def solution(mesh):
    spec = P("layer", "split", None)
    return jax.shard_map(
        functools.partial(per_device, mesh.shape["layer"], mesh.shape["split"]),
        mesh=mesh,
        in_specs=(spec, spec, P("layer", None, "split")),
        out_specs=(spec, spec),
        check_vma=False,
    )
```

```python
import functools

import jax
import jax.numpy as jnp
from jax import lax
from jax.experimental import pallas as pl
from jax.experimental.pallas import tpu as pltpu
from jax.sharding import PartitionSpec as P

MESH = pl.DeviceIdType.MESH
F32 = jnp.float32
BF16 = jnp.bfloat16


def split2(x):
    high = x.astype(BF16)
    return high, (x - high.astype(F32)).astype(BF16)


def mm(x, w_high, w_low):
    high, low = split2(x)
    dot = functools.partial(jnp.dot, preferred_element_type=F32)
    n = x.shape[0]
    if n > 128:
        return dot(high, w_high) + (dot(low, w_high) + dot(high, w_low))
    both = dot(jnp.concatenate([high, low], 0), w_high)
    return both[:n] + (both[n:] + dot(high, w_low))


def mm_ref(x, pair):
    return mm(x, pair[0], pair[1])


def mm_pairs(x, pair):
    dot = functools.partial(jnp.dot, preferred_element_type=F32)
    return dot(x[0], pair[0]) + (dot(x[1], pair[0]) + dot(x[0], pair[1]))


def store_pair(pair, x):
    high, low = split2(x)
    pair[0] = high
    pair[1] = low


def sweep_kernel(
    nlayer, nsplit, nchunk, nrow,
    rhs_ref, diag_ref, inv_ref, sol_ref, res_ref,
    gbuf, mats, rsend, dsend, cols, dcols, low, dirb, imb, aimb, arb,
    pf, qf, pown, qown, pall, qall, q1, pin, qin,
    cvec, cin, ain, amid, evec, ein, bin_, bcore, zin, zout,
    xf, mbuf, xpair, xrow, vown, vbuf, inbuf,
    prefix, rf, rin, rpair, azero, ezero, ein0,
    zlow, zhigh, ylow, yhigh, edges, lines, flat, part, group, whole,
    rs_send, rs_recv, g_send, g_recv, c_send, c_recv,
    x_send, x_recv, v_send, v_recv, i_send, i_recv, z_send, z_recv, y_send, y_recv,
    h_send, h_recv, l_send, l_recv, n_send, n_recv, w_send, w_recv,
):
    planes, nx, width = inv_ref.shape
    ysize = rhs_ref.shape[2]
    yb = ysize // nsplit
    cb = yb // nchunk
    half = width // 2
    layer = lax.axis_index("layer")
    s = lax.axis_index("split")
    core = lax.rem(layer, 2)
    chip = layer // 2
    nchip = nlayer // 2
    right = lax.rem(s + 1, nsplit)
    left = lax.rem(s + nsplit - 1, nsplit)
    other = layer + 1 - 2 * core
    npos = 4
    pos, line = lax.rem(chip, npos), chip // npos
    nline = nchip // npos

    def rows(owner, start, size):
        return pl.ds(pl.multiple_of(owner * width + start, half), size)

    def lanes(t):
        return pl.ds(pl.multiple_of(t * width, width), width)

    def lines_of(t):
        return pl.ds(pl.multiple_of(t * yb, yb), yb)

    for empty in (zlow, zhigh, ylow, yhigh, edges, part):
        empty[...] = jnp.zeros_like(empty)

    barrier = pltpu.get_barrier_semaphore()

    def greet(l, t):
        pl.semaphore_signal(barrier, inc=1, device_id=(l, t), device_id_type=MESH)

    for d in range(1, nsplit):
        greet(layer, lax.rem(s + d, nsplit))
    for d in range(nsplit):
        greet(other, lax.rem(s + d, nsplit))
    for d in range(1, nchip):
        greet(2 * lax.rem(chip + d, nchip) + core, s)
    side = layer - 1 + 2 * core
    inner = jnp.logical_and(side >= 0, side < nlayer)

    @pl.when(inner)
    def _():
        greet(side, s)

    for k in range(planes):
        gbuf[k, rows(s, 0, width), :] = inv_ref[k].T
    for source, sent, mine in ((rhs_ref, rsend, cols), (diag_ref, dsend, dcols)):
        for k in range(planes):
            sent[k] = source[k].T
        for k in range(planes):
            mine[k, :, lanes(s)] = sent[k, lines_of(s), :]

    pl.semaphore_wait(barrier, 2 * nsplit - 1 + nchip - 1 + jnp.where(inner, 1, 0))

    def remote(src, dst, send, recv, l, t):
        return pltpu.make_async_remote_copy(
            src_ref=src, dst_ref=dst, send_sem=send, recv_sem=recv,
            device_id=(l, t), device_id_type=MESH,
        )

    def regroup(n, d):
        t = lax.rem(s + d, nsplit)
        sent, mine = ((rsend, cols), (dsend, dcols))[n]
        return remote(
            sent.at[:, lines_of(t), :], mine.at[:, :, lanes(s)],
            rs_send.at[n, d - 1], rs_recv.at[n, d - 1], layer, t,
        )

    def spread(n, d):
        t = lax.rem(s + d, nsplit)
        return remote(
            (dirb, imb, aimb, arb)[n].at[:, :, lanes(t)], lines.at[n, :, lines_of(s), :],
            l_send.at[n, d - 1], l_recv.at[n, d - 1], layer, t,
        )

    def spread_start(n, distances=None):
        for d in range(1, nsplit) if distances is None else distances:
            spread(n, d).start()
        if distances is not None and 1 not in distances:
            return
        for k in range(planes):
            lines[n, k, lines_of(s), :] = (dirb, imb, aimb, arb)[n][k, :, lanes(s)]

    def spread_finish(n):
        for d in range(1, nsplit):
            spread(n, d).wait_recv()
        for k in range(planes):
            flat[n, k] = lines[n, k].T

    def halo(n, i):
        values = (cols, dirb, imb)[n]
        src = (values.at[planes - 1], values.at[0], edges.at[n, 0], edges.at[n, 1])[i]
        dst = (zlow, zhigh, ylow, yhigh)[i].at[n]
        l, t = ((layer + 1, s), (layer - 1, s), (layer, s + 1), (layer, s - 1))[i]
        return remote(src, dst, h_send.at[n, i], h_recv.at[n, i], l, t)

    to_high, to_low = layer < nlayer - 1, layer > 0
    to_right, to_left = s < nsplit - 1, s > 0
    gives = (to_high, to_low, to_right, to_left)
    takes = (to_low, to_high, to_left, to_right)

    def halo_start(n):
        values = (cols, dirb, imb)[n]
        for i in range(2):
            pl.when(gives[i])(lambda i=i: halo(n, i).start())
        for k in range(planes):
            edges[n, 0, k : k + 1, :] = values[k, yb - 1 : yb, :]
            edges[n, 1, k : k + 1, :] = values[k, 0:1, :]
        for i in range(2, 4):
            pl.when(gives[i])(lambda i=i: halo(n, i).start())

    def halo_wait(n):
        for i in range(4):
            pl.when(takes[i])(lambda i=i: halo(n, i).wait_recv())

    row = lax.broadcasted_iota(jnp.int32, (yb, nx), 0)
    lane = lax.broadcasted_iota(jnp.int32, (yb, nx), 1)

    def apply_operator(n, result):
        values = (cols, dirb, imb)[n]
        for k in range(planes):
            v = values[k]
            below = values[k - 1] if k > 0 else zlow[n]
            above = values[k + 1] if k < planes - 1 else zhigh[n]
            x_low = jnp.where(lane == 0, 0.0, pltpu.roll(v, 1, 1))
            x_high = jnp.where(lane == nx - 1, 0.0, pltpu.roll(v, nx - 1, 1))
            y_low = jnp.where(row == 0, ylow[n, k : k + 1, :], pltpu.roll(v, 1, 0))
            y_high = jnp.where(row == yb - 1, yhigh[n, k : k + 1, :], pltpu.roll(v, yb - 1, 0))
            beside = (below + above) + (x_low + x_high) + (y_low + y_high)
            result[k] = (6.0 + dcols[k]) * v - beside

    def put_sum(i, a, b):
        total = a[0] * b[0]
        for k in range(1, planes):
            total = total + a[k] * b[k]
        total = jnp.sum(total, axis=0, keepdims=True)
        lane_sum = total[:, :width]
        for t in range(1, nsplit):
            lane_sum = lane_sum + total[:, t * width : (t + 1) * width]
        part[i : i + 1, :] = lane_sum

    def prepare():
        for d in range(1, nsplit):
            regroup(1, d).wait_recv()
        halo_wait(0)
        apply_operator(0, arb)
        spread_start(3)
        put_sum(0, cols, cols)
        put_sum(1, arb, cols)
        put_sum(2, arb, arb)

    def own_right(k):
        part = gbuf.at[k, rows(s, 0, width), :]
        return remote(part, part, g_send.at[0, k], g_recv.at[0, k], layer, right)

    def own_left(k):
        part = gbuf.at[k, rows(s, 0, width), :]
        return remote(part, part, g_send.at[1, k], g_recv.at[1, k], layer, left)

    def pass_right(k):
        part = gbuf.at[k, rows(left, 0, half), :]
        return remote(part, part, g_send.at[2, k], g_recv.at[2, k], layer, right)

    def pass_left(k):
        part = gbuf.at[k, rows(right, half, half), :]
        return remote(part, part, g_send.at[3, k], g_recv.at[3, k], layer, left)

    for d in range(1, nsplit):
        regroup(0, d).start()
    for k in range(min(2, planes)):
        own_right(k).start()
        own_left(k).start()

    def relay(k):
        own_right(k).wait_recv()
        pass_right(k).start()
        own_left(k).wait_recv()
        pass_left(k).start()
        if k + 2 < planes:
            own_right(k + 2).start()
            own_left(k + 2).start()
        if k == planes - 1:
            for d in range(1, nsplit):
                regroup(1, d).start()

    def absorb(k):
        pass_right(k).wait_recv()
        pass_left(k).wait_recv()
        full = gbuf[k]
        high, lowpart = split2(full)
        mats[k, 0] = high
        mats[k, 1] = lowpart
        if k == 0:
            for d in range(1, nsplit):
                regroup(0, d).wait_recv()
            halo_start(0)
            cvec[...] = mm(cols[0], high, lowpart)
            pf[...] = full
            qown[0] = high
            qown[1] = lowpart
        else:
            cvec[...] = mm(cols[k] + cvec[...], high, lowpart)
            prefix[k - 1] = pf[...]
            pf[...] = mm(pf[...], high, lowpart)

    def absorb_up(k):
        if k > 0:
            qf[...] = mm(gbuf[k], qown[0], qown[1])
            store_pair(qown, qf[...])

    for k in range(planes):
        relay(k)
        if k > 0:
            absorb(k - 1)
            absorb_up(k - 1)
    absorb(planes - 1)

    give_p = remote(pf, pin, c_send.at[0], c_recv.at[0], other, s)
    give_q = remote(qf, qin, c_send.at[1], c_recv.at[1], other, s)
    give_c = remote(cvec, cin, c_send.at[2], c_recv.at[2], other, s)
    give_a = remote(amid, ain, c_send.at[3], c_recv.at[3], other, s)
    give_e = remote(evec, ein, c_send.at[4], c_recv.at[4], other, s)
    give_b = remote(bin_, bcore, c_send.at[5], c_recv.at[5], other, s)
    give_r = remote(rf, rin, c_send.at[6], c_recv.at[6], other, s)
    give_a0 = remote(cvec, azero, c_send.at[7], c_recv.at[7], other, s)
    give_e0 = remote(ezero, ein0, c_send.at[8], c_recv.at[8], other, s)

    hosts = (npos - 1, 0)

    def row_layer(at):
        return 2 * (line * npos + at)

    def chunk(q):
        return pl.ds(q * cb, cb)

    def shared(step):
        return (0, width) if step == 1 else (nx - nx // 4, width // 4)

    def hand_share(way, step):
        base, size = shared(step)
        part = pl.ds(pl.multiple_of(base + s * size, size), size)
        return remote(
            xf.at[way, part, :], mbuf.at[step, part, :],
            x_send.at[way, 0], x_recv.at[step, 0], row_layer(hosts[way]), s,
        )

    def hand_whole(way, step):
        part = pl.ds(0, nx - nx // 4)
        return remote(
            xf.at[way, part, :], mbuf.at[step, part, :],
            x_send.at[way, 1], x_recv.at[step, 1], row_layer(hosts[way]), s,
        )

    def hand_wholes(way, do):
        for step in (0, 2):
            at = step if way == 0 else npos - 1 - step
            pl.when(pos == at)(functools.partial(do, step))

    def hand_vector(way, step):
        return remote(
            vown.at[way], vbuf.at[step], v_send.at[way], v_recv.at[step],
            row_layer(hosts[way]), s,
        )

    def hand_input(way, step):
        return remote(
            inbuf.at[step], (ain, bin_)[way], i_send.at[step], i_recv.at[way],
            row_layer(step if way == 0 else npos - 1 - step), s,
        )

    def hand_on(way, q):
        return remote(
            zout.at[chunk(q), :], zin.at[chunk(q), :], z_send.at[q], z_recv.at[q],
            layer + (2 - 4 * way) * npos, s,
        )

    def ring(step, i):
        base, size = shared(step)
        owner, start, length = (
            (s, 0, size), (s, 0, size), (left, 0, size // 2), (right, size // 2, size // 2)
        )[i]
        rows_at = pl.multiple_of(base + owner * size + start, size // 2)
        part = mbuf.at[step, pl.ds(rows_at, length), :]
        return remote(
            part, part, y_send.at[step, i], y_recv.at[step, i], layer,
            (right, left, right, left)[i],
        )

    def for_step(way, do):
        for step in range(npos - 1):
            at = step if way == 0 else npos - 1 - step
            pl.when(pos == at)(functools.partial(do, step))

    def row_vector(way):
        own = pall if way == 0 else qall
        for step in range(npos - 1):
            hand_vector(way, step).wait_recv()
        total = vbuf[0]
        for step in range(1, npos - 1):
            total = vbuf[step] + mm_ref(total, xpair.at[step])
        zout[...] = vown[way] + mm_ref(total, own)

    def line_starts(way):
        return line == 0 if way == 0 else line == nline - 1

    def line_ends(way):
        return line == nline - 1 if way == 0 else line == 0

    def send_first(way):
        row_vector(way)
        if nline > 1:
            for q in range(nchunk):
                hand_on(way, q).start()

    def host_prepare(way, meanwhile):
        own = pall if way == 0 else qall
        store_pair(own, xf[way])
        order = (1, 2, 0)
        for step in order:
            hand_share(way, step).wait_recv()
            ring(step, 0).start()
            ring(step, 1).start()
        meanwhile()
        for step in order:
            ring(step, 0).wait_recv()
            ring(step, 2).start()
            ring(step, 1).wait_recv()
            ring(step, 3).start()
        upper, lower = pl.ds(0, nx - nx // 4), pl.ds(nx - nx // 4, nx // 4)
        for step in order:
            ring(step, 2).wait_recv()
            ring(step, 3).wait_recv()
            if step == 1:
                store_pair(xpair.at[1], mbuf[1])
            if step == 2:
                hand_whole(way, 2).wait_recv()
                store_pair(xpair.at[2], mbuf[2])
        if way == 0:
            pl.when(line_starts(way))(functools.partial(send_first, way))

        @pl.when(jnp.logical_not(line_starts(way)))
        def _():
            store_pair(xrow, mm_pairs(xpair.at[2], own))
            pf[lower, :] = mm_ref(mbuf[0, lower, :], xpair.at[1])

        hand_whole(way, 0).wait_recv()

        @pl.when(jnp.logical_not(line_starts(way)))
        def _():
            pf[upper, :] = mm_ref(mbuf[0, upper, :], xpair.at[1])
            store_pair(xrow, mm_ref(pf[...], xrow))

        store_pair(xpair.at[0], mbuf[0])

    def host_chain(way):
        starts, ends = line_starts(way), line_ends(way)

        @pl.when(starts)
        def _():
            inbuf[0] = jnp.zeros((yb, nx), F32)
            if way == 1:
                send_first(way)

        @pl.when(jnp.logical_not(starts))
        def _():
            row_vector(way)
            for q in range(nchunk):
                hand_on(way, q).wait_recv()

                @pl.when(jnp.logical_not(ends))
                def _():
                    zout[chunk(q), :] = zout[chunk(q), :] + mm_ref(zin[chunk(q), :], xrow)
                    hand_on(way, q).start()

            inbuf[0] = zin[...]

        state = inbuf[0]
        for step in range(npos - 1):
            hand_input(way, step).start()
            state = vbuf[step] + mm_ref(state, xpair.at[step])
            if step < npos - 2:
                inbuf[step + 1] = state
        (ain, bin_)[way][...] = state

    def host_finish(way):
        ends = line_ends(way)
        for step in range(npos - 1):
            hand_input(way, step).wait_send()
        for step in range(npos - 1):
            for i in range(4):
                ring(step, i).wait_send()

        @pl.when(jnp.logical_not(ends))
        def _():
            for q in range(nchunk):
                hand_on(way, q).wait_send()

    @pl.when(core == 1)
    def _():
        give_c.start()
        give_p.start()

    absorb_up(planes - 1)

    def down_sweep(state):
        for k in range(planes):
            state = mm(cols[k] + state, mats[k, 0], mats[k, 1])
            low[k] = state

    def up_partial(result):
        state = low[planes - 1]
        for k in range(planes - 2, -1, -1):
            state = low[k] + mm(state, mats[k, 0], mats[k, 1])
        result[...] = state

    def response():
        rf[...] = prefix[planes - 2] + mm(pf[...], mats[planes - 2, 0], mats[planes - 2, 1])
        for k in range(planes - 3, -1, -1):
            rf[...] = prefix[k] + mm(rf[...], mats[k, 0], mats[k, 1])

    def up_sweep(state):
        for k in range(planes - 1, -1, -1):
            state = low[k] + mm(state, mats[k, 0], mats[k, 1])
            dirb[k] = state

    @pl.when(core == 1)
    def _():
        give_q.start()
        response()
        give_r.start()
        give_a0.wait_recv()
        down_sweep(azero[...])
        up_partial(ezero)
        give_e0.start()
        prepare()
        give_a.wait_recv()
        down_sweep(ain[...])
        up_partial(evec)
        give_e.start()
        give_b.wait_recv()
        up_sweep(bcore[...])
        for give in (give_c, give_p, give_q, give_r, give_e0, give_e):
            give.wait_send()

    @pl.when(core == 0)
    def _():
        give_a0.start()
        store_pair(pown, pf[...])
        give_c.wait_recv()
        give_p.wait_recv()
        store_pair(pall, pin[...])
        vown[0] = mm_ref(cvec[...], pall) + cin[...]
        for_step(0, lambda step: hand_vector(0, step).start())
        xf[0] = mm_pairs(pown, pall)
        for_step(0, lambda step: hand_share(0, step).start())
        give_q.wait_recv()
        store_pair(q1, qin[...])
        xf[1] = mm_pairs(q1, qown)
        for_step(1, lambda step: hand_share(1, step).start())
        hand_wholes(0, lambda step: hand_whole(0, step).start())
        hand_wholes(1, lambda step: hand_whole(1, step).start())
        prepare()

        response()
        give_r.wait_recv()
        store_pair(rpair, rin[...])
        rin[...] = mm_ref(pf[...], rpair)
        rf[...] = rf[...] + mm_ref(rin[...], qown)
        store_pair(rpair, rf[...])

        def still():
            down_sweep(jnp.zeros((yb, nx), F32))
            up_partial(ezero)
            give_e0.wait_recv()
            ezero[...] = ezero[...] + mm_ref(ein0[...], qown)

        @pl.when(pos == hosts[0])
        def _():
            host_prepare(0, still)
            host_chain(0)

        @pl.when(pos == hosts[1])
        def _():
            host_prepare(1, still)

        @pl.when(jnp.logical_and(pos != hosts[0], pos != hosts[1]))
        def _():
            still()

        for_step(0, lambda step: hand_input(0, step).wait_recv())
        vown[1] = ezero[...] + mm_ref(ain[...], rpair)
        for_step(1, lambda step: hand_vector(1, step).start())
        amid[...] = cvec[...] + mm_ref(ain[...], pown)
        give_a.start()
        down_sweep(ain[...])

        @pl.when(pos == hosts[1])
        def _():
            host_chain(1)

        give_e.wait_recv()
        for_step(1, lambda step: hand_input(1, step).wait_recv())
        give_b.start()
        up_sweep(ein[...] + mm_ref(bin_[...], q1))
        give_a0.wait_send()
        give_a.wait_send()
        give_b.wait_send()
        for way in range(2):
            for_step(way, lambda step, way=way: hand_vector(way, step).wait_send())
            for_step(way, lambda step, way=way: hand_share(way, step).wait_send())
            hand_wholes(way, lambda step, way=way: hand_whole(way, step).wait_send())
            pl.when(pos == hosts[way])(functools.partial(host_finish, way))

    halo_start(1)
    spread_start(0)
    halo_wait(1)
    apply_operator(1, imb)
    halo_start(2)
    spread_start(1, (1, nsplit - 1))
    halo_wait(2)
    apply_operator(2, aimb)
    put_sum(3, cols, imb)
    put_sum(4, arb, imb)
    put_sum(5, aimb, cols)
    put_sum(6, aimb, imb)
    put_sum(7, arb, aimb)
    put_sum(8, aimb, aimb)

    place = core * nsplit + s
    count = 2 * nsplit

    def near(d):
        at = lax.rem(place + d, count)
        return remote(
            group.at[place], group.at[place], n_send.at[d - 1], n_recv.at[d - 1],
            2 * chip + at // nsplit, lax.rem(at, nsplit),
        )

    def far(d):
        at = lax.rem(chip + d, nchip)
        return remote(
            whole.at[chip], whole.at[chip], w_send.at[d - 1], w_recv.at[d - 1],
            2 * at + core, s,
        )

    diagonal = lax.broadcasted_iota(jnp.int32, (nrow, width), 0) == lax.broadcasted_iota(
        jnp.int32, (nrow, width), 1
    )
    sums = jnp.where(diagonal, jnp.sum(part[...], axis=1, keepdims=True), 0.0)
    group[place] = jnp.sum(sums, axis=0, keepdims=True)
    for d in range(1, count):
        near(d).start()
    spread_start(1, range(2, nsplit - 1))
    spread_start(2)
    for n in (3, 0):
        spread_finish(n)
    for d in range(1, count):
        near(d).wait_recv()
    total = group[0]
    for i in range(1, count):
        total = total + group[i]
    whole[chip] = total
    for d in range(1, nchip):
        far(d).start()
    for n in (1, 2):
        spread_finish(n)
    for d in range(1, nchip):
        far(d).wait_recv()
    total = whole[0]
    for i in range(1, nchip):
        total = total + whole[i]
    rr, ar, aa, ri, ai, br, bi, ab, bb = [total[:, i : i + 1] for i in range(9)]
    alpha = rr / ri
    cross = ar - alpha * (ai + br) + alpha * alpha * bi
    own = aa - 2.0 * alpha * ab + alpha * alpha * bb
    omega = cross / own
    for k in range(planes):
        middle = rhs_ref[k] - alpha * flat[1, k]
        sol_ref[k] = alpha * flat[0, k] + omega * middle
        res_ref[k] = middle - omega * (flat[3, k] - alpha * flat[2, k])

    for n in range(2):
        for d in range(1, nsplit):
            regroup(n, d).wait_send()
    for k in range(planes):
        own_right(k).wait_send()
        own_left(k).wait_send()
        pass_right(k).wait_send()
        pass_left(k).wait_send()
    for n in range(4):
        for d in range(1, nsplit):
            spread(n, d).wait_send()
    for n in range(3):
        for i in range(4):
            pl.when(gives[i])(lambda n=n, i=i: halo(n, i).wait_send())
    for d in range(1, count):
        near(d).wait_send()
    for d in range(1, nchip):
        far(d).wait_send()


def per_device(nlayer, nsplit, right_side, diagonal, inverses):
    planes, nx, width = inverses.shape
    ysize = right_side.shape[2]
    yb = ysize // nsplit
    nchip = nlayer // 2
    nchunk = 2
    nrow = 16
    vmem = pl.BlockSpec(memory_space=pltpu.VMEM)
    square = pltpu.VMEM((nx, nx), F32)
    pair = pltpu.VMEM((2, nx, nx), BF16)
    strip = pltpu.VMEM((yb, nx), F32)
    columns = pltpu.VMEM((planes, yb, nx), F32)
    block = pltpu.VMEM((planes, ysize, width), F32)
    dma = pltpu.SemaphoreType.DMA
    shape = jax.ShapeDtypeStruct((planes, width, ysize), F32)
    return pl.pallas_call(
        functools.partial(sweep_kernel, nlayer, nsplit, nchunk, nrow),
        out_shape=(shape, shape),
        in_specs=[vmem] * 3,
        out_specs=(vmem, vmem),
        scratch_shapes=[
            pltpu.VMEM((planes, nx, nx), F32),
            pltpu.VMEM((planes, 2, nx, nx), BF16),
            block, block,
            columns, columns, columns, columns, columns, columns, columns,
            square, square, pair, pair, pair, pair, pair, square, square,
            strip, strip, strip, strip, strip, strip, strip, strip, strip, strip,
            pltpu.VMEM((2, nx, nx), F32), pltpu.VMEM((3, nx, nx), F32),
            pltpu.VMEM((3, 2, nx, nx), BF16), pair,
            pltpu.VMEM((2, yb, nx), F32), pltpu.VMEM((3, yb, nx), F32),
            pltpu.VMEM((3, yb, nx), F32),
            pltpu.VMEM((planes - 1, nx, nx), F32), square, square, pair, strip, strip, strip,
            pltpu.VMEM((3, yb, nx), F32), pltpu.VMEM((3, yb, nx), F32),
            pltpu.VMEM((3, 8, nx), F32), pltpu.VMEM((3, 8, nx), F32),
            pltpu.VMEM((3, 2, 8, nx), F32),
            pltpu.VMEM((4, planes, ysize, width), F32),
            pltpu.VMEM((4, planes, width, ysize), F32),
            pltpu.VMEM((nrow, width), F32),
            pltpu.VMEM((2 * nsplit, 1, width), F32),
            pltpu.VMEM((nchip, 1, width), F32),
            dma((2, nsplit - 1)), dma((2, nsplit - 1)),
            dma((4, planes)), dma((4, planes)),
            dma((9,)), dma((9,)),
            dma((2, 2)), dma((3, 2)), dma((2,)), dma((3,)), dma((3,)), dma((2,)),
            dma((nchunk,)), dma((nchunk,)), dma((3, 4)), dma((3, 4)),
            dma((3, 4)), dma((3, 4)),
            dma((4, nsplit - 1)), dma((4, nsplit - 1)),
            dma((2 * nsplit - 1,)), dma((2 * nsplit - 1,)),
            dma((nchip - 1,)), dma((nchip - 1,)),
        ],
        compiler_params=pltpu.CompilerParams(
            collective_id=0, has_side_effects=True, vmem_limit_bytes=56 * 1024 * 1024
        ),
        name="sweeps",
    )(right_side, diagonal, inverses)


def solution(mesh):
    spec = P("layer", "split", None)
    return jax.shard_map(
        functools.partial(per_device, mesh.shape["layer"], mesh.shape["split"]),
        mesh=mesh,
        in_specs=(spec, spec, P("layer", None, "split")),
        out_specs=(spec, spec),
        check_vma=False,
    )
```

```python
import functools

import jax
import jax.numpy as jnp
from jax import lax
from jax.experimental import pallas as pl
from jax.experimental.pallas import tpu as pltpu
from jax.sharding import PartitionSpec as P

MESH = pl.DeviceIdType.MESH
F32 = jnp.float32
BF16 = jnp.bfloat16


def split2(x):
    high = x.astype(BF16)
    return high, (x - high.astype(F32)).astype(BF16)


def mm(x, w_high, w_low):
    high, low = split2(x)
    dot = functools.partial(jnp.dot, preferred_element_type=F32)
    n = x.shape[0]
    if n > 128:
        return dot(high, w_high) + (dot(low, w_high) + dot(high, w_low))
    both = dot(jnp.concatenate([high, low], 0), w_high)
    return both[:n] + (both[n:] + dot(high, w_low))


def mm_ref(x, pair):
    return mm(x, pair[0], pair[1])


def mm_pairs(x, pair):
    dot = functools.partial(jnp.dot, preferred_element_type=F32)
    return dot(x[0], pair[0]) + (dot(x[1], pair[0]) + dot(x[0], pair[1]))


def store_pair(pair, x):
    high, low = split2(x)
    pair[0] = high
    pair[1] = low


def sweep_kernel(
    nlayer, nsplit, nchunk, nrow,
    rhs_ref, diag_ref, inv_ref, sol_ref, res_ref,
    gbuf, mats, rsend, dsend, cols, dcols, low, dirb, imb, aimb, arb,
    pf, qf, pown, qown, pall, qall, q1, pin, qin,
    cvec, cin, ain, amid, evec, ein, bin_, bcore, zin, zout,
    xf, mbuf, xpair, xrow, vown, vbuf, inbuf,
    prefix, rf, rin, rpair, azero, ezero, ein0,
    zlow, zhigh, ylow, yhigh, edges, lines, flat, part, group, whole,
    rs_send, rs_recv, g_send, g_recv, c_send, c_recv,
    x_send, x_recv, v_send, v_recv, i_send, i_recv, z_send, z_recv, y_send, y_recv,
    h_send, h_recv, l_send, l_recv, n_send, n_recv, w_send, w_recv,
):
    planes, nx, width = inv_ref.shape
    ysize = rhs_ref.shape[2]
    yb = ysize // nsplit
    cb = yb // nchunk
    half = width // 2
    layer = lax.axis_index("layer")
    s = lax.axis_index("split")
    core = lax.rem(layer, 2)
    chip = layer // 2
    nchip = nlayer // 2
    right = lax.rem(s + 1, nsplit)
    left = lax.rem(s + nsplit - 1, nsplit)
    other = layer + 1 - 2 * core
    npos = 4
    pos, line = lax.rem(chip, npos), chip // npos
    nline = nchip // npos

    def rows(owner, start, size):
        return pl.ds(pl.multiple_of(owner * width + start, half), size)

    def lanes(t):
        return pl.ds(pl.multiple_of(t * width, width), width)

    def lines_of(t):
        return pl.ds(pl.multiple_of(t * yb, yb), yb)

    for empty in (zlow, zhigh, ylow, yhigh, edges, part):
        empty[...] = jnp.zeros_like(empty)

    barrier = pltpu.get_barrier_semaphore()

    def greet(l, t):
        pl.semaphore_signal(barrier, inc=1, device_id=(l, t), device_id_type=MESH)

    for d in range(1, nsplit):
        greet(layer, lax.rem(s + d, nsplit))
    for d in range(nsplit):
        greet(other, lax.rem(s + d, nsplit))
    for d in range(1, nchip):
        greet(2 * lax.rem(chip + d, nchip) + core, s)
    side = layer - 1 + 2 * core
    inner = jnp.logical_and(side >= 0, side < nlayer)

    @pl.when(inner)
    def _():
        greet(side, s)

    for k in range(planes):
        gbuf[k, rows(s, 0, width), :] = inv_ref[k].T
    for source, sent, mine in ((rhs_ref, rsend, cols), (diag_ref, dsend, dcols)):
        for k in range(planes):
            sent[k] = source[k].T
        for k in range(planes):
            mine[k, :, lanes(s)] = sent[k, lines_of(s), :]

    pl.semaphore_wait(barrier, 2 * nsplit - 1 + nchip - 1 + jnp.where(inner, 1, 0))

    def remote(src, dst, send, recv, l, t):
        return pltpu.make_async_remote_copy(
            src_ref=src, dst_ref=dst, send_sem=send, recv_sem=recv,
            device_id=(l, t), device_id_type=MESH,
        )

    def regroup(n, d):
        t = lax.rem(s + d, nsplit)
        sent, mine = ((rsend, cols), (dsend, dcols))[n]
        return remote(
            sent.at[:, lines_of(t), :], mine.at[:, :, lanes(s)],
            rs_send.at[n, d - 1], rs_recv.at[n, d - 1], layer, t,
        )

    def spread(n, d):
        t = lax.rem(s + d, nsplit)
        return remote(
            (dirb, imb, aimb, arb)[n].at[:, :, lanes(t)], lines.at[n, :, lines_of(s), :],
            l_send.at[n, d - 1], l_recv.at[n, d - 1], layer, t,
        )

    def spread_start(n, distances=None):
        for d in range(1, nsplit) if distances is None else distances:
            spread(n, d).start()
        if distances is not None and 1 not in distances:
            return
        for k in range(planes):
            lines[n, k, lines_of(s), :] = (dirb, imb, aimb, arb)[n][k, :, lanes(s)]

    def spread_finish(n):
        for d in range(1, nsplit):
            spread(n, d).wait_recv()
        for k in range(planes):
            flat[n, k] = lines[n, k].T

    def halo(n, i):
        values = (cols, dirb, imb)[n]
        src = (values.at[planes - 1], values.at[0], edges.at[n, 0], edges.at[n, 1])[i]
        dst = (zlow, zhigh, ylow, yhigh)[i].at[n]
        l, t = ((layer + 1, s), (layer - 1, s), (layer, s + 1), (layer, s - 1))[i]
        return remote(src, dst, h_send.at[n, i], h_recv.at[n, i], l, t)

    to_high, to_low = layer < nlayer - 1, layer > 0
    to_right, to_left = s < nsplit - 1, s > 0
    gives = (to_high, to_low, to_right, to_left)
    takes = (to_low, to_high, to_left, to_right)

    def halo_start(n):
        values = (cols, dirb, imb)[n]
        for i in range(2):
            pl.when(gives[i])(lambda i=i: halo(n, i).start())
        for k in range(planes):
            edges[n, 0, k : k + 1, :] = values[k, yb - 1 : yb, :]
            edges[n, 1, k : k + 1, :] = values[k, 0:1, :]
        for i in range(2, 4):
            pl.when(gives[i])(lambda i=i: halo(n, i).start())

    def halo_wait(n):
        for i in range(4):
            pl.when(takes[i])(lambda i=i: halo(n, i).wait_recv())

    row = lax.broadcasted_iota(jnp.int32, (yb, nx), 0)
    lane = lax.broadcasted_iota(jnp.int32, (yb, nx), 1)

    def apply_operator(n, result):
        values = (cols, dirb, imb)[n]
        for k in range(planes):
            v = values[k]
            below = values[k - 1] if k > 0 else zlow[n]
            above = values[k + 1] if k < planes - 1 else zhigh[n]
            x_low = jnp.where(lane == 0, 0.0, pltpu.roll(v, 1, 1))
            x_high = jnp.where(lane == nx - 1, 0.0, pltpu.roll(v, nx - 1, 1))
            y_low = jnp.where(row == 0, ylow[n, k : k + 1, :], pltpu.roll(v, 1, 0))
            y_high = jnp.where(row == yb - 1, yhigh[n, k : k + 1, :], pltpu.roll(v, yb - 1, 0))
            beside = (below + above) + (x_low + x_high) + (y_low + y_high)
            result[k] = (6.0 + dcols[k]) * v - beside

    def put_sum(i, a, b):
        total = a[0] * b[0]
        for k in range(1, planes):
            total = total + a[k] * b[k]
        total = jnp.sum(total, axis=0, keepdims=True)
        lane_sum = total[:, :width]
        for t in range(1, nsplit):
            lane_sum = lane_sum + total[:, t * width : (t + 1) * width]
        part[i : i + 1, :] = lane_sum

    def prepare():
        for d in range(1, nsplit):
            regroup(1, d).wait_recv()
        halo_wait(0)
        apply_operator(0, arb)
        put_sum(0, cols, cols)
        put_sum(1, arb, cols)
        put_sum(2, arb, arb)

    def own_right(k):
        part = gbuf.at[k, rows(s, 0, width), :]
        return remote(part, part, g_send.at[0, k], g_recv.at[0, k], layer, right)

    def own_left(k):
        part = gbuf.at[k, rows(s, 0, width), :]
        return remote(part, part, g_send.at[1, k], g_recv.at[1, k], layer, left)

    def pass_right(k):
        part = gbuf.at[k, rows(left, 0, half), :]
        return remote(part, part, g_send.at[2, k], g_recv.at[2, k], layer, right)

    def pass_left(k):
        part = gbuf.at[k, rows(right, half, half), :]
        return remote(part, part, g_send.at[3, k], g_recv.at[3, k], layer, left)

    for d in range(1, nsplit):
        regroup(0, d).start()
    for k in range(min(2, planes)):
        own_right(k).start()
        own_left(k).start()

    def relay(k):
        own_right(k).wait_recv()
        pass_right(k).start()
        own_left(k).wait_recv()
        pass_left(k).start()
        if k + 2 < planes:
            own_right(k + 2).start()
            own_left(k + 2).start()
        if k == planes - 1:
            for d in range(1, nsplit):
                regroup(1, d).start()

    def absorb(k):
        pass_right(k).wait_recv()
        pass_left(k).wait_recv()
        full = gbuf[k]
        high, lowpart = split2(full)
        mats[k, 0] = high
        mats[k, 1] = lowpart
        if k == 0:
            for d in range(1, nsplit):
                regroup(0, d).wait_recv()
            halo_start(0)
            cvec[...] = mm(cols[0], high, lowpart)
            pf[...] = full
            qown[0] = high
            qown[1] = lowpart
        else:
            cvec[...] = mm(cols[k] + cvec[...], high, lowpart)
            prefix[k - 1] = pf[...]
            pf[...] = mm(pf[...], high, lowpart)

    def absorb_up(k):
        if k > 0:
            qf[...] = mm(gbuf[k], qown[0], qown[1])
            store_pair(qown, qf[...])

    for k in range(planes):
        relay(k)
        if k > 0:
            absorb(k - 1)
            absorb_up(k - 1)
    absorb(planes - 1)

    give_p = remote(pf, pin, c_send.at[0], c_recv.at[0], other, s)
    give_q = remote(qf, qin, c_send.at[1], c_recv.at[1], other, s)
    give_c = remote(cvec, cin, c_send.at[2], c_recv.at[2], other, s)
    give_a = remote(amid, ain, c_send.at[3], c_recv.at[3], other, s)
    give_e = remote(evec, ein, c_send.at[4], c_recv.at[4], other, s)
    give_b = remote(bin_, bcore, c_send.at[5], c_recv.at[5], other, s)
    give_r = remote(rf, rin, c_send.at[6], c_recv.at[6], other, s)
    give_a0 = remote(cvec, azero, c_send.at[7], c_recv.at[7], other, s)
    give_e0 = remote(ezero, ein0, c_send.at[8], c_recv.at[8], other, s)

    hosts = (npos - 1, 0)

    def row_layer(at):
        return 2 * (line * npos + at)

    def chunk(q):
        return pl.ds(q * cb, cb)

    def shared(step):
        return (0, width) if step == 1 else (nx - nx // 4, width // 4)

    def hand_share(way, step):
        base, size = shared(step)
        part = pl.ds(pl.multiple_of(base + s * size, size), size)
        return remote(
            xf.at[way, part, :], mbuf.at[step, part, :],
            x_send.at[way, 0], x_recv.at[step, 0], row_layer(hosts[way]), s,
        )

    def hand_whole(way, step):
        part = pl.ds(0, nx - nx // 4)
        return remote(
            xf.at[way, part, :], mbuf.at[step, part, :],
            x_send.at[way, 1], x_recv.at[step, 1], row_layer(hosts[way]), s,
        )

    def hand_wholes(way, do):
        for step in (0, 2):
            at = step if way == 0 else npos - 1 - step
            pl.when(pos == at)(functools.partial(do, step))

    def hand_vector(way, step):
        return remote(
            vown.at[way], vbuf.at[step], v_send.at[way], v_recv.at[step],
            row_layer(hosts[way]), s,
        )

    def hand_input(way, step):
        return remote(
            inbuf.at[step], (ain, bin_)[way], i_send.at[step], i_recv.at[way],
            row_layer(step if way == 0 else npos - 1 - step), s,
        )

    def hand_on(way, q):
        return remote(
            zout.at[chunk(q), :], zin.at[chunk(q), :], z_send.at[q], z_recv.at[q],
            layer + (2 - 4 * way) * npos, s,
        )

    def ring(step, i):
        base, size = shared(step)
        owner, start, length = (
            (s, 0, size), (s, 0, size), (left, 0, size // 2), (right, size // 2, size // 2)
        )[i]
        rows_at = pl.multiple_of(base + owner * size + start, size // 2)
        part = mbuf.at[step, pl.ds(rows_at, length), :]
        return remote(
            part, part, y_send.at[step, i], y_recv.at[step, i], layer,
            (right, left, right, left)[i],
        )

    def for_step(way, do):
        for step in range(npos - 1):
            at = step if way == 0 else npos - 1 - step
            pl.when(pos == at)(functools.partial(do, step))

    def row_vector(way):
        own = pall if way == 0 else qall
        for step in range(npos - 1):
            hand_vector(way, step).wait_recv()
        total = vbuf[0]
        for step in range(1, npos - 1):
            total = vbuf[step] + mm_ref(total, xpair.at[step])
        zout[...] = vown[way] + mm_ref(total, own)

    def line_starts(way):
        return line == 0 if way == 0 else line == nline - 1

    def line_ends(way):
        return line == nline - 1 if way == 0 else line == 0

    def send_first(way):
        for q in range(nchunk):
            hand_on(way, q).start()

    def host_prepare(way, meanwhile):
        own = pall if way == 0 else qall
        store_pair(own, xf[way])
        order = (1, 2, 0)
        for step in order:
            hand_share(way, step).wait_recv()
            ring(step, 0).start()
            ring(step, 1).start()
        meanwhile()
        for step in order:
            ring(step, 0).wait_recv()
            ring(step, 2).start()
            ring(step, 1).wait_recv()
            ring(step, 3).start()
        starts = line_starts(way)
        upper, lower = pl.ds(0, nx - nx // 4), pl.ds(nx - nx // 4, nx // 4)

        def passed(step):
            ring(step, 2).wait_recv()
            ring(step, 3).wait_recv()

        def ahead_of_rest(part):
            pin[part, :] = mm_ref(mbuf[2, part, :], own)

        hand_whole(way, 2).wait_recv()
        pl.when(jnp.logical_not(starts))(functools.partial(ahead_of_rest, upper))
        passed(1)
        store_pair(xpair.at[1], mbuf[1])
        passed(2)
        store_pair(xpair.at[2], mbuf[2])
        if way == 0:
            row_vector(way)
            if nline > 1:
                pl.when(starts)(functools.partial(send_first, way))
        hand_whole(way, 0).wait_recv()

        @pl.when(jnp.logical_not(starts))
        def _():
            pf[upper, :] = mm_ref(mbuf[0, upper, :], xpair.at[1])
            ahead_of_rest(lower)
            store_pair(xrow, pin[...])

        passed(0)

        @pl.when(jnp.logical_not(starts))
        def _():
            pf[lower, :] = mm_ref(mbuf[0, lower, :], xpair.at[1])
            store_pair(xrow, mm_ref(pf[...], xrow))

        store_pair(xpair.at[0], mbuf[0])

    def host_chain(way):
        starts, ends = line_starts(way), line_ends(way)
        if way == 1:
            row_vector(way)

        @pl.when(starts)
        def _():
            inbuf[0] = jnp.zeros((yb, nx), F32)
            if way == 1 and nline > 1:
                send_first(way)

        @pl.when(jnp.logical_not(starts))
        def _():
            for q in range(nchunk):
                hand_on(way, q).wait_recv()

                @pl.when(jnp.logical_not(ends))
                def _():
                    zout[chunk(q), :] = zout[chunk(q), :] + mm_ref(zin[chunk(q), :], xrow)
                    hand_on(way, q).start()

            inbuf[0] = zin[...]

        state = inbuf[0]
        for step in range(npos - 1):
            hand_input(way, step).start()
            state = vbuf[step] + mm_ref(state, xpair.at[step])
            if step < npos - 2:
                inbuf[step + 1] = state
        (ain, bin_)[way][...] = state

    def host_finish(way):
        ends = line_ends(way)
        for step in range(npos - 1):
            hand_input(way, step).wait_send()
        for step in range(npos - 1):
            for i in range(4):
                ring(step, i).wait_send()

        @pl.when(jnp.logical_not(ends))
        def _():
            for q in range(nchunk):
                hand_on(way, q).wait_send()

    @pl.when(core == 1)
    def _():
        give_c.start()
        give_p.start()
        absorb_up(planes - 1)

    def down_sweep(state):
        for k in range(planes):
            state = mm(cols[k] + state, mats[k, 0], mats[k, 1])
            low[k] = state

    def up_partial(result):
        state = low[planes - 1]
        for k in range(planes - 2, -1, -1):
            state = low[k] + mm(state, mats[k, 0], mats[k, 1])
        result[...] = state

    def response():
        rf[...] = prefix[planes - 2] + mm(pf[...], mats[planes - 2, 0], mats[planes - 2, 1])
        for k in range(planes - 3, -1, -1):
            rf[...] = prefix[k] + mm(rf[...], mats[k, 0], mats[k, 1])

    def up_sweep(state):
        for k in range(planes - 1, -1, -1):
            state = low[k] + mm(state, mats[k, 0], mats[k, 1])
            dirb[k] = state

    @pl.when(core == 1)
    def _():
        give_q.start()
        response()
        give_r.start()
        give_a0.wait_recv()
        down_sweep(azero[...])
        up_partial(ezero)
        give_e0.start()
        prepare()
        give_a.wait_recv()
        down_sweep(ain[...])
        up_partial(evec)
        give_e.start()
        spread_start(3)
        give_b.wait_recv()
        up_sweep(bcore[...])
        for give in (give_c, give_p, give_q, give_r, give_e0, give_e):
            give.wait_send()

    @pl.when(core == 0)
    def _():
        give_a0.start()
        store_pair(pown, pf[...])
        give_c.wait_recv()
        give_p.wait_recv()
        store_pair(pall, pin[...])
        vown[0] = mm_ref(cvec[...], pall) + cin[...]
        for_step(0, lambda step: hand_vector(0, step).start())
        xf[0] = mm_pairs(pown, pall)
        for_step(0, lambda step: hand_share(0, step).start())
        absorb_up(planes - 1)
        give_q.wait_recv()
        store_pair(q1, qin[...])
        xf[1] = mm_pairs(q1, qown)
        for_step(1, lambda step: hand_share(1, step).start())
        hand_wholes(0, lambda step: hand_whole(0, step).start())
        hand_wholes(1, lambda step: hand_whole(1, step).start())
        prepare()

        response()

        def still():
            give_r.wait_recv()
            store_pair(rpair, rin[...])
            rin[...] = mm_pairs(pown, rpair)
            rf[...] = rf[...] + mm_ref(rin[...], qown)
            store_pair(rpair, rf[...])
            down_sweep(jnp.zeros((yb, nx), F32))
            up_partial(ezero)
            give_e0.wait_recv()
            ezero[...] = ezero[...] + mm_ref(ein0[...], qown)

        @pl.when(pos == hosts[0])
        def _():
            host_prepare(0, still)
            host_chain(0)

        @pl.when(pos == hosts[1])
        def _():
            host_prepare(1, still)

        @pl.when(jnp.logical_and(pos != hosts[0], pos != hosts[1]))
        def _():
            still()

        for_step(0, lambda step: hand_input(0, step).wait_recv())
        vown[1] = ezero[...] + mm_ref(ain[...], rpair)
        for_step(1, lambda step: hand_vector(1, step).start())
        amid[...] = cvec[...] + mm_ref(ain[...], pown)
        give_a.start()
        spread_start(3)
        down_sweep(ain[...])

        @pl.when(pos == hosts[1])
        def _():
            host_chain(1)

        give_e.wait_recv()
        for_step(1, lambda step: hand_input(1, step).wait_recv())
        give_b.start()
        up_sweep(ein[...] + mm_ref(bin_[...], q1))
        give_a0.wait_send()
        give_a.wait_send()
        give_b.wait_send()
        for way in range(2):
            for_step(way, lambda step, way=way: hand_vector(way, step).wait_send())
            for_step(way, lambda step, way=way: hand_share(way, step).wait_send())
            hand_wholes(way, lambda step, way=way: hand_whole(way, step).wait_send())
            pl.when(pos == hosts[way])(functools.partial(host_finish, way))

    halo_start(1)
    spread_start(0)
    halo_wait(1)
    apply_operator(1, imb)
    halo_start(2)
    spread_start(1, (1, nsplit - 1))
    halo_wait(2)
    apply_operator(2, aimb)
    put_sum(3, cols, imb)
    put_sum(4, arb, imb)
    put_sum(5, aimb, cols)
    put_sum(6, aimb, imb)
    put_sum(7, arb, aimb)
    put_sum(8, aimb, aimb)

    place = core * nsplit + s
    count = 2 * nsplit

    def near(d):
        at = lax.rem(place + d, count)
        return remote(
            group.at[place], group.at[place], n_send.at[d - 1], n_recv.at[d - 1],
            2 * chip + at // nsplit, lax.rem(at, nsplit),
        )

    def far(d):
        at = lax.rem(chip + d, nchip)
        return remote(
            whole.at[chip], whole.at[chip], w_send.at[d - 1], w_recv.at[d - 1],
            2 * at + core, s,
        )

    diagonal = lax.broadcasted_iota(jnp.int32, (nrow, width), 0) == lax.broadcasted_iota(
        jnp.int32, (nrow, width), 1
    )
    sums = jnp.where(diagonal, jnp.sum(part[...], axis=1, keepdims=True), 0.0)
    group[place] = jnp.sum(sums, axis=0, keepdims=True)
    for d in range(1, count):
        near(d).start()
    spread_start(1, range(2, nsplit - 1))
    spread_start(2)
    for n in (3, 0):
        spread_finish(n)
    for d in range(1, count):
        near(d).wait_recv()
    total = group[0]
    for i in range(1, count):
        total = total + group[i]
    whole[chip] = total
    for d in range(1, nchip):
        far(d).start()
    for n in (1, 2):
        spread_finish(n)
    for d in range(1, nchip):
        far(d).wait_recv()
    total = whole[0]
    for i in range(1, nchip):
        total = total + whole[i]
    rr, ar, aa, ri, ai, br, bi, ab, bb = [total[:, i : i + 1] for i in range(9)]
    alpha = rr / ri
    cross = ar - alpha * (ai + br) + alpha * alpha * bi
    own = aa - 2.0 * alpha * ab + alpha * alpha * bb
    omega = cross / own
    for k in range(planes):
        middle = rhs_ref[k] - alpha * flat[1, k]
        sol_ref[k] = alpha * flat[0, k] + omega * middle
        res_ref[k] = middle - omega * (flat[3, k] - alpha * flat[2, k])

    for n in range(2):
        for d in range(1, nsplit):
            regroup(n, d).wait_send()
    for k in range(planes):
        own_right(k).wait_send()
        own_left(k).wait_send()
        pass_right(k).wait_send()
        pass_left(k).wait_send()
    for n in range(4):
        for d in range(1, nsplit):
            spread(n, d).wait_send()
    for n in range(3):
        for i in range(4):
            pl.when(gives[i])(lambda n=n, i=i: halo(n, i).wait_send())
    for d in range(1, count):
        near(d).wait_send()
    for d in range(1, nchip):
        far(d).wait_send()


def per_device(nlayer, nsplit, right_side, diagonal, inverses):
    planes, nx, width = inverses.shape
    ysize = right_side.shape[2]
    yb = ysize // nsplit
    nchip = nlayer // 2
    nchunk = 2
    nrow = 16
    vmem = pl.BlockSpec(memory_space=pltpu.VMEM)
    square = pltpu.VMEM((nx, nx), F32)
    pair = pltpu.VMEM((2, nx, nx), BF16)
    strip = pltpu.VMEM((yb, nx), F32)
    columns = pltpu.VMEM((planes, yb, nx), F32)
    block = pltpu.VMEM((planes, ysize, width), F32)
    dma = pltpu.SemaphoreType.DMA
    shape = jax.ShapeDtypeStruct((planes, width, ysize), F32)
    return pl.pallas_call(
        functools.partial(sweep_kernel, nlayer, nsplit, nchunk, nrow),
        out_shape=(shape, shape),
        in_specs=[vmem] * 3,
        out_specs=(vmem, vmem),
        scratch_shapes=[
            pltpu.VMEM((planes, nx, nx), F32),
            pltpu.VMEM((planes, 2, nx, nx), BF16),
            block, block,
            columns, columns, columns, columns, columns, columns, columns,
            square, square, pair, pair, pair, pair, pair, square, square,
            strip, strip, strip, strip, strip, strip, strip, strip, strip, strip,
            pltpu.VMEM((2, nx, nx), F32), pltpu.VMEM((3, nx, nx), F32),
            pltpu.VMEM((3, 2, nx, nx), BF16), pair,
            pltpu.VMEM((2, yb, nx), F32), pltpu.VMEM((3, yb, nx), F32),
            pltpu.VMEM((3, yb, nx), F32),
            pltpu.VMEM((planes - 1, nx, nx), F32), square, square, pair, strip, strip, strip,
            pltpu.VMEM((3, yb, nx), F32), pltpu.VMEM((3, yb, nx), F32),
            pltpu.VMEM((3, 8, nx), F32), pltpu.VMEM((3, 8, nx), F32),
            pltpu.VMEM((3, 2, 8, nx), F32),
            pltpu.VMEM((4, planes, ysize, width), F32),
            pltpu.VMEM((4, planes, width, ysize), F32),
            pltpu.VMEM((nrow, width), F32),
            pltpu.VMEM((2 * nsplit, 1, width), F32),
            pltpu.VMEM((nchip, 1, width), F32),
            dma((2, nsplit - 1)), dma((2, nsplit - 1)),
            dma((4, planes)), dma((4, planes)),
            dma((9,)), dma((9,)),
            dma((2, 2)), dma((3, 2)), dma((2,)), dma((3,)), dma((3,)), dma((2,)),
            dma((nchunk,)), dma((nchunk,)), dma((3, 4)), dma((3, 4)),
            dma((3, 4)), dma((3, 4)),
            dma((4, nsplit - 1)), dma((4, nsplit - 1)),
            dma((2 * nsplit - 1,)), dma((2 * nsplit - 1,)),
            dma((nchip - 1,)), dma((nchip - 1,)),
        ],
        compiler_params=pltpu.CompilerParams(
            collective_id=0, has_side_effects=True, vmem_limit_bytes=50 * 1024 * 1024
        ),
        name="sweeps",
    )(right_side, diagonal, inverses)


def solution(mesh):
    spec = P("layer", "split", None)
    return jax.shard_map(
        functools.partial(per_device, mesh.shape["layer"], mesh.shape["split"]),
        mesh=mesh,
        in_specs=(spec, spec, P("layer", None, "split")),
        out_specs=(spec, spec),
        check_vma=False,
    )
```

```python
import functools

import jax
import jax.numpy as jnp
from jax import lax
from jax.experimental import pallas as pl
from jax.experimental.pallas import tpu as pltpu
from jax.sharding import PartitionSpec as P

MESH = pl.DeviceIdType.MESH
F32 = jnp.float32
BF16 = jnp.bfloat16


def split2(x):
    high = x.astype(BF16)
    return high, (x - high.astype(F32)).astype(BF16)


def mm(x, w_high, w_low):
    high, low = split2(x)
    dot = functools.partial(jnp.dot, preferred_element_type=F32)
    n = x.shape[0]
    if n > 128:
        return dot(high, w_high) + (dot(low, w_high) + dot(high, w_low))
    both = dot(jnp.concatenate([high, low], 0), w_high)
    return both[:n] + (both[n:] + dot(high, w_low))


def mm_ref(x, pair):
    return mm(x, pair[0], pair[1])


def mm_pairs(x, pair):
    dot = functools.partial(jnp.dot, preferred_element_type=F32)
    return dot(x[0], pair[0]) + (dot(x[1], pair[0]) + dot(x[0], pair[1]))


def store_pair(pair, x):
    high, low = split2(x)
    pair[0] = high
    pair[1] = low


def sweep_kernel(
    nlayer, nsplit, nchunk, nrow,
    rhs_in, diag_in, inv_in, sol_ref, res_ref,
    gbuf, mats, rsend, dsend, cols, dcols, low, dirb, imb, aimb, arb,
    pf, qf, pown, qown, pall, qall, q1, pin, qin,
    cvec, cin, ain, amid, evec, ein, bin_, bcore, zin, zout,
    xf, mbuf, xpair, xrow, vown, vbuf, inbuf,
    prefix, rf, rin, rpair, azero, ezero, ein0,
    zlow, zhigh, ylow, yhigh, edges, lines, flat, part, group, whole,
    rhs_ref, diag_ref, inv_ref, in_sem,
    rs_send, rs_recv, g_send, g_recv, c_send, c_recv,
    x_send, x_recv, v_send, v_recv, i_send, i_recv, z_send, z_recv, y_send, y_recv,
    h_send, h_recv, l_send, l_recv, n_send, n_recv, w_send, w_recv,
):
    planes, nx, width = inv_in.shape
    ysize = rhs_in.shape[2]
    yb = ysize // nsplit
    cb = yb // nchunk
    half = width // 2
    layer = lax.axis_index("layer")
    s = lax.axis_index("split")
    core = lax.rem(layer, 2)
    chip = layer // 2
    nchip = nlayer // 2
    right = lax.rem(s + 1, nsplit)
    left = lax.rem(s + nsplit - 1, nsplit)
    other = layer + 1 - 2 * core
    npos = 4
    pos, line = lax.rem(chip, npos), chip // npos
    nline = nchip // npos

    def rows(owner, start, size):
        return pl.ds(pl.multiple_of(owner * width + start, half), size)

    def lanes(t):
        return pl.ds(pl.multiple_of(t * width, width), width)

    def lines_of(t):
        return pl.ds(pl.multiple_of(t * yb, yb), yb)

    loads = [
        pltpu.make_async_copy(src, dst, in_sem.at[i])
        for i, (src, dst) in enumerate(
            ((inv_in, inv_ref), (rhs_in, rhs_ref), (diag_in, diag_ref))
        )
    ]
    for load in loads:
        load.start()
    for empty in (zlow, zhigh, ylow, yhigh, edges, part):
        empty[...] = jnp.zeros_like(empty)

    barrier = pltpu.get_barrier_semaphore()

    def greet(l, t):
        pl.semaphore_signal(barrier, inc=1, device_id=(l, t), device_id_type=MESH)

    for d in range(1, nsplit):
        greet(layer, lax.rem(s + d, nsplit))
    for d in range(nsplit):
        greet(other, lax.rem(s + d, nsplit))
    for d in range(1, nchip):
        greet(2 * lax.rem(chip + d, nchip) + core, s)
    side = layer - 1 + 2 * core
    inner = jnp.logical_and(side >= 0, side < nlayer)

    @pl.when(inner)
    def _():
        greet(side, s)

    loads[0].wait()
    for k in range(planes):
        gbuf[k, rows(s, 0, width), :] = inv_ref[k].T
    for i, (source, sent, mine) in enumerate(
        ((rhs_ref, rsend, cols), (diag_ref, dsend, dcols))
    ):
        loads[i + 1].wait()
        for k in range(planes):
            sent[k] = source[k].T
        for k in range(planes):
            mine[k, :, lanes(s)] = sent[k, lines_of(s), :]

    pl.semaphore_wait(barrier, 2 * nsplit - 1 + nchip - 1 + jnp.where(inner, 1, 0))

    def remote(src, dst, send, recv, l, t):
        return pltpu.make_async_remote_copy(
            src_ref=src, dst_ref=dst, send_sem=send, recv_sem=recv,
            device_id=(l, t), device_id_type=MESH,
        )

    def regroup(n, d):
        t = lax.rem(s + d, nsplit)
        sent, mine = ((rsend, cols), (dsend, dcols))[n]
        return remote(
            sent.at[:, lines_of(t), :], mine.at[:, :, lanes(s)],
            rs_send.at[n, d - 1], rs_recv.at[n, d - 1], layer, t,
        )

    def spread(n, d):
        t = lax.rem(s + d, nsplit)
        return remote(
            (dirb, imb, aimb, arb)[n].at[:, :, lanes(t)], lines.at[n, :, lines_of(s), :],
            l_send.at[n, d - 1], l_recv.at[n, d - 1], layer, t,
        )

    def spread_start(n, distances=None):
        for d in range(1, nsplit) if distances is None else distances:
            spread(n, d).start()
        if distances is not None and 1 not in distances:
            return
        for k in range(planes):
            lines[n, k, lines_of(s), :] = (dirb, imb, aimb, arb)[n][k, :, lanes(s)]

    def spread_finish(n):
        for d in range(1, nsplit):
            spread(n, d).wait_recv()
        for k in range(planes):
            flat[n, k] = lines[n, k].T

    def halo(n, i):
        values = (cols, dirb, imb)[n]
        src = (values.at[planes - 1], values.at[0], edges.at[n, 0], edges.at[n, 1])[i]
        dst = (zlow, zhigh, ylow, yhigh)[i].at[n]
        l, t = ((layer + 1, s), (layer - 1, s), (layer, s + 1), (layer, s - 1))[i]
        return remote(src, dst, h_send.at[n, i], h_recv.at[n, i], l, t)

    to_high, to_low = layer < nlayer - 1, layer > 0
    to_right, to_left = s < nsplit - 1, s > 0
    gives = (to_high, to_low, to_right, to_left)
    takes = (to_low, to_high, to_left, to_right)

    def halo_start(n):
        values = (cols, dirb, imb)[n]
        for i in range(2):
            pl.when(gives[i])(lambda i=i: halo(n, i).start())
        for k in range(planes):
            edges[n, 0, k : k + 1, :] = values[k, yb - 1 : yb, :]
            edges[n, 1, k : k + 1, :] = values[k, 0:1, :]
        for i in range(2, 4):
            pl.when(gives[i])(lambda i=i: halo(n, i).start())

    def halo_wait(n):
        for i in range(4):
            pl.when(takes[i])(lambda i=i: halo(n, i).wait_recv())

    row = lax.broadcasted_iota(jnp.int32, (yb, nx), 0)
    lane = lax.broadcasted_iota(jnp.int32, (yb, nx), 1)

    def apply_operator(n, result):
        values = (cols, dirb, imb)[n]
        for k in range(planes):
            v = values[k]
            below = values[k - 1] if k > 0 else zlow[n]
            above = values[k + 1] if k < planes - 1 else zhigh[n]
            x_low = jnp.where(lane == 0, 0.0, pltpu.roll(v, 1, 1))
            x_high = jnp.where(lane == nx - 1, 0.0, pltpu.roll(v, nx - 1, 1))
            y_low = jnp.where(row == 0, ylow[n, k : k + 1, :], pltpu.roll(v, 1, 0))
            y_high = jnp.where(row == yb - 1, yhigh[n, k : k + 1, :], pltpu.roll(v, yb - 1, 0))
            beside = (below + above) + (x_low + x_high) + (y_low + y_high)
            result[k] = (6.0 + dcols[k]) * v - beside

    def put_sum(i, a, b):
        total = a[0] * b[0]
        for k in range(1, planes):
            total = total + a[k] * b[k]
        total = jnp.sum(total, axis=0, keepdims=True)
        lane_sum = total[:, :width]
        for t in range(1, nsplit):
            lane_sum = lane_sum + total[:, t * width : (t + 1) * width]
        part[i : i + 1, :] = lane_sum

    def prepare():
        for d in range(1, nsplit):
            regroup(1, d).wait_recv()
        halo_wait(0)
        apply_operator(0, arb)
        put_sum(0, cols, cols)
        put_sum(1, arb, cols)
        put_sum(2, arb, arb)

    def own_right(k):
        part = gbuf.at[k, rows(s, 0, width), :]
        return remote(part, part, g_send.at[0, k], g_recv.at[0, k], layer, right)

    def own_left(k):
        part = gbuf.at[k, rows(s, 0, width), :]
        return remote(part, part, g_send.at[1, k], g_recv.at[1, k], layer, left)

    def pass_right(k):
        part = gbuf.at[k, rows(left, 0, half), :]
        return remote(part, part, g_send.at[2, k], g_recv.at[2, k], layer, right)

    def pass_left(k):
        part = gbuf.at[k, rows(right, half, half), :]
        return remote(part, part, g_send.at[3, k], g_recv.at[3, k], layer, left)

    for d in range(1, nsplit):
        regroup(0, d).start()
    for k in range(min(2, planes)):
        own_right(k).start()
        own_left(k).start()

    def relay(k):
        own_right(k).wait_recv()
        pass_right(k).start()
        own_left(k).wait_recv()
        pass_left(k).start()
        if k + 2 < planes:
            own_right(k + 2).start()
            own_left(k + 2).start()
        if k == planes - 1:
            for d in range(1, nsplit):
                regroup(1, d).start()

    def absorb(k):
        pass_right(k).wait_recv()
        pass_left(k).wait_recv()
        full = gbuf[k]
        high, lowpart = split2(full)
        mats[k, 0] = high
        mats[k, 1] = lowpart
        if k == 0:
            for d in range(1, nsplit):
                regroup(0, d).wait_recv()
            halo_start(0)
            cvec[...] = mm(cols[0], high, lowpart)
            pf[...] = full
            qown[0] = high
            qown[1] = lowpart
        else:
            prefix[k - 1] = pf[...]
            pf[...] = mm(pf[...], high, lowpart)
            if k == planes - 1:
                pl.when(core == 1)(lambda: give_p.start())
            cvec[...] = mm(cols[k] + cvec[...], high, lowpart)

    def absorb_up(k):
        if k > 0:
            qf[...] = mm(gbuf[k], qown[0], qown[1])
            store_pair(qown, qf[...])

    give_p = remote(pf, pin, c_send.at[0], c_recv.at[0], other, s)
    for k in range(planes):
        relay(k)
        if k > 0:
            absorb(k - 1)
            absorb_up(k - 1)
    absorb(planes - 1)

    give_q = remote(qf, qin, c_send.at[1], c_recv.at[1], other, s)
    give_c = remote(cvec, cin, c_send.at[2], c_recv.at[2], other, s)
    give_a = remote(amid, ain, c_send.at[3], c_recv.at[3], other, s)
    give_e = remote(evec, ein, c_send.at[4], c_recv.at[4], other, s)
    give_b = remote(bin_, bcore, c_send.at[5], c_recv.at[5], other, s)
    give_r = remote(rf, rin, c_send.at[6], c_recv.at[6], other, s)
    give_a0 = remote(cvec, azero, c_send.at[7], c_recv.at[7], other, s)
    give_e0 = remote(ezero, ein0, c_send.at[8], c_recv.at[8], other, s)

    hosts = (npos - 1, 0)

    def row_layer(at):
        return 2 * (line * npos + at)

    def chunk(q):
        return pl.ds(q * cb, cb)

    def shared(step):
        return (0, width) if step == 1 else (nx - nx // 4, width // 4)

    def hand_share(way, step):
        base, size = shared(step)
        part = pl.ds(pl.multiple_of(base + s * size, size), size)
        return remote(
            xf.at[way, part, :], mbuf.at[step, part, :],
            x_send.at[way, 0], x_recv.at[step, 0], row_layer(hosts[way]), s,
        )

    def hand_whole(way, step):
        part = pl.ds(0, nx - nx // 4)
        return remote(
            xf.at[way, part, :], mbuf.at[step, part, :],
            x_send.at[way, 1], x_recv.at[step, 1], row_layer(hosts[way]), s,
        )

    def hand_wholes(way, do):
        for step in (0, 2):
            at = step if way == 0 else npos - 1 - step
            pl.when(pos == at)(functools.partial(do, step))

    def hand_vector(way, step):
        return remote(
            vown.at[way], vbuf.at[step], v_send.at[way], v_recv.at[step],
            row_layer(hosts[way]), s,
        )

    def hand_input(way, step):
        return remote(
            inbuf.at[step], (ain, bin_)[way], i_send.at[step], i_recv.at[way],
            row_layer(step if way == 0 else npos - 1 - step), s,
        )

    def hand_on(way, q):
        return remote(
            zout.at[chunk(q), :], zin.at[chunk(q), :], z_send.at[q], z_recv.at[q],
            layer + (2 - 4 * way) * npos, s,
        )

    def ring(step, i):
        base, size = shared(step)
        owner, start, length = (
            (s, 0, size), (s, 0, size), (left, 0, size // 2), (right, size // 2, size // 2)
        )[i]
        rows_at = pl.multiple_of(base + owner * size + start, size // 2)
        part = mbuf.at[step, pl.ds(rows_at, length), :]
        return remote(
            part, part, y_send.at[step, i], y_recv.at[step, i], layer,
            (right, left, right, left)[i],
        )

    def for_step(way, do):
        for step in range(npos - 1):
            at = step if way == 0 else npos - 1 - step
            pl.when(pos == at)(functools.partial(do, step))

    def row_vector(way):
        own = pall if way == 0 else qall
        for step in range(npos - 1):
            hand_vector(way, step).wait_recv()
        total = vbuf[0]
        for step in range(1, npos - 1):
            total = vbuf[step] + mm_ref(total, xpair.at[step])
        zout[...] = vown[way] + mm_ref(total, own)

    def line_starts(way):
        return line == 0 if way == 0 else line == nline - 1

    def line_ends(way):
        return line == nline - 1 if way == 0 else line == 0

    def send_first(way):
        for q in range(nchunk):
            hand_on(way, q).start()

    def host_prepare(way, meanwhile):
        own = pall if way == 0 else qall
        store_pair(own, xf[way])
        order = (1, 2, 0)
        for step in order:
            hand_share(way, step).wait_recv()
            ring(step, 0).start()
            ring(step, 1).start()
        meanwhile()
        for step in order:
            ring(step, 0).wait_recv()
            ring(step, 2).start()
            ring(step, 1).wait_recv()
            ring(step, 3).start()
        starts = line_starts(way)
        upper, lower = pl.ds(0, nx - nx // 4), pl.ds(nx - nx // 4, nx // 4)

        def passed(step):
            ring(step, 2).wait_recv()
            ring(step, 3).wait_recv()

        def ahead_of_rest(part):
            pin[part, :] = mm_ref(mbuf[2, part, :], own)

        hand_whole(way, 2).wait_recv()
        pl.when(jnp.logical_not(starts))(functools.partial(ahead_of_rest, upper))
        passed(1)
        store_pair(xpair.at[1], mbuf[1])
        passed(2)
        store_pair(xpair.at[2], mbuf[2])
        if way == 0:
            row_vector(way)
            if nline > 1:
                pl.when(starts)(functools.partial(send_first, way))
        hand_whole(way, 0).wait_recv()

        @pl.when(jnp.logical_not(starts))
        def _():
            pf[upper, :] = mm_ref(mbuf[0, upper, :], xpair.at[1])
            ahead_of_rest(lower)
            store_pair(xrow, pin[...])

        passed(0)

        @pl.when(jnp.logical_not(starts))
        def _():
            pf[lower, :] = mm_ref(mbuf[0, lower, :], xpair.at[1])
            store_pair(xrow, mm_ref(pf[...], xrow))

        store_pair(xpair.at[0], mbuf[0])

    def host_chain(way):
        starts, ends = line_starts(way), line_ends(way)
        if way == 1:
            row_vector(way)

        @pl.when(starts)
        def _():
            inbuf[0] = jnp.zeros((yb, nx), F32)
            if way == 1 and nline > 1:
                send_first(way)

        @pl.when(jnp.logical_not(starts))
        def _():
            for q in range(nchunk):
                hand_on(way, q).wait_recv()

                @pl.when(jnp.logical_not(ends))
                def _():
                    zout[chunk(q), :] = zout[chunk(q), :] + mm_ref(zin[chunk(q), :], xrow)
                    hand_on(way, q).start()

            inbuf[0] = zin[...]

        state = inbuf[0]
        for step in range(npos - 1):
            hand_input(way, step).start()
            state = vbuf[step] + mm_ref(state, xpair.at[step])
            if step < npos - 2:
                inbuf[step + 1] = state
        (ain, bin_)[way][...] = state

    def host_finish(way):
        ends = line_ends(way)
        for step in range(npos - 1):
            hand_input(way, step).wait_send()
        for step in range(npos - 1):
            for i in range(4):
                ring(step, i).wait_send()

        @pl.when(jnp.logical_not(ends))
        def _():
            for q in range(nchunk):
                hand_on(way, q).wait_send()

    @pl.when(core == 1)
    def _():
        give_c.start()
        absorb_up(planes - 1)

    def down_sweep(state):
        for k in range(planes):
            state = mm(cols[k] + state, mats[k, 0], mats[k, 1])
            low[k] = state

    def up_partial(result):
        state = low[planes - 1]
        for k in range(planes - 2, -1, -1):
            state = low[k] + mm(state, mats[k, 0], mats[k, 1])
        result[...] = state

    def response():
        rf[...] = prefix[planes - 2] + mm(pf[...], mats[planes - 2, 0], mats[planes - 2, 1])
        for k in range(planes - 3, -1, -1):
            rf[...] = prefix[k] + mm(rf[...], mats[k, 0], mats[k, 1])

    def up_sweep(state):
        for k in range(planes - 1, -1, -1):
            state = low[k] + mm(state, mats[k, 0], mats[k, 1])
            dirb[k] = state

    @pl.when(core == 1)
    def _():
        give_q.start()
        response()
        give_r.start()
        give_a0.wait_recv()
        down_sweep(azero[...])
        up_partial(ezero)
        give_e0.start()
        prepare()
        give_a.wait_recv()
        down_sweep(ain[...])
        up_partial(evec)
        give_e.start()
        spread_start(3)
        give_b.wait_recv()
        up_sweep(bcore[...])
        for give in (give_c, give_p, give_q, give_r, give_e0, give_e):
            give.wait_send()

    @pl.when(core == 0)
    def _():
        give_a0.start()
        store_pair(pown, pf[...])
        give_p.wait_recv()
        store_pair(pall, pin[...])
        xf[0] = mm_pairs(pown, pall)
        for_step(0, lambda step: hand_share(0, step).start())
        give_c.wait_recv()
        vown[0] = mm_ref(cvec[...], pall) + cin[...]
        for_step(0, lambda step: hand_vector(0, step).start())
        absorb_up(planes - 1)
        give_q.wait_recv()
        store_pair(q1, qin[...])
        xf[1] = mm_pairs(q1, qown)
        for_step(1, lambda step: hand_share(1, step).start())
        hand_wholes(0, lambda step: hand_whole(0, step).start())
        hand_wholes(1, lambda step: hand_whole(1, step).start())
        prepare()

        response()

        def still():
            give_r.wait_recv()
            store_pair(rpair, rin[...])
            rin[...] = mm_pairs(pown, rpair)
            rf[...] = rf[...] + mm_ref(rin[...], qown)
            store_pair(rpair, rf[...])
            down_sweep(jnp.zeros((yb, nx), F32))
            up_partial(ezero)
            give_e0.wait_recv()
            ezero[...] = ezero[...] + mm_ref(ein0[...], qown)

        @pl.when(pos == hosts[0])
        def _():
            host_prepare(0, still)
            host_chain(0)

        @pl.when(pos == hosts[1])
        def _():
            host_prepare(1, still)

        @pl.when(jnp.logical_and(pos != hosts[0], pos != hosts[1]))
        def _():
            still()

        for_step(0, lambda step: hand_input(0, step).wait_recv())
        vown[1] = ezero[...] + mm_ref(ain[...], rpair)
        for_step(1, lambda step: hand_vector(1, step).start())
        amid[...] = cvec[...] + mm_ref(ain[...], pown)
        give_a.start()
        spread_start(3)
        down_sweep(ain[...])

        @pl.when(pos == hosts[1])
        def _():
            host_chain(1)

        give_e.wait_recv()
        for_step(1, lambda step: hand_input(1, step).wait_recv())
        give_b.start()
        up_sweep(ein[...] + mm_ref(bin_[...], q1))
        give_a0.wait_send()
        give_a.wait_send()
        give_b.wait_send()
        for way in range(2):
            for_step(way, lambda step, way=way: hand_vector(way, step).wait_send())
            for_step(way, lambda step, way=way: hand_share(way, step).wait_send())
            hand_wholes(way, lambda step, way=way: hand_whole(way, step).wait_send())
            pl.when(pos == hosts[way])(functools.partial(host_finish, way))

    halo_start(1)
    spread_start(0)
    halo_wait(1)
    apply_operator(1, imb)
    halo_start(2)
    spread_start(1, (1, nsplit - 1))
    halo_wait(2)
    apply_operator(2, aimb)
    put_sum(3, cols, imb)
    put_sum(4, arb, imb)
    put_sum(5, aimb, cols)
    put_sum(6, aimb, imb)
    put_sum(7, arb, aimb)
    put_sum(8, aimb, aimb)

    place = core * nsplit + s
    count = 2 * nsplit

    def near(d):
        at = lax.rem(place + d, count)
        return remote(
            group.at[place], group.at[place], n_send.at[d - 1], n_recv.at[d - 1],
            2 * chip + at // nsplit, lax.rem(at, nsplit),
        )

    def far(d):
        at = lax.rem(chip + d, nchip)
        return remote(
            whole.at[chip], whole.at[chip], w_send.at[d - 1], w_recv.at[d - 1],
            2 * at + core, s,
        )

    diagonal = lax.broadcasted_iota(jnp.int32, (nrow, width), 0) == lax.broadcasted_iota(
        jnp.int32, (nrow, width), 1
    )
    sums = jnp.where(diagonal, jnp.sum(part[...], axis=1, keepdims=True), 0.0)
    group[place] = jnp.sum(sums, axis=0, keepdims=True)
    for d in range(1, count):
        near(d).start()
    spread_start(1, range(2, nsplit - 1))
    spread_start(2)
    for n in (3, 0):
        spread_finish(n)
    for d in range(1, count):
        near(d).wait_recv()
    total = group[0]
    for i in range(1, count):
        total = total + group[i]
    whole[chip] = total
    for d in range(1, nchip):
        far(d).start()
    for n in (1, 2):
        spread_finish(n)
    for d in range(1, nchip):
        far(d).wait_recv()
    total = whole[0]
    for i in range(1, nchip):
        total = total + whole[i]
    rr, ar, aa, ri, ai, br, bi, ab, bb = [total[:, i : i + 1] for i in range(9)]
    alpha = rr / ri
    cross = ar - alpha * (ai + br) + alpha * alpha * bi
    own = aa - 2.0 * alpha * ab + alpha * alpha * bb
    omega = cross / own
    for k in range(planes):
        middle = rhs_ref[k] - alpha * flat[1, k]
        sol_ref[k] = alpha * flat[0, k] + omega * middle
        res_ref[k] = middle - omega * (flat[3, k] - alpha * flat[2, k])

    for n in range(2):
        for d in range(1, nsplit):
            regroup(n, d).wait_send()
    for k in range(planes):
        own_right(k).wait_send()
        own_left(k).wait_send()
        pass_right(k).wait_send()
        pass_left(k).wait_send()
    for n in range(4):
        for d in range(1, nsplit):
            spread(n, d).wait_send()
    for n in range(3):
        for i in range(4):
            pl.when(gives[i])(lambda n=n, i=i: halo(n, i).wait_send())
    for d in range(1, count):
        near(d).wait_send()
    for d in range(1, nchip):
        far(d).wait_send()


def per_device(nlayer, nsplit, right_side, diagonal, inverses):
    planes, nx, width = inverses.shape
    ysize = right_side.shape[2]
    yb = ysize // nsplit
    nchip = nlayer // 2
    nchunk = 2
    nrow = 16
    vmem = pl.BlockSpec(memory_space=pltpu.VMEM)
    square = pltpu.VMEM((nx, nx), F32)
    pair = pltpu.VMEM((2, nx, nx), BF16)
    strip = pltpu.VMEM((yb, nx), F32)
    columns = pltpu.VMEM((planes, yb, nx), F32)
    block = pltpu.VMEM((planes, ysize, width), F32)
    dma = pltpu.SemaphoreType.DMA
    shape = jax.ShapeDtypeStruct((planes, width, ysize), F32)
    return pl.pallas_call(
        functools.partial(sweep_kernel, nlayer, nsplit, nchunk, nrow),
        out_shape=(shape, shape),
        in_specs=[pl.BlockSpec(memory_space=pltpu.HBM)] * 3,
        out_specs=(vmem, vmem),
        scratch_shapes=[
            pltpu.VMEM((planes, nx, nx), F32),
            pltpu.VMEM((planes, 2, nx, nx), BF16),
            block, block,
            columns, columns, columns, columns, columns, columns, columns,
            square, square, pair, pair, pair, pair, pair, square, square,
            strip, strip, strip, strip, strip, strip, strip, strip, strip, strip,
            pltpu.VMEM((2, nx, nx), F32), pltpu.VMEM((3, nx, nx), F32),
            pltpu.VMEM((3, 2, nx, nx), BF16), pair,
            pltpu.VMEM((2, yb, nx), F32), pltpu.VMEM((3, yb, nx), F32),
            pltpu.VMEM((3, yb, nx), F32),
            pltpu.VMEM((planes - 1, nx, nx), F32), square, square, pair, strip, strip, strip,
            pltpu.VMEM((3, yb, nx), F32), pltpu.VMEM((3, yb, nx), F32),
            pltpu.VMEM((3, 8, nx), F32), pltpu.VMEM((3, 8, nx), F32),
            pltpu.VMEM((3, 2, 8, nx), F32),
            pltpu.VMEM((4, planes, ysize, width), F32),
            pltpu.VMEM((4, planes, width, ysize), F32),
            pltpu.VMEM((nrow, width), F32),
            pltpu.VMEM((2 * nsplit, 1, width), F32),
            pltpu.VMEM((nchip, 1, width), F32),
            pltpu.VMEM((planes, width, ysize), F32), pltpu.VMEM((planes, width, ysize), F32),
            pltpu.VMEM((planes, nx, width), F32), dma((3,)),
            dma((2, nsplit - 1)), dma((2, nsplit - 1)),
            dma((4, planes)), dma((4, planes)),
            dma((9,)), dma((9,)),
            dma((2, 2)), dma((3, 2)), dma((2,)), dma((3,)), dma((3,)), dma((2,)),
            dma((nchunk,)), dma((nchunk,)), dma((3, 4)), dma((3, 4)),
            dma((3, 4)), dma((3, 4)),
            dma((4, nsplit - 1)), dma((4, nsplit - 1)),
            dma((2 * nsplit - 1,)), dma((2 * nsplit - 1,)),
            dma((nchip - 1,)), dma((nchip - 1,)),
        ],
        compiler_params=pltpu.CompilerParams(
            collective_id=0, has_side_effects=True, vmem_limit_bytes=56 * 1024 * 1024
        ),
        name="sweeps",
    )(right_side, diagonal, inverses)


def solution(mesh):
    spec = P("layer", "split", None)
    return jax.shard_map(
        functools.partial(per_device, mesh.shape["layer"], mesh.shape["split"]),
        mesh=mesh,
        in_specs=(spec, spec, P("layer", None, "split")),
        out_specs=(spec, spec),
        check_vma=False,
    )
```

```python
import functools

import jax
import jax.numpy as jnp
from jax import lax
from jax.experimental import pallas as pl
from jax.experimental.pallas import tpu as pltpu
from jax.sharding import PartitionSpec as P

MESH = pl.DeviceIdType.MESH
F32 = jnp.float32
BF16 = jnp.bfloat16


def split2(x):
    high = x.astype(BF16)
    return high, (x - high.astype(F32)).astype(BF16)


def mm(x, w_high, w_low):
    high, low = split2(x)
    dot = functools.partial(jnp.dot, preferred_element_type=F32)
    n = x.shape[0]
    if n > 128:
        return dot(high, w_high) + (dot(low, w_high) + dot(high, w_low))
    both = dot(jnp.concatenate([high, low], 0), w_high)
    return both[:n] + (both[n:] + dot(high, w_low))


def mm_ref(x, pair):
    return mm(x, pair[0], pair[1])


def mm_pairs(x, pair):
    dot = functools.partial(jnp.dot, preferred_element_type=F32)
    return dot(x[0], pair[0]) + (dot(x[1], pair[0]) + dot(x[0], pair[1]))


def store_pair(pair, x):
    high, low = split2(x)
    pair[0] = high
    pair[1] = low


def sweep_kernel(
    nlayer, nsplit, nchunk, nrow,
    rhs_in, diag_in, inv_in, sol_ref, res_ref,
    gbuf, mats, rsend, dsend, cols, dcols, low, dirb, imb, aimb, arb,
    pf, qf, pown, qown, pall, qall, q1, pin, qin,
    cvec, cin, ain, amid, evec, ein, bin_, bcore, zin, zout,
    xf, mbuf, xpair, xrow, vown, vbuf, inbuf,
    prefix, rf, rin, rpair, azero, ezero, ein0,
    zlow, zhigh, ylow, yhigh, edges, lines, flat, part, group, whole,
    rhs_ref, diag_ref, inv_ref, in_sem,
    rs_send, rs_recv, g_send, g_recv, c_send, c_recv,
    x_send, x_recv, v_send, v_recv, i_send, i_recv, z_send, z_recv, y_send, y_recv,
    h_send, h_recv, l_send, l_recv, n_send, n_recv, w_send, w_recv,
):
    planes, nx, width = inv_in.shape
    ysize = rhs_in.shape[2]
    yb = ysize // nsplit
    cb = yb // nchunk
    half = width // 2
    layer = lax.axis_index("layer")
    s = lax.axis_index("split")
    core = lax.rem(layer, 2)
    chip = layer // 2
    nchip = nlayer // 2
    right = lax.rem(s + 1, nsplit)
    left = lax.rem(s + nsplit - 1, nsplit)
    other = layer + 1 - 2 * core
    npos = 4
    pos, line = lax.rem(chip, npos), chip // npos
    nline = nchip // npos

    def rows(owner, start, size):
        return pl.ds(pl.multiple_of(owner * width + start, half), size)

    def lanes(t):
        return pl.ds(pl.multiple_of(t * width, width), width)

    def lines_of(t):
        return pl.ds(pl.multiple_of(t * yb, yb), yb)

    loads = [
        pltpu.make_async_copy(src, dst, in_sem.at[i])
        for i, (src, dst) in enumerate(
            ((inv_in, inv_ref), (rhs_in, rhs_ref), (diag_in, diag_ref))
        )
    ]
    for load in loads:
        load.start()
    for empty in (zlow, zhigh, ylow, yhigh, edges, part):
        empty[...] = jnp.zeros_like(empty)

    barrier = pltpu.get_barrier_semaphore()

    def greet(l, t):
        pl.semaphore_signal(barrier, inc=1, device_id=(l, t), device_id_type=MESH)

    for d in range(1, nsplit):
        greet(layer, lax.rem(s + d, nsplit))
    for d in range(nsplit):
        greet(other, lax.rem(s + d, nsplit))
    for d in range(1, nchip):
        greet(2 * lax.rem(chip + d, nchip) + core, s)
    side = layer - 1 + 2 * core
    inner = jnp.logical_and(side >= 0, side < nlayer)

    @pl.when(inner)
    def _():
        greet(side, s)

    loads[0].wait()
    for k in range(planes):
        gbuf[k, rows(s, 0, width), :] = inv_ref[k].T
    for i, (source, sent, mine) in enumerate(
        ((rhs_ref, rsend, cols), (diag_ref, dsend, dcols))
    ):
        loads[i + 1].wait()
        for k in range(planes):
            sent[k] = source[k].T
        for k in range(planes):
            mine[k, :, lanes(s)] = sent[k, lines_of(s), :]

    pl.semaphore_wait(barrier, 2 * nsplit - 1 + nchip - 1 + jnp.where(inner, 1, 0))

    def remote(src, dst, send, recv, l, t):
        return pltpu.make_async_remote_copy(
            src_ref=src, dst_ref=dst, send_sem=send, recv_sem=recv,
            device_id=(l, t), device_id_type=MESH,
        )

    def regroup(n, d):
        t = lax.rem(s + d, nsplit)
        sent, mine = ((rsend, cols), (dsend, dcols))[n]
        return remote(
            sent.at[:, lines_of(t), :], mine.at[:, :, lanes(s)],
            rs_send.at[n, d - 1], rs_recv.at[n, d - 1], layer, t,
        )

    def spread(n, d):
        t = lax.rem(s + d, nsplit)
        return remote(
            (dirb, imb, aimb, arb)[n].at[:, :, lanes(t)], lines.at[n, :, lines_of(s), :],
            l_send.at[n, d - 1], l_recv.at[n, d - 1], layer, t,
        )

    def spread_start(n, distances=None):
        for d in range(1, nsplit) if distances is None else distances:
            spread(n, d).start()
        if distances is not None and 1 not in distances:
            return
        for k in range(planes):
            lines[n, k, lines_of(s), :] = (dirb, imb, aimb, arb)[n][k, :, lanes(s)]

    def spread_finish(n):
        for d in range(1, nsplit):
            spread(n, d).wait_recv()
        for k in range(planes):
            flat[n, k] = lines[n, k].T

    def halo(n, i):
        values = (cols, dirb, imb)[n]
        src = (values.at[planes - 1], values.at[0], edges.at[n, 0], edges.at[n, 1])[i]
        dst = (zlow, zhigh, ylow, yhigh)[i].at[n]
        l, t = ((layer + 1, s), (layer - 1, s), (layer, s + 1), (layer, s - 1))[i]
        return remote(src, dst, h_send.at[n, i], h_recv.at[n, i], l, t)

    to_high, to_low = layer < nlayer - 1, layer > 0
    to_right, to_left = s < nsplit - 1, s > 0
    gives = (to_high, to_low, to_right, to_left)
    takes = (to_low, to_high, to_left, to_right)

    def halo_start(n):
        values = (cols, dirb, imb)[n]
        for i in range(2):
            pl.when(gives[i])(lambda i=i: halo(n, i).start())
        for k in range(planes):
            edges[n, 0, k : k + 1, :] = values[k, yb - 1 : yb, :]
            edges[n, 1, k : k + 1, :] = values[k, 0:1, :]
        for i in range(2, 4):
            pl.when(gives[i])(lambda i=i: halo(n, i).start())

    def halo_wait(n):
        for i in range(4):
            pl.when(takes[i])(lambda i=i: halo(n, i).wait_recv())

    row = lax.broadcasted_iota(jnp.int32, (yb, nx), 0)
    lane = lax.broadcasted_iota(jnp.int32, (yb, nx), 1)

    def apply_operator(n, result):
        values = (cols, dirb, imb)[n]
        for k in range(planes):
            v = values[k]
            below = values[k - 1] if k > 0 else zlow[n]
            above = values[k + 1] if k < planes - 1 else zhigh[n]
            x_low = jnp.where(lane == 0, 0.0, pltpu.roll(v, 1, 1))
            x_high = jnp.where(lane == nx - 1, 0.0, pltpu.roll(v, nx - 1, 1))
            y_low = jnp.where(row == 0, ylow[n, k : k + 1, :], pltpu.roll(v, 1, 0))
            y_high = jnp.where(row == yb - 1, yhigh[n, k : k + 1, :], pltpu.roll(v, yb - 1, 0))
            beside = (below + above) + (x_low + x_high) + (y_low + y_high)
            result[k] = (6.0 + dcols[k]) * v - beside

    def put_sum(i, a, b):
        total = a[0] * b[0]
        for k in range(1, planes):
            total = total + a[k] * b[k]
        total = jnp.sum(total, axis=0, keepdims=True)
        lane_sum = total[:, :width]
        for t in range(1, nsplit):
            lane_sum = lane_sum + total[:, t * width : (t + 1) * width]
        part[i : i + 1, :] = lane_sum

    def prepare():
        for d in range(1, nsplit):
            regroup(1, d).wait_recv()
        halo_wait(0)
        apply_operator(0, arb)
        put_sum(0, cols, cols)
        put_sum(1, arb, cols)
        put_sum(2, arb, arb)

    def own_right(k):
        part = gbuf.at[k, rows(s, 0, width), :]
        return remote(part, part, g_send.at[0, k], g_recv.at[0, k], layer, right)

    def own_left(k):
        part = gbuf.at[k, rows(s, 0, width), :]
        return remote(part, part, g_send.at[1, k], g_recv.at[1, k], layer, left)

    def pass_right(k):
        part = gbuf.at[k, rows(left, 0, half), :]
        return remote(part, part, g_send.at[2, k], g_recv.at[2, k], layer, right)

    def pass_left(k):
        part = gbuf.at[k, rows(right, half, half), :]
        return remote(part, part, g_send.at[3, k], g_recv.at[3, k], layer, left)

    for d in range(1, nsplit):
        regroup(0, d).start()
    for k in range(min(2, planes)):
        own_right(k).start()
        own_left(k).start()

    def relay(k):
        own_right(k).wait_recv()
        pass_right(k).start()
        own_left(k).wait_recv()
        pass_left(k).start()
        if k + 2 < planes:
            own_right(k + 2).start()
            own_left(k + 2).start()
        if k == planes - 1:
            for d in range(1, nsplit):
                regroup(1, d).start()

    def absorb(k):
        pass_right(k).wait_recv()
        pass_left(k).wait_recv()
        full = gbuf[k]
        high, lowpart = split2(full)
        mats[k, 0] = high
        mats[k, 1] = lowpart
        if k == 0:
            for d in range(1, nsplit):
                regroup(0, d).wait_recv()
            halo_start(0)
            cvec[...] = mm(cols[0], high, lowpart)
            pf[...] = full
            qown[0] = high
            qown[1] = lowpart
        else:
            prefix[k - 1] = pf[...]
            pf[...] = mm(pf[...], high, lowpart)
            if k == planes - 1:
                pl.when(core == 1)(lambda: give_p.start())
            cvec[...] = mm(cols[k] + cvec[...], high, lowpart)

    def absorb_up(k):
        if k > 0:
            qf[...] = mm(gbuf[k], qown[0], qown[1])
            store_pair(qown, qf[...])

    give_p = remote(pf, pin, c_send.at[0], c_recv.at[0], other, s)
    for k in range(planes):
        relay(k)
        if k > 0:
            absorb(k - 1)
            absorb_up(k - 1)
    absorb(planes - 1)

    give_q = remote(qf, qin, c_send.at[1], c_recv.at[1], other, s)
    give_c = remote(cvec, cin, c_send.at[2], c_recv.at[2], other, s)
    give_a = remote(amid, ain, c_send.at[3], c_recv.at[3], other, s)
    give_e = remote(evec, ein, c_send.at[4], c_recv.at[4], other, s)
    give_b = remote(bin_, bcore, c_send.at[5], c_recv.at[5], other, s)
    give_r = remote(rf, rin, c_send.at[6], c_recv.at[6], other, s)
    give_a0 = remote(cvec, azero, c_send.at[7], c_recv.at[7], other, s)
    give_e0 = remote(ezero, ein0, c_send.at[8], c_recv.at[8], other, s)

    hosts = (npos - 1, 0)

    def row_layer(at):
        return 2 * (line * npos + at)

    def chunk(q):
        return pl.ds(q * cb, cb)

    def shared(step):
        return (0, width) if step == 1 else (nx - nx // 4, width // 4)

    def hand_share(way, step, piece=0):
        base, size = shared(step)
        length = size // 2 if step == 1 else size
        part = pl.ds(pl.multiple_of(base + s * size + piece * length, length), length)
        return remote(
            xf.at[way, part, :], mbuf.at[step, part, :],
            x_send.at[way, 2 * piece], x_recv.at[step, 2 * piece], row_layer(hosts[way]), s,
        )

    def pieces(step):
        return (0, 1) if step == 1 else (0,)

    def shares_start(way, step):
        for piece in pieces(step):
            hand_share(way, step, piece).start()

    def shares_end(way, step):
        for piece in pieces(step):
            hand_share(way, step, piece).wait_send()

    def hand_whole(way, step):
        part = pl.ds(0, nx - nx // 4)
        return remote(
            xf.at[way, part, :], mbuf.at[step, part, :],
            x_send.at[way, 1], x_recv.at[step, 1], row_layer(hosts[way]), s,
        )

    def hand_wholes(way, do):
        for step in (0, 2):
            at = step if way == 0 else npos - 1 - step
            pl.when(pos == at)(functools.partial(do, step))

    def hand_vector(way, step):
        return remote(
            vown.at[way], vbuf.at[step], v_send.at[way], v_recv.at[step],
            row_layer(hosts[way]), s,
        )

    def hand_input(way, step):
        return remote(
            inbuf.at[step], (ain, bin_)[way], i_send.at[step], i_recv.at[way],
            row_layer(step if way == 0 else npos - 1 - step), s,
        )

    def hand_on(way, q):
        return remote(
            zout.at[chunk(q), :], zin.at[chunk(q), :], z_send.at[q], z_recv.at[q],
            layer + (2 - 4 * way) * npos, s,
        )

    def ring(step, i):
        base, size = shared(step)
        h = size // 2
        own = (s, 0, size)
        owner, start, length = (
            (s, 0, h) if step == 1 else own, (s, h, h) if step == 1 else own,
            (left, 0, h), (right, h, h), (s, h, h), (s, 0, h),
        )[i]
        rows_at = pl.multiple_of(base + owner * size + start, h)
        part = mbuf.at[step, pl.ds(rows_at, length), :]
        return remote(
            part, part, y_send.at[step, i], y_recv.at[step, i], layer,
            (right, left, right, left, right, left)[i],
        )

    def ring_copies(step):
        return range(6) if step == 1 else range(4)

    def for_step(way, do):
        for step in range(npos - 1):
            at = step if way == 0 else npos - 1 - step
            pl.when(pos == at)(functools.partial(do, step))

    def row_vector(way):
        own = pall if way == 0 else qall
        for step in range(npos - 1):
            hand_vector(way, step).wait_recv()
        total = vbuf[0]
        for step in range(1, npos - 1):
            total = vbuf[step] + mm_ref(total, xpair.at[step])
        zout[...] = vown[way] + mm_ref(total, own)

    def line_starts(way):
        return line == 0 if way == 0 else line == nline - 1

    def line_ends(way):
        return line == nline - 1 if way == 0 else line == 0

    def send_first(way):
        for q in range(nchunk):
            hand_on(way, q).start()

    def host_prepare(way, meanwhile):
        own = pall if way == 0 else qall
        store_pair(own, xf[way])
        order = (1, 2, 0)
        for step in order:
            hand_share(way, step).wait_recv()
            ring(step, 0).start()
            if step == 1:
                ring(step, 5).start()
                hand_share(way, step, 1).wait_recv()
                ring(step, 4).start()
            ring(step, 1).start()
        for step in order:
            ring(step, 0).wait_recv()
            ring(step, 2).start()
            ring(step, 1).wait_recv()
            ring(step, 3).start()
        meanwhile()
        starts = line_starts(way)
        upper, lower = pl.ds(0, nx - nx // 4), pl.ds(nx - nx // 4, nx // 4)

        def passed(step):
            for i in ring_copies(step)[2:]:
                ring(step, i).wait_recv()

        def ahead_of_rest(part):
            pin[part, :] = mm_ref(mbuf[2, part, :], own)

        hand_whole(way, 2).wait_recv()
        pl.when(jnp.logical_not(starts))(functools.partial(ahead_of_rest, upper))
        passed(1)
        store_pair(xpair.at[1], mbuf[1])
        passed(2)
        store_pair(xpair.at[2], mbuf[2])
        if way == 0:
            row_vector(way)
            if nline > 1:
                pl.when(starts)(functools.partial(send_first, way))
        hand_whole(way, 0).wait_recv()

        @pl.when(jnp.logical_not(starts))
        def _():
            pf[upper, :] = mm_ref(mbuf[0, upper, :], xpair.at[1])
            ahead_of_rest(lower)
            store_pair(xrow, pin[...])

        passed(0)

        @pl.when(jnp.logical_not(starts))
        def _():
            pf[lower, :] = mm_ref(mbuf[0, lower, :], xpair.at[1])
            store_pair(xrow, mm_ref(pf[...], xrow))

        store_pair(xpair.at[0], mbuf[0])

    def host_chain(way):
        starts, ends = line_starts(way), line_ends(way)
        if way == 1:
            row_vector(way)

        @pl.when(starts)
        def _():
            inbuf[0] = jnp.zeros((yb, nx), F32)
            if way == 1 and nline > 1:
                send_first(way)

        @pl.when(jnp.logical_not(starts))
        def _():
            for q in range(nchunk):
                hand_on(way, q).wait_recv()

                @pl.when(jnp.logical_not(ends))
                def _():
                    zout[chunk(q), :] = zout[chunk(q), :] + mm_ref(zin[chunk(q), :], xrow)
                    hand_on(way, q).start()

            inbuf[0] = zin[...]

        state = inbuf[0]
        for step in range(npos - 1):
            hand_input(way, step).start()
            state = vbuf[step] + mm_ref(state, xpair.at[step])
            if step < npos - 2:
                inbuf[step + 1] = state
        (ain, bin_)[way][...] = state

    def host_finish(way):
        ends = line_ends(way)
        for step in range(npos - 1):
            hand_input(way, step).wait_send()
        for step in range(npos - 1):
            for i in ring_copies(step):
                ring(step, i).wait_send()

        @pl.when(jnp.logical_not(ends))
        def _():
            for q in range(nchunk):
                hand_on(way, q).wait_send()

    @pl.when(core == 1)
    def _():
        give_c.start()
        absorb_up(planes - 1)

    def down_sweep(state):
        for k in range(planes):
            state = mm(cols[k] + state, mats[k, 0], mats[k, 1])
            low[k] = state

    def up_partial(result):
        state = low[planes - 1]
        for k in range(planes - 2, -1, -1):
            state = low[k] + mm(state, mats[k, 0], mats[k, 1])
        result[...] = state

    def response():
        rf[...] = prefix[planes - 2] + mm(pf[...], mats[planes - 2, 0], mats[planes - 2, 1])
        for k in range(planes - 3, -1, -1):
            rf[...] = prefix[k] + mm(rf[...], mats[k, 0], mats[k, 1])

    def up_sweep(state):
        for k in range(planes - 1, -1, -1):
            state = low[k] + mm(state, mats[k, 0], mats[k, 1])
            dirb[k] = state

    @pl.when(core == 1)
    def _():
        give_q.start()
        response()
        give_r.start()
        give_a0.wait_recv()
        down_sweep(azero[...])
        up_partial(ezero)
        give_e0.start()
        prepare()
        give_a.wait_recv()
        down_sweep(ain[...])
        up_partial(evec)
        give_e.start()
        spread_start(3)
        give_b.wait_recv()
        up_sweep(bcore[...])
        for give in (give_c, give_p, give_q, give_r, give_e0, give_e):
            give.wait_send()

    @pl.when(core == 0)
    def _():
        give_a0.start()
        store_pair(pown, pf[...])
        give_p.wait_recv()
        store_pair(pall, pin[...])
        xf[0] = mm_pairs(pown, pall)
        for_step(0, functools.partial(shares_start, 0))
        give_c.wait_recv()
        vown[0] = mm_ref(cvec[...], pall) + cin[...]
        for_step(0, lambda step: hand_vector(0, step).start())
        absorb_up(planes - 1)
        give_q.wait_recv()
        store_pair(q1, qin[...])
        xf[1] = mm_pairs(q1, qown)
        for_step(1, functools.partial(shares_start, 1))
        hand_wholes(0, lambda step: hand_whole(0, step).start())
        hand_wholes(1, lambda step: hand_whole(1, step).start())
        prepare()

        response()

        def still():
            give_r.wait_recv()
            store_pair(rpair, rin[...])
            rin[...] = mm_pairs(pown, rpair)
            rf[...] = rf[...] + mm_ref(rin[...], qown)
            store_pair(rpair, rf[...])
            down_sweep(jnp.zeros((yb, nx), F32))
            up_partial(ezero)
            give_e0.wait_recv()
            ezero[...] = ezero[...] + mm_ref(ein0[...], qown)

        @pl.when(pos == hosts[0])
        def _():
            host_prepare(0, still)
            host_chain(0)

        @pl.when(pos == hosts[1])
        def _():
            host_prepare(1, still)

        @pl.when(jnp.logical_and(pos != hosts[0], pos != hosts[1]))
        def _():
            still()

        for_step(0, lambda step: hand_input(0, step).wait_recv())
        vown[1] = ezero[...] + mm_ref(ain[...], rpair)
        for_step(1, lambda step: hand_vector(1, step).start())
        amid[...] = cvec[...] + mm_ref(ain[...], pown)
        give_a.start()
        spread_start(3)
        down_sweep(ain[...])

        @pl.when(pos == hosts[1])
        def _():
            host_chain(1)

        give_e.wait_recv()
        for_step(1, lambda step: hand_input(1, step).wait_recv())
        give_b.start()
        up_sweep(ein[...] + mm_ref(bin_[...], q1))
        give_a0.wait_send()
        give_a.wait_send()
        give_b.wait_send()
        for way in range(2):
            for_step(way, lambda step, way=way: hand_vector(way, step).wait_send())
            for_step(way, functools.partial(shares_end, way))
            hand_wholes(way, lambda step, way=way: hand_whole(way, step).wait_send())
            pl.when(pos == hosts[way])(functools.partial(host_finish, way))

    halo_start(1)
    spread_start(0)
    halo_wait(1)
    apply_operator(1, imb)
    halo_start(2)
    spread_start(1, (1, nsplit - 1))
    halo_wait(2)
    apply_operator(2, aimb)
    put_sum(3, cols, imb)
    put_sum(4, arb, imb)
    put_sum(5, aimb, cols)
    put_sum(6, aimb, imb)
    put_sum(7, arb, aimb)
    put_sum(8, aimb, aimb)

    place = core * nsplit + s
    count = 2 * nsplit

    def near(d):
        at = lax.rem(place + d, count)
        return remote(
            group.at[place], group.at[place], n_send.at[d - 1], n_recv.at[d - 1],
            2 * chip + at // nsplit, lax.rem(at, nsplit),
        )

    def far(d):
        at = lax.rem(chip + d, nchip)
        return remote(
            whole.at[chip], whole.at[chip], w_send.at[d - 1], w_recv.at[d - 1],
            2 * at + core, s,
        )

    diagonal = lax.broadcasted_iota(jnp.int32, (nrow, width), 0) == lax.broadcasted_iota(
        jnp.int32, (nrow, width), 1
    )
    sums = jnp.where(diagonal, jnp.sum(part[...], axis=1, keepdims=True), 0.0)
    group[place] = jnp.sum(sums, axis=0, keepdims=True)
    for d in range(1, count):
        near(d).start()
    spread_start(1, range(2, nsplit - 1))
    spread_start(2)
    for n in (3, 0):
        spread_finish(n)
    for d in range(1, count):
        near(d).wait_recv()
    total = group[0]
    for i in range(1, count):
        total = total + group[i]
    whole[chip] = total
    for d in range(1, nchip):
        far(d).start()
    for n in (1, 2):
        spread_finish(n)
    for d in range(1, nchip):
        far(d).wait_recv()
    total = whole[0]
    for i in range(1, nchip):
        total = total + whole[i]
    rr, ar, aa, ri, ai, br, bi, ab, bb = [total[:, i : i + 1] for i in range(9)]
    alpha = rr / ri
    cross = ar - alpha * (ai + br) + alpha * alpha * bi
    own = aa - 2.0 * alpha * ab + alpha * alpha * bb
    omega = cross / own
    for k in range(planes):
        middle = rhs_ref[k] - alpha * flat[1, k]
        sol_ref[k] = alpha * flat[0, k] + omega * middle
        res_ref[k] = middle - omega * (flat[3, k] - alpha * flat[2, k])

    for n in range(2):
        for d in range(1, nsplit):
            regroup(n, d).wait_send()
    for k in range(planes):
        own_right(k).wait_send()
        own_left(k).wait_send()
        pass_right(k).wait_send()
        pass_left(k).wait_send()
    for n in range(4):
        for d in range(1, nsplit):
            spread(n, d).wait_send()
    for n in range(3):
        for i in range(4):
            pl.when(gives[i])(lambda n=n, i=i: halo(n, i).wait_send())
    for d in range(1, count):
        near(d).wait_send()
    for d in range(1, nchip):
        far(d).wait_send()


def per_device(nlayer, nsplit, right_side, diagonal, inverses):
    planes, nx, width = inverses.shape
    ysize = right_side.shape[2]
    yb = ysize // nsplit
    nchip = nlayer // 2
    nchunk = 2
    nrow = 16
    vmem = pl.BlockSpec(memory_space=pltpu.VMEM)
    square = pltpu.VMEM((nx, nx), F32)
    pair = pltpu.VMEM((2, nx, nx), BF16)
    strip = pltpu.VMEM((yb, nx), F32)
    columns = pltpu.VMEM((planes, yb, nx), F32)
    block = pltpu.VMEM((planes, ysize, width), F32)
    dma = pltpu.SemaphoreType.DMA
    shape = jax.ShapeDtypeStruct((planes, width, ysize), F32)
    return pl.pallas_call(
        functools.partial(sweep_kernel, nlayer, nsplit, nchunk, nrow),
        out_shape=(shape, shape),
        in_specs=[pl.BlockSpec(memory_space=pltpu.HBM)] * 3,
        out_specs=(vmem, vmem),
        scratch_shapes=[
            pltpu.VMEM((planes, nx, nx), F32),
            pltpu.VMEM((planes, 2, nx, nx), BF16),
            block, block,
            columns, columns, columns, columns, columns, columns, columns,
            square, square, pair, pair, pair, pair, pair, square, square,
            strip, strip, strip, strip, strip, strip, strip, strip, strip, strip,
            pltpu.VMEM((2, nx, nx), F32), pltpu.VMEM((3, nx, nx), F32),
            pltpu.VMEM((3, 2, nx, nx), BF16), pair,
            pltpu.VMEM((2, yb, nx), F32), pltpu.VMEM((3, yb, nx), F32),
            pltpu.VMEM((3, yb, nx), F32),
            pltpu.VMEM((planes - 1, nx, nx), F32), square, square, pair, strip, strip, strip,
            pltpu.VMEM((3, yb, nx), F32), pltpu.VMEM((3, yb, nx), F32),
            pltpu.VMEM((3, 8, nx), F32), pltpu.VMEM((3, 8, nx), F32),
            pltpu.VMEM((3, 2, 8, nx), F32),
            pltpu.VMEM((4, planes, ysize, width), F32),
            pltpu.VMEM((4, planes, width, ysize), F32),
            pltpu.VMEM((nrow, width), F32),
            pltpu.VMEM((2 * nsplit, 1, width), F32),
            pltpu.VMEM((nchip, 1, width), F32),
            pltpu.VMEM((planes, width, ysize), F32), pltpu.VMEM((planes, width, ysize), F32),
            pltpu.VMEM((planes, nx, width), F32), dma((3,)),
            dma((2, nsplit - 1)), dma((2, nsplit - 1)),
            dma((4, planes)), dma((4, planes)),
            dma((9,)), dma((9,)),
            dma((2, 3)), dma((3, 3)), dma((2,)), dma((3,)), dma((3,)), dma((2,)),
            dma((nchunk,)), dma((nchunk,)), dma((3, 6)), dma((3, 6)),
            dma((3, 4)), dma((3, 4)),
            dma((4, nsplit - 1)), dma((4, nsplit - 1)),
            dma((2 * nsplit - 1,)), dma((2 * nsplit - 1,)),
            dma((nchip - 1,)), dma((nchip - 1,)),
        ],
        compiler_params=pltpu.CompilerParams(
            collective_id=0, has_side_effects=True, vmem_limit_bytes=56 * 1024 * 1024
        ),
        name="sweeps",
    )(right_side, diagonal, inverses)


def solution(mesh):
    spec = P("layer", "split", None)
    return jax.shard_map(
        functools.partial(per_device, mesh.shape["layer"], mesh.shape["split"]),
        mesh=mesh,
        in_specs=(spec, spec, P("layer", None, "split")),
        out_specs=(spec, spec),
        check_vma=False,
    )
```

```python
import functools

import jax
import jax.numpy as jnp
from jax import lax
from jax.experimental import pallas as pl
from jax.experimental.pallas import tpu as pltpu
from jax.sharding import PartitionSpec as P

MESH = pl.DeviceIdType.MESH
F32 = jnp.float32
BF16 = jnp.bfloat16


def split2(x):
    high = x.astype(BF16)
    return high, (x - high.astype(F32)).astype(BF16)


def mm(x, w_high, w_low):
    high, low = split2(x)
    dot = functools.partial(jnp.dot, preferred_element_type=F32)
    n = x.shape[0]
    if n > 128:
        return dot(high, w_high) + (dot(low, w_high) + dot(high, w_low))
    both = dot(jnp.concatenate([high, low], 0), w_high)
    return both[:n] + (both[n:] + dot(high, w_low))


def mm_ref(x, pair):
    return mm(x, pair[0], pair[1])


def mm_pairs(x, pair):
    dot = functools.partial(jnp.dot, preferred_element_type=F32)
    return dot(x[0], pair[0]) + (dot(x[1], pair[0]) + dot(x[0], pair[1]))


def store_pair(pair, x):
    high, low = split2(x)
    pair[0] = high
    pair[1] = low


def sweep_kernel(
    nlayer, nsplit, nchunk, nrow,
    rhs_in, diag_in, inv_in, sol_ref, res_ref,
    gbuf, mats, rsend, dsend, cols, dcols, low, dirb, imb, aimb, arb,
    pf, qf, pown, qown, pall, qall, q1, pin, qin,
    cvec, cin, ain, amid, evec, ein, bin_, bcore, zin, zout,
    xf, mbuf, xpair, xrow, vown, vbuf, inbuf,
    prefix, rf, rin, rpair, azero, ezero, ein0,
    zlow, zhigh, ylow, yhigh, edges, lines, flat, part, group, whole,
    rhs_ref, diag_ref, inv_ref, in_sem,
    rs_send, rs_recv, g_send, g_recv, c_send, c_recv,
    x_send, x_recv, v_send, v_recv, i_send, i_recv, z_send, z_recv, y_send, y_recv,
    h_send, h_recv, l_send, l_recv, n_send, n_recv, w_send, w_recv,
):
    planes, nx, width = inv_in.shape
    ysize = rhs_in.shape[2]
    yb = ysize // nsplit
    cb = yb // nchunk
    half = width // 2
    layer = lax.axis_index("layer")
    s = lax.axis_index("split")
    core = lax.rem(layer, 2)
    chip = layer // 2
    nchip = nlayer // 2
    right = lax.rem(s + 1, nsplit)
    left = lax.rem(s + nsplit - 1, nsplit)
    other = layer + 1 - 2 * core
    npos = 4
    pos, line = lax.rem(chip, npos), chip // npos
    nline = nchip // npos

    def rows(owner, start, size):
        return pl.ds(pl.multiple_of(owner * width + start, half), size)

    def lanes(t):
        return pl.ds(pl.multiple_of(t * width, width), width)

    def lines_of(t):
        return pl.ds(pl.multiple_of(t * yb, yb), yb)

    loads = [
        pltpu.make_async_copy(src, dst, in_sem.at[i])
        for i, (src, dst) in enumerate(
            ((inv_in, inv_ref), (rhs_in, rhs_ref), (diag_in, diag_ref))
        )
    ]
    for load in loads:
        load.start()
    for empty in (zlow, zhigh, ylow, yhigh, edges, part):
        empty[...] = jnp.zeros_like(empty)

    barrier = pltpu.get_barrier_semaphore()

    def greet(l, t):
        pl.semaphore_signal(barrier, inc=1, device_id=(l, t), device_id_type=MESH)

    for d in range(1, nsplit):
        greet(layer, lax.rem(s + d, nsplit))
    for d in range(nsplit):
        greet(other, lax.rem(s + d, nsplit))
    for d in range(1, nchip):
        greet(2 * lax.rem(chip + d, nchip) + core, s)
    side = layer - 1 + 2 * core
    inner = jnp.logical_and(side >= 0, side < nlayer)

    @pl.when(inner)
    def _():
        greet(side, s)

    loads[0].wait()
    for k in range(planes):
        gbuf[k, rows(s, 0, width), :] = inv_ref[k].T
    for i, (source, sent, mine) in enumerate(
        ((rhs_ref, rsend, cols), (diag_ref, dsend, dcols))
    ):
        loads[i + 1].wait()
        for k in range(planes):
            sent[k] = source[k].T
        for k in range(planes):
            mine[k, :, lanes(s)] = sent[k, lines_of(s), :]

    pl.semaphore_wait(barrier, 2 * nsplit - 1 + nchip - 1 + jnp.where(inner, 1, 0))

    def remote(src, dst, send, recv, l, t):
        return pltpu.make_async_remote_copy(
            src_ref=src, dst_ref=dst, send_sem=send, recv_sem=recv,
            device_id=(l, t), device_id_type=MESH,
        )

    def regroup(n, d):
        t = lax.rem(s + d, nsplit)
        sent, mine = ((rsend, cols), (dsend, dcols))[n]
        return remote(
            sent.at[:, lines_of(t), :], mine.at[:, :, lanes(s)],
            rs_send.at[n, d - 1], rs_recv.at[n, d - 1], layer, t,
        )

    def spread(n, d):
        t = lax.rem(s + d, nsplit)
        return remote(
            (dirb, imb, aimb, arb)[n].at[:, :, lanes(t)], lines.at[n, :, lines_of(s), :],
            l_send.at[n, d - 1], l_recv.at[n, d - 1], layer, t,
        )

    def spread_start(n, distances=None):
        for d in range(1, nsplit) if distances is None else distances:
            spread(n, d).start()
        if distances is not None and 1 not in distances:
            return
        for k in range(planes):
            lines[n, k, lines_of(s), :] = (dirb, imb, aimb, arb)[n][k, :, lanes(s)]

    def spread_finish(n):
        for d in range(1, nsplit):
            spread(n, d).wait_recv()
        for k in range(planes):
            flat[n, k] = lines[n, k].T

    def halo(n, i):
        values = (cols, dirb, imb)[n]
        src = (values.at[planes - 1], values.at[0], edges.at[n, 0], edges.at[n, 1])[i]
        dst = (zlow, zhigh, ylow, yhigh)[i].at[n]
        up, down = lax.rem(layer + 1, nlayer), lax.rem(layer + nlayer - 1, nlayer)
        l, t = ((up, s), (down, s), (layer, right), (layer, left))[i]
        return remote(src, dst, h_send.at[n, i], h_recv.at[n, i], l, t)

    to_high, to_low = layer < nlayer - 1, layer > 0
    to_right, to_left = s < nsplit - 1, s > 0
    gives = (to_high, to_low, to_right, to_left)
    takes = (to_low, to_high, to_left, to_right)

    def halo_start(n):
        values = (cols, dirb, imb)[n]
        for i in range(2):
            pl.when(gives[i])(lambda i=i: halo(n, i).start())
        for k in range(planes):
            edges[n, 0, k : k + 1, :] = values[k, yb - 1 : yb, :]
            edges[n, 1, k : k + 1, :] = values[k, 0:1, :]
        for i in range(2, 4):
            pl.when(gives[i])(lambda i=i: halo(n, i).start())

    def halo_wait(n):
        for i in range(4):
            pl.when(takes[i])(lambda i=i: halo(n, i).wait_recv())

    row = lax.broadcasted_iota(jnp.int32, (yb, nx), 0)
    lane = lax.broadcasted_iota(jnp.int32, (yb, nx), 1)

    def apply_operator(n, result):
        values = (cols, dirb, imb)[n]
        for k in range(planes):
            v = values[k]
            below = values[k - 1] if k > 0 else zlow[n]
            above = values[k + 1] if k < planes - 1 else zhigh[n]
            x_low = jnp.where(lane == 0, 0.0, pltpu.roll(v, 1, 1))
            x_high = jnp.where(lane == nx - 1, 0.0, pltpu.roll(v, nx - 1, 1))
            y_low = jnp.where(row == 0, ylow[n, k : k + 1, :], pltpu.roll(v, 1, 0))
            y_high = jnp.where(row == yb - 1, yhigh[n, k : k + 1, :], pltpu.roll(v, yb - 1, 0))
            beside = (below + above) + (x_low + x_high) + (y_low + y_high)
            result[k] = (6.0 + dcols[k]) * v - beside

    def put_sum(i, a, b):
        total = a[0] * b[0]
        for k in range(1, planes):
            total = total + a[k] * b[k]
        total = jnp.sum(total, axis=0, keepdims=True)
        lane_sum = total[:, :width]
        for t in range(1, nsplit):
            lane_sum = lane_sum + total[:, t * width : (t + 1) * width]
        part[i : i + 1, :] = lane_sum

    def prepare():
        for d in range(1, nsplit):
            regroup(1, d).wait_recv()
        halo_wait(0)
        apply_operator(0, arb)
        put_sum(0, cols, cols)
        put_sum(1, arb, cols)
        put_sum(2, arb, arb)

    def own_right(k):
        part = gbuf.at[k, rows(s, 0, width), :]
        return remote(part, part, g_send.at[0, k], g_recv.at[0, k], layer, right)

    def own_left(k):
        part = gbuf.at[k, rows(s, 0, width), :]
        return remote(part, part, g_send.at[1, k], g_recv.at[1, k], layer, left)

    def pass_right(k):
        part = gbuf.at[k, rows(left, 0, half), :]
        return remote(part, part, g_send.at[2, k], g_recv.at[2, k], layer, right)

    def pass_left(k):
        part = gbuf.at[k, rows(right, half, half), :]
        return remote(part, part, g_send.at[3, k], g_recv.at[3, k], layer, left)

    for d in range(1, nsplit):
        regroup(0, d).start()
    for k in range(min(2, planes)):
        own_right(k).start()
        own_left(k).start()

    def relay(k):
        own_right(k).wait_recv()
        pass_right(k).start()
        own_left(k).wait_recv()
        pass_left(k).start()
        if k + 2 < planes:
            own_right(k + 2).start()
            own_left(k + 2).start()
        if k == planes - 1:
            for d in range(1, nsplit):
                regroup(1, d).start()

    def absorb(k):
        pass_right(k).wait_recv()
        pass_left(k).wait_recv()
        full = gbuf[k]
        high, lowpart = split2(full)
        mats[k, 0] = high
        mats[k, 1] = lowpart
        if k == 0:
            for d in range(1, nsplit):
                regroup(0, d).wait_recv()
            halo_start(0)
            cvec[...] = mm(cols[0], high, lowpart)
            pf[...] = full
            qown[0] = high
            qown[1] = lowpart
        else:
            prefix[k - 1] = pf[...]
            pf[...] = mm(pf[...], high, lowpart)
            if k == planes - 1:
                pl.when(core == 1)(lambda: give_p.start())
            cvec[...] = mm(cols[k] + cvec[...], high, lowpart)

    def absorb_up(k):
        if k > 0:
            qf[...] = mm(gbuf[k], qown[0], qown[1])
            store_pair(qown, qf[...])

    give_p = remote(pf, pin, c_send.at[0], c_recv.at[0], other, s)
    for k in range(planes):
        relay(k)
        if k > 0:
            absorb(k - 1)
            absorb_up(k - 1)
    absorb(planes - 1)

    give_q = remote(qf, qin, c_send.at[1], c_recv.at[1], other, s)
    give_c = remote(cvec, cin, c_send.at[2], c_recv.at[2], other, s)
    give_a = remote(amid, ain, c_send.at[3], c_recv.at[3], other, s)
    give_e = remote(evec, ein, c_send.at[4], c_recv.at[4], other, s)
    give_b = remote(bin_, bcore, c_send.at[5], c_recv.at[5], other, s)
    give_r = remote(rf, rin, c_send.at[6], c_recv.at[6], other, s)
    give_a0 = remote(cvec, azero, c_send.at[7], c_recv.at[7], other, s)
    give_e0 = remote(ezero, ein0, c_send.at[8], c_recv.at[8], other, s)

    hosts = (npos - 1, 0)

    def row_layer(at):
        return 2 * (line * npos + at)

    def chunk(q):
        return pl.ds(q * cb, cb)

    def shared(step):
        return (0, width) if step == 1 else (nx - nx // 4, width // 4)

    def hand_share(way, step, piece=0):
        base, size = shared(step)
        length = size // 2 if step == 1 else size
        part = pl.ds(pl.multiple_of(base + s * size + piece * length, length), length)
        return remote(
            xf.at[way, part, :], mbuf.at[step, part, :],
            x_send.at[way, 2 * piece], x_recv.at[step, 2 * piece], row_layer(hosts[way]), s,
        )

    def pieces(step):
        return (0, 1) if step == 1 else (0,)

    def shares_start(way, step):
        for piece in pieces(step):
            hand_share(way, step, piece).start()

    def shares_end(way, step):
        for piece in pieces(step):
            hand_share(way, step, piece).wait_send()

    def hand_whole(way, step):
        part = pl.ds(0, nx - nx // 4)
        return remote(
            xf.at[way, part, :], mbuf.at[step, part, :],
            x_send.at[way, 1], x_recv.at[step, 1], row_layer(hosts[way]), s,
        )

    def hand_wholes(way, do):
        for step in (0, 2):
            at = step if way == 0 else npos - 1 - step
            pl.when(pos == at)(functools.partial(do, step))

    def hand_vector(way, step):
        return remote(
            vown.at[way], vbuf.at[step], v_send.at[way], v_recv.at[step],
            row_layer(hosts[way]), s,
        )

    def hand_input(way, step):
        return remote(
            inbuf.at[step], (ain, bin_)[way], i_send.at[step], i_recv.at[way],
            row_layer(step if way == 0 else npos - 1 - step), s,
        )

    def hand_on(way, q):
        return remote(
            zout.at[chunk(q), :], zin.at[chunk(q), :], z_send.at[q], z_recv.at[q],
            lax.rem(layer + nlayer + (2 - 4 * way) * npos, nlayer), s,
        )

    def ring(step, i):
        base, size = shared(step)
        h = size // 2
        own = (s, 0, size)
        owner, start, length = (
            (s, 0, h) if step == 1 else own, (s, h, h) if step == 1 else own,
            (left, 0, h), (right, h, h), (s, h, h), (s, 0, h),
        )[i]
        rows_at = pl.multiple_of(base + owner * size + start, h)
        part = mbuf.at[step, pl.ds(rows_at, length), :]
        return remote(
            part, part, y_send.at[step, i], y_recv.at[step, i], layer,
            (right, left, right, left, right, left)[i],
        )

    def ring_copies(step):
        return range(6) if step == 1 else range(4)

    def for_step(way, do):
        for step in range(npos - 1):
            at = step if way == 0 else npos - 1 - step
            pl.when(pos == at)(functools.partial(do, step))

    def row_vector(way):
        own = pall if way == 0 else qall
        for step in range(npos - 1):
            hand_vector(way, step).wait_recv()
        total = vbuf[0]
        for step in range(1, npos - 1):
            total = vbuf[step] + mm_ref(total, xpair.at[step])
        zout[...] = vown[way] + mm_ref(total, own)

    def line_starts(way):
        return line == 0 if way == 0 else line == nline - 1

    def line_ends(way):
        return line == nline - 1 if way == 0 else line == 0

    def send_first(way):
        for q in range(nchunk):
            hand_on(way, q).start()

    def host_prepare(way, meanwhile):
        own = pall if way == 0 else qall
        store_pair(own, xf[way])
        order = (1, 2, 0)
        for step in order:
            hand_share(way, step).wait_recv()
            ring(step, 0).start()
            if step == 1:
                ring(step, 5).start()
                hand_share(way, step, 1).wait_recv()
                ring(step, 4).start()
            ring(step, 1).start()
        for step in order:
            ring(step, 0).wait_recv()
            ring(step, 2).start()
            ring(step, 1).wait_recv()
            ring(step, 3).start()
        meanwhile()
        starts = line_starts(way)
        upper, lower = pl.ds(0, nx - nx // 4), pl.ds(nx - nx // 4, nx // 4)

        def passed(step):
            for i in ring_copies(step)[2:]:
                ring(step, i).wait_recv()

        def ahead_of_rest(part):
            pin[part, :] = mm_ref(mbuf[2, part, :], own)

        hand_whole(way, 2).wait_recv()
        pl.when(jnp.logical_not(starts))(functools.partial(ahead_of_rest, upper))
        passed(1)
        store_pair(xpair.at[1], mbuf[1])
        passed(2)
        store_pair(xpair.at[2], mbuf[2])
        if way == 0:
            row_vector(way)
            if nline > 1:
                pl.when(starts)(functools.partial(send_first, way))
        hand_whole(way, 0).wait_recv()

        @pl.when(jnp.logical_not(starts))
        def _():
            pf[upper, :] = mm_ref(mbuf[0, upper, :], xpair.at[1])
            ahead_of_rest(lower)
            store_pair(xrow, pin[...])

        passed(0)

        @pl.when(jnp.logical_not(starts))
        def _():
            pf[lower, :] = mm_ref(mbuf[0, lower, :], xpair.at[1])
            store_pair(xrow, mm_ref(pf[...], xrow))

        store_pair(xpair.at[0], mbuf[0])

    def host_chain(way):
        starts, ends = line_starts(way), line_ends(way)
        if way == 1:
            row_vector(way)

        @pl.when(starts)
        def _():
            inbuf[0] = jnp.zeros((yb, nx), F32)
            if way == 1 and nline > 1:
                send_first(way)

        @pl.when(jnp.logical_not(starts))
        def _():
            for q in range(nchunk):
                hand_on(way, q).wait_recv()

                @pl.when(jnp.logical_not(ends))
                def _():
                    zout[chunk(q), :] = zout[chunk(q), :] + mm_ref(zin[chunk(q), :], xrow)
                    hand_on(way, q).start()

            inbuf[0] = zin[...]

        state = inbuf[0]
        for step in range(npos - 1):
            hand_input(way, step).start()
            state = vbuf[step] + mm_ref(state, xpair.at[step])
            if step < npos - 2:
                inbuf[step + 1] = state
        (ain, bin_)[way][...] = state

    def host_finish(way):
        ends = line_ends(way)
        for step in range(npos - 1):
            hand_input(way, step).wait_send()
        for step in range(npos - 1):
            for i in ring_copies(step):
                ring(step, i).wait_send()

        @pl.when(jnp.logical_not(ends))
        def _():
            for q in range(nchunk):
                hand_on(way, q).wait_send()

    @pl.when(core == 1)
    def _():
        give_c.start()
        absorb_up(planes - 1)

    def down_sweep(state):
        for k in range(planes):
            state = mm(cols[k] + state, mats[k, 0], mats[k, 1])
            low[k] = state

    def up_partial(result):
        state = low[planes - 1]
        for k in range(planes - 2, -1, -1):
            state = low[k] + mm(state, mats[k, 0], mats[k, 1])
        result[...] = state

    def response():
        rf[...] = prefix[planes - 2] + mm(pf[...], mats[planes - 2, 0], mats[planes - 2, 1])
        for k in range(planes - 3, -1, -1):
            rf[...] = prefix[k] + mm(rf[...], mats[k, 0], mats[k, 1])

    def up_sweep(state):
        for k in range(planes - 1, -1, -1):
            state = low[k] + mm(state, mats[k, 0], mats[k, 1])
            dirb[k] = state

    @pl.when(core == 1)
    def _():
        give_q.start()
        response()
        give_r.start()
        give_a0.wait_recv()
        down_sweep(azero[...])
        up_partial(ezero)
        give_e0.start()
        prepare()
        give_a.wait_recv()
        down_sweep(ain[...])
        up_partial(evec)
        give_e.start()
        spread_start(3)
        give_b.wait_recv()
        up_sweep(bcore[...])
        for give in (give_c, give_p, give_q, give_r, give_e0, give_e):
            give.wait_send()

    @pl.when(core == 0)
    def _():
        give_a0.start()
        store_pair(pown, pf[...])
        give_p.wait_recv()
        store_pair(pall, pin[...])
        xf[0] = mm_pairs(pown, pall)
        for_step(0, functools.partial(shares_start, 0))
        give_c.wait_recv()
        vown[0] = mm_ref(cvec[...], pall) + cin[...]
        for_step(0, lambda step: hand_vector(0, step).start())
        absorb_up(planes - 1)
        give_q.wait_recv()
        store_pair(q1, qin[...])
        xf[1] = mm_pairs(q1, qown)
        for_step(1, functools.partial(shares_start, 1))
        hand_wholes(0, lambda step: hand_whole(0, step).start())
        hand_wholes(1, lambda step: hand_whole(1, step).start())
        prepare()

        response()

        def still():
            give_r.wait_recv()
            store_pair(rpair, rin[...])
            rin[...] = mm_pairs(pown, rpair)
            rf[...] = rf[...] + mm_ref(rin[...], qown)
            store_pair(rpair, rf[...])
            down_sweep(jnp.zeros((yb, nx), F32))
            up_partial(ezero)
            give_e0.wait_recv()
            ezero[...] = ezero[...] + mm_ref(ein0[...], qown)

        @pl.when(pos == hosts[0])
        def _():
            host_prepare(0, still)
            host_chain(0)

        @pl.when(pos == hosts[1])
        def _():
            host_prepare(1, still)

        @pl.when(jnp.logical_and(pos != hosts[0], pos != hosts[1]))
        def _():
            still()

        for_step(0, lambda step: hand_input(0, step).wait_recv())
        vown[1] = ezero[...] + mm_ref(ain[...], rpair)
        for_step(1, lambda step: hand_vector(1, step).start())
        amid[...] = cvec[...] + mm_ref(ain[...], pown)
        give_a.start()
        spread_start(3)
        down_sweep(ain[...])

        @pl.when(pos == hosts[1])
        def _():
            host_chain(1)

        give_e.wait_recv()
        for_step(1, lambda step: hand_input(1, step).wait_recv())
        give_b.start()
        up_sweep(ein[...] + mm_ref(bin_[...], q1))
        give_a0.wait_send()
        give_a.wait_send()
        give_b.wait_send()
        for way in range(2):
            for_step(way, lambda step, way=way: hand_vector(way, step).wait_send())
            for_step(way, functools.partial(shares_end, way))
            hand_wholes(way, lambda step, way=way: hand_whole(way, step).wait_send())
            pl.when(pos == hosts[way])(functools.partial(host_finish, way))

    halo_start(1)
    spread_start(0)
    halo_wait(1)
    apply_operator(1, imb)
    halo_start(2)
    spread_start(1, (1, nsplit - 1))
    halo_wait(2)
    apply_operator(2, aimb)
    put_sum(3, cols, imb)
    put_sum(4, arb, imb)
    put_sum(5, aimb, cols)
    put_sum(6, aimb, imb)
    put_sum(7, arb, aimb)
    put_sum(8, aimb, aimb)

    place = core * nsplit + s
    count = 2 * nsplit

    def near(d):
        at = lax.rem(place + d, count)
        return remote(
            group.at[place], group.at[place], n_send.at[d - 1], n_recv.at[d - 1],
            2 * chip + at // nsplit, lax.rem(at, nsplit),
        )

    def far(d):
        at = lax.rem(chip + d, nchip)
        return remote(
            whole.at[chip], whole.at[chip], w_send.at[d - 1], w_recv.at[d - 1],
            2 * at + core, s,
        )

    diagonal = lax.broadcasted_iota(jnp.int32, (nrow, width), 0) == lax.broadcasted_iota(
        jnp.int32, (nrow, width), 1
    )
    sums = jnp.where(diagonal, jnp.sum(part[...], axis=1, keepdims=True), 0.0)
    group[place] = jnp.sum(sums, axis=0, keepdims=True)
    for d in range(1, count):
        near(d).start()
    spread_start(1, range(2, nsplit - 1))
    spread_start(2)
    for n in (3, 0):
        spread_finish(n)
    for d in range(1, count):
        near(d).wait_recv()
    total = group[0]
    for i in range(1, count):
        total = total + group[i]
    whole[chip] = total
    for d in range(1, nchip):
        far(d).start()
    for n in (1, 2):
        spread_finish(n)
    for d in range(1, nchip):
        far(d).wait_recv()
    total = whole[0]
    for i in range(1, nchip):
        total = total + whole[i]
    rr, ar, aa, ri, ai, br, bi, ab, bb = [total[:, i : i + 1] for i in range(9)]
    alpha = rr / ri
    cross = ar - alpha * (ai + br) + alpha * alpha * bi
    own = aa - 2.0 * alpha * ab + alpha * alpha * bb
    omega = cross / own
    for k in range(planes):
        middle = rhs_ref[k] - alpha * flat[1, k]
        sol_ref[k] = alpha * flat[0, k] + omega * middle
        res_ref[k] = middle - omega * (flat[3, k] - alpha * flat[2, k])

    for n in range(2):
        for d in range(1, nsplit):
            regroup(n, d).wait_send()
    for k in range(planes):
        own_right(k).wait_send()
        own_left(k).wait_send()
        pass_right(k).wait_send()
        pass_left(k).wait_send()
    for n in range(4):
        for d in range(1, nsplit):
            spread(n, d).wait_send()
    for n in range(3):
        for i in range(4):
            pl.when(gives[i])(lambda n=n, i=i: halo(n, i).wait_send())
    for d in range(1, count):
        near(d).wait_send()
    for d in range(1, nchip):
        far(d).wait_send()


def per_device(nlayer, nsplit, right_side, diagonal, inverses):
    planes, nx, width = inverses.shape
    ysize = right_side.shape[2]
    yb = ysize // nsplit
    nchip = nlayer // 2
    nchunk = 2
    nrow = 16
    vmem = pl.BlockSpec(memory_space=pltpu.VMEM)
    square = pltpu.VMEM((nx, nx), F32)
    pair = pltpu.VMEM((2, nx, nx), BF16)
    strip = pltpu.VMEM((yb, nx), F32)
    columns = pltpu.VMEM((planes, yb, nx), F32)
    block = pltpu.VMEM((planes, ysize, width), F32)
    dma = pltpu.SemaphoreType.DMA
    shape = jax.ShapeDtypeStruct((planes, width, ysize), F32)
    return pl.pallas_call(
        functools.partial(sweep_kernel, nlayer, nsplit, nchunk, nrow),
        out_shape=(shape, shape),
        in_specs=[pl.BlockSpec(memory_space=pltpu.HBM)] * 3,
        out_specs=(vmem, vmem),
        scratch_shapes=[
            pltpu.VMEM((planes, nx, nx), F32),
            pltpu.VMEM((planes, 2, nx, nx), BF16),
            block, block,
            columns, columns, columns, columns, columns, columns, columns,
            square, square, pair, pair, pair, pair, pair, square, square,
            strip, strip, strip, strip, strip, strip, strip, strip, strip, strip,
            pltpu.VMEM((2, nx, nx), F32), pltpu.VMEM((3, nx, nx), F32),
            pltpu.VMEM((3, 2, nx, nx), BF16), pair,
            pltpu.VMEM((2, yb, nx), F32), pltpu.VMEM((3, yb, nx), F32),
            pltpu.VMEM((3, yb, nx), F32),
            pltpu.VMEM((planes - 1, nx, nx), F32), square, square, pair, strip, strip, strip,
            pltpu.VMEM((3, yb, nx), F32), pltpu.VMEM((3, yb, nx), F32),
            pltpu.VMEM((3, 8, nx), F32), pltpu.VMEM((3, 8, nx), F32),
            pltpu.VMEM((3, 2, 8, nx), F32),
            pltpu.VMEM((4, planes, ysize, width), F32),
            pltpu.VMEM((4, planes, width, ysize), F32),
            pltpu.VMEM((nrow, width), F32),
            pltpu.VMEM((2 * nsplit, 1, width), F32),
            pltpu.VMEM((nchip, 1, width), F32),
            pltpu.VMEM((planes, width, ysize), F32), pltpu.VMEM((planes, width, ysize), F32),
            pltpu.VMEM((planes, nx, width), F32), dma((3,)),
            dma((2, nsplit - 1)), dma((2, nsplit - 1)),
            dma((4, planes)), dma((4, planes)),
            dma((9,)), dma((9,)),
            dma((2, 3)), dma((3, 3)), dma((2,)), dma((3,)), dma((3,)), dma((2,)),
            dma((nchunk,)), dma((nchunk,)), dma((3, 6)), dma((3, 6)),
            dma((3, 4)), dma((3, 4)),
            dma((4, nsplit - 1)), dma((4, nsplit - 1)),
            dma((2 * nsplit - 1,)), dma((2 * nsplit - 1,)),
            dma((nchip - 1,)), dma((nchip - 1,)),
        ],
        compiler_params=pltpu.CompilerParams(
            collective_id=0, has_side_effects=True, vmem_limit_bytes=56 * 1024 * 1024
        ),
        name="sweeps",
    )(right_side, diagonal, inverses)


def solution(mesh):
    spec = P("layer", "split", None)
    return jax.shard_map(
        functools.partial(per_device, mesh.shape["layer"], mesh.shape["split"]),
        mesh=mesh,
        in_specs=(spec, spec, P("layer", None, "split")),
        out_specs=(spec, spec),
        check_vma=False,
    )
```
